8 devices in a mesh: dp: 1 (over z), ep: 8 (over y, x, core).
Axes of the slice: x: 2, y: 2, z: 1, core: 2. Of those that a mesh axis runs over, the one named last changes fastest.
Arguments:
- hidden: bfloat16 [512, 768], P(('dp', 'ep'))
- self_pos: int32 [512], P(('dp', 'ep'))
- src_len: int32 [512], P(('dp', 'ep'))
- cache_a: bfloat16 [2, 512, 16, 12, 64], P(None, ('dp', 'ep'))
- cross_a: bfloat16 [2, 512, 64, 12, 64], P(None, ('dp', 'ep'))
- cache_b: bfloat16 [2, 512, 16, 12, 64], P(None, ('dp', 'ep'))
- cross_b: bfloat16 [2, 512, 64, 12, 64], P(None, ('dp', 'ep'))
- route_ids: int32 [512, 2], P(('dp', 'ep'))
- ln_gain: float32 [2, 3, 768], replicated
- ln_shift: float32 [2, 3, 768], replicated
- attn_w: bfloat16 [2, 6, 768, 768], replicated
- attn_b: bfloat16 [2, 6, 768], replicated
- ffn_w1: bfloat16 [768, 3072], replicated
- ffn_b1: bfloat16 [3072], replicated
- ffn_w2: bfloat16 [3072, 768], replicated
- ffn_b2: bfloat16 [768], replicated
- router_w: bfloat16 [768, 128], replicated
- exp_w1: bfloat16 [128, 768, 3072], P('ep')
- exp_b1: bfloat16 [128, 3072], P('ep')
- exp_w2: bfloat16 [128, 3072, 768], P('ep')
- exp_b2: bfloat16 [128, 768], P('ep')
Outputs:
- output 1: bfloat16 [512, 768], P(('dp', 'ep'))
- output 2: bfloat16 [2, 512, 16, 12, 64], P(None, ('dp', 'ep'))
- output 3: bfloat16 [2, 512, 16, 12, 64], P(None, ('dp', 'ep'))
All inputs are finite; a program needn't handle non-finite values.
Results may differ from the reference program's by a relative error of at most 0.00603.
Values are sent between devices in bfloat16 or wider.
A program may use at most 1 GiB of HBM per device.

```python
import jax
import jax.numpy as jnp
from jax import lax

D_MODEL = 768
NUM_HEADS = 12
HEAD_DIM = 64
FF_DIM = 3072
EXPERTS = 128
GROUP_SIZE = 8
TOK_DEV = 64
SELF_LEN = 16
SRC_LEN = 64

TOKENS = GROUP_SIZE * TOK_DEV
CAPACITY = max(1, (4 * TOK_DEV) // GROUP_SIZE)
LOCAL_EXPERTS = EXPERTS // GROUP_SIZE
LN_EPS = 1e-5


def draw_routes(route_key):
    blocks = TOK_DEV // CAPACITY
    key_loc, key_base, key_perm, key_swap = jax.random.split(route_key, 4)
    src_dev = jnp.arange(GROUP_SIZE)
    rand_base = jax.random.randint(key_base, (GROUP_SIZE,), 0, GROUP_SIZE)
    base_dev = jnp.where(src_dev % 2 == 0, src_dev * blocks, rand_base)
    dev_first = (base_dev[:, None] + jnp.arange(blocks)[None, :]) % GROUP_SIZE
    dev_second = (dev_first + blocks) % GROUP_SIZE
    local_ids = jax.random.randint(key_loc, (2, GROUP_SIZE, blocks), 0, LOCAL_EXPERTS)
    pair_ids = jnp.stack([dev_first * LOCAL_EXPERTS + local_ids[0], dev_second * LOCAL_EXPERTS + local_ids[1]], axis=-1)
    pair_ids = jnp.repeat(pair_ids, CAPACITY, axis=1)
    perm_keys = jax.random.split(key_perm, GROUP_SIZE)
    tok_perm = jax.vmap(lambda one_key: jax.random.permutation(one_key, TOK_DEV))(perm_keys)
    pair_ids = jnp.take_along_axis(pair_ids, tok_perm[:, :, None], axis=1)
    swap_flag = jax.random.randint(key_swap, (GROUP_SIZE, TOK_DEV, 1), 0, 2)
    pair_ids = jnp.where(swap_flag == 1, pair_ids[:, :, ::-1], pair_ids)
    return pair_ids.reshape(TOKENS, 2).astype(jnp.int32)


def draw_cache(one_key, length, used_len):
    raw_vals = jax.random.normal(one_key, (2, TOKENS, length, NUM_HEADS, HEAD_DIM), jnp.float32)
    v_scale = jnp.sqrt(used_len.astype(jnp.float32) * 0.25 + 1.0)
    kv_scale = jnp.stack([jnp.ones_like(v_scale), v_scale])[:, :, None, None, None]
    return (raw_vals * kv_scale).astype(jnp.bfloat16)


def normal_bf(one_key, shape_t, scale_f):
    return (jax.random.normal(one_key, shape_t, jnp.float32) * scale_f).astype(jnp.bfloat16)


def setup_inputs(seed: int = 0, part: int = 0) -> dict:
    part_keys = jax.random.split(jax.random.fold_in(jax.random.key(seed), part), 8)
    weight_keys = jax.random.split(jax.random.key(seed + 1), 13)
    self_pos = jax.random.randint(part_keys[0], (TOKENS,), 0, SELF_LEN).at[0].set(SELF_LEN - 1)
    src_len = jax.random.randint(part_keys[1], (TOKENS,), 1, SRC_LEN + 1).at[0].set(SRC_LEN)
    hidden = jax.random.normal(part_keys[2], (TOKENS, D_MODEL), jnp.float32).astype(jnp.bfloat16)
    d_scale = D_MODEL ** -0.5
    f_scale = FF_DIM ** -0.5
    return {
        'hidden': hidden,
        'self_pos': self_pos.astype(jnp.int32),
        'src_len': src_len.astype(jnp.int32),
        'cache_a': draw_cache(part_keys[3], SELF_LEN, self_pos + 1),
        'cross_a': draw_cache(part_keys[4], SRC_LEN, src_len),
        'cache_b': draw_cache(part_keys[5], SELF_LEN, self_pos + 1),
        'cross_b': draw_cache(part_keys[6], SRC_LEN, src_len),
        'route_ids': draw_routes(part_keys[7]),
        'ln_gain': 1.0 + 0.2 * jax.random.normal(weight_keys[0], (2, 3, D_MODEL), jnp.float32),
        'ln_shift': 0.2 * jax.random.normal(weight_keys[1], (2, 3, D_MODEL), jnp.float32),
        'attn_w': normal_bf(weight_keys[2], (2, 6, D_MODEL, D_MODEL), d_scale),
        'attn_b': normal_bf(weight_keys[3], (2, 6, D_MODEL), 0.2),
        'ffn_w1': normal_bf(weight_keys[4], (D_MODEL, FF_DIM), d_scale),
        'ffn_b1': normal_bf(weight_keys[5], (FF_DIM,), 0.2),
        'ffn_w2': normal_bf(weight_keys[6], (FF_DIM, D_MODEL), f_scale),
        'ffn_b2': normal_bf(weight_keys[7], (D_MODEL,), 0.2),
        'router_w': normal_bf(weight_keys[8], (D_MODEL, EXPERTS), 2.0 * d_scale),
        'exp_w1': normal_bf(weight_keys[9], (EXPERTS, D_MODEL, FF_DIM), d_scale),
        'exp_b1': normal_bf(weight_keys[10], (EXPERTS, FF_DIM), 0.2),
        'exp_w2': normal_bf(weight_keys[11], (EXPERTS, FF_DIM, D_MODEL), f_scale),
        'exp_b2': normal_bf(weight_keys[12], (EXPERTS, D_MODEL), 0.2),
    }


def layer_norm(x_val, gain_vec, shift_vec):
    mean_val = jnp.mean(x_val, axis=-1, keepdims=True)
    centered = x_val - mean_val
    var_val = jnp.mean(centered * centered, axis=-1, keepdims=True)
    return (centered * lax.rsqrt(var_val + LN_EPS) * gain_vec + shift_vec).astype(jnp.bfloat16)


def project(x_bf, w_mat, b_vec):
    return jnp.dot(x_bf, w_mat, preferred_element_type=jnp.float32) + b_vec.astype(jnp.float32)


def attend_rows(query_h, keys_all, vals_all, valid_mask):
    def one_row(row_args):
        q_row, k_rows, v_rows, m_row = row_args
        scores = jnp.einsum('hd,shd->hs', q_row.astype(jnp.float32), k_rows.astype(jnp.float32)) * HEAD_DIM ** -0.5
        scores = jnp.where(m_row[None, :], scores, -1e30)
        prob_w = jax.nn.softmax(scores, axis=-1).astype(jnp.bfloat16)
        context = jnp.einsum('hs,shd->hd', prob_w.astype(jnp.float32), v_rows.astype(jnp.float32))
        return context.astype(jnp.bfloat16)
    context = lax.map(one_row, (query_h, keys_all, vals_all, valid_mask))
    return context.reshape(TOKENS, D_MODEL)


def self_block(hid_f32, self_cache, self_pos, gain_vec, shift_vec, w_layer, b_layer):
    x_bf = layer_norm(hid_f32, gain_vec, shift_vec)
    query_h = project(x_bf, w_layer[0], b_layer[0]).astype(jnp.bfloat16).reshape(TOKENS, NUM_HEADS, HEAD_DIM)
    new_k = project(x_bf, w_layer[1], b_layer[1]).astype(jnp.bfloat16).reshape(TOKENS, NUM_HEADS, HEAD_DIM)
    new_v = project(x_bf, w_layer[2], b_layer[2]).astype(jnp.bfloat16).reshape(TOKENS, NUM_HEADS, HEAD_DIM)
    row_ids = jnp.arange(SELF_LEN)[None, :]
    row_hit = row_ids == self_pos[:, None]
    new_kv = jnp.stack([new_k, new_v])
    cache_new = jnp.where(row_hit[None, :, :, None, None], new_kv[:, :, None], self_cache)
    context = attend_rows(query_h, cache_new[0], cache_new[1], row_ids <= self_pos[:, None])
    return hid_f32 + project(context, w_layer[3], b_layer[3]), cache_new


def cross_block(hid_f32, cross_cache, src_len, gain_vec, shift_vec, w_layer, b_layer):
    x_bf = layer_norm(hid_f32, gain_vec, shift_vec)
    query_h = project(x_bf, w_layer[4], b_layer[4]).astype(jnp.bfloat16).reshape(TOKENS, NUM_HEADS, HEAD_DIM)
    valid_mask = jnp.arange(SRC_LEN)[None, :] < src_len[:, None]
    context = attend_rows(query_h, cross_cache[0], cross_cache[1], valid_mask)
    return hid_f32 + project(context, w_layer[5], b_layer[5])


def reference(hidden, self_pos, src_len, cache_a, cross_a, cache_b, cross_b, route_ids, ln_gain, ln_shift, attn_w, attn_b, ffn_w1, ffn_b1, ffn_w2, ffn_b2, router_w, exp_w1, exp_b1, exp_w2, exp_b2):
    hid_f32 = hidden.astype(jnp.float32)
    hid_f32, cache_a_new = self_block(hid_f32, cache_a, self_pos, ln_gain[0, 0], ln_shift[0, 0], attn_w[0], attn_b[0])
    hid_f32 = cross_block(hid_f32, cross_a, src_len, ln_gain[0, 1], ln_shift[0, 1], attn_w[0], attn_b[0])
    x_bf = layer_norm(hid_f32, ln_gain[0, 2], ln_shift[0, 2])
    inner = jnp.maximum(project(x_bf, ffn_w1, ffn_b1), 0.0).astype(jnp.bfloat16)
    hid_f32 = hid_f32 + project(inner, ffn_w2, ffn_b2)
    hid_f32, cache_b_new = self_block(hid_f32, cache_b, self_pos, ln_gain[1, 0], ln_shift[1, 0], attn_w[1], attn_b[1])
    hid_f32 = cross_block(hid_f32, cross_b, src_len, ln_gain[1, 1], ln_shift[1, 1], attn_w[1], attn_b[1])
    z_bf = layer_norm(hid_f32, ln_gain[1, 2], ln_shift[1, 2])
    probs_r = jax.nn.softmax(jnp.dot(z_bf, router_w, preferred_element_type=jnp.float32), axis=-1)
    chosen = jnp.take_along_axis(probs_r, route_ids, axis=1)
    gate_w = chosen / jnp.sum(chosen, axis=1, keepdims=True)

    def one_token(tok_args):
        z_row, ids_row = tok_args
        inner_k = jnp.einsum('d,kdf->kf', z_row.astype(jnp.float32), exp_w1[ids_row].astype(jnp.float32)) + exp_b1[ids_row].astype(jnp.float32)
        inner_k = jnp.maximum(inner_k, 0.0).astype(jnp.bfloat16)
        out_k = jnp.einsum('kf,kfd->kd', inner_k.astype(jnp.float32), exp_w2[ids_row].astype(jnp.float32)) + exp_b2[ids_row].astype(jnp.float32)
        return out_k.astype(jnp.bfloat16)

    expert_out = lax.map(one_token, (z_bf, route_ids))
    hid_f32 = hid_f32 + jnp.sum(gate_w[:, :, None] * expert_out.astype(jnp.float32), axis=1)
    return (hid_f32.astype(jnp.bfloat16), cache_a_new, cache_b_new)
```

```python
import functools

import jax
import jax.numpy as jnp
from jax import lax
from jax.experimental import pallas as pl
from jax.experimental.pallas import tpu as pltpu
from jax.sharding import PartitionSpec as P

LN_EPS = 1e-5
F32 = jnp.float32
BF16 = jnp.bfloat16
VMEM = pltpu.VMEM


def layer_norm(x_val, gain_vec, shift_vec):
    mean_val = jnp.mean(x_val, axis=-1, keepdims=True)
    centered = x_val - mean_val
    var_val = jnp.mean(centered * centered, axis=-1, keepdims=True)
    return (centered * lax.rsqrt(var_val + LN_EPS) * gain_vec + shift_vec).astype(jnp.bfloat16)


def project(x_bf, w_mat, b_vec):
    return jnp.dot(x_bf, w_mat, preferred_element_type=jnp.float32) + b_vec.astype(jnp.float32)


def attend(query_h, keys_all, vals_all, valid_mask):
    attn_scale = keys_all.shape[-1] ** -0.5
    scores = jnp.einsum('bhd,bshd->bhs', query_h, keys_all, preferred_element_type=jnp.float32) * attn_scale
    scores = jnp.where(valid_mask[:, None, :], scores, -1e30)
    prob_w = jax.nn.softmax(scores, axis=-1).astype(jnp.bfloat16)
    context = jnp.einsum('bhs,bshd->bhd', prob_w, vals_all, preferred_element_type=jnp.float32)
    return context.astype(jnp.bfloat16).reshape(query_h.shape[0], -1)


def self_block(hid_f32, self_cache, self_pos, gain_vec, shift_vec, w_layer, b_layer):
    n_heads, head_dim = self_cache.shape[3], self_cache.shape[4]
    x_bf = layer_norm(hid_f32, gain_vec, shift_vec)
    query_h = project(x_bf, w_layer[0], b_layer[0]).astype(jnp.bfloat16).reshape(-1, n_heads, head_dim)
    new_k = project(x_bf, w_layer[1], b_layer[1]).astype(jnp.bfloat16).reshape(-1, n_heads, head_dim)
    new_v = project(x_bf, w_layer[2], b_layer[2]).astype(jnp.bfloat16).reshape(-1, n_heads, head_dim)
    row_ids = jnp.arange(self_cache.shape[2])[None, :]
    row_hit = row_ids == self_pos[:, None]
    new_kv = jnp.stack([new_k, new_v])
    cache_new = jnp.where(row_hit[None, :, :, None, None], new_kv[:, :, None], self_cache)
    context = attend(query_h, cache_new[0], cache_new[1], row_ids <= self_pos[:, None])
    return hid_f32 + project(context, w_layer[3], b_layer[3]), cache_new


def cross_block(hid_f32, cross_cache, src_len, gain_vec, shift_vec, w_layer, b_layer):
    n_heads, head_dim = cross_cache.shape[3], cross_cache.shape[4]
    x_bf = layer_norm(hid_f32, gain_vec, shift_vec)
    query_h = project(x_bf, w_layer[4], b_layer[4]).astype(jnp.bfloat16).reshape(-1, n_heads, head_dim)
    valid_mask = jnp.arange(cross_cache.shape[2])[None, :] < src_len[:, None]
    context = attend(query_h, cross_cache[0], cross_cache[1], valid_mask)
    return hid_f32 + project(context, w_layer[5], b_layer[5])


def dense_layers(hidden, self_pos, src_len, cache_a, cross_a, cache_b, cross_b, ln_gain, ln_shift, attn_w, attn_b, ffn_w1, ffn_b1, ffn_w2, ffn_b2):
    hid_f32 = hidden.astype(jnp.float32)
    hid_f32, cache_a_new = self_block(hid_f32, cache_a, self_pos, ln_gain[0, 0], ln_shift[0, 0], attn_w[0], attn_b[0])
    hid_f32 = cross_block(hid_f32, cross_a, src_len, ln_gain[0, 1], ln_shift[0, 1], attn_w[0], attn_b[0])
    x_bf = layer_norm(hid_f32, ln_gain[0, 2], ln_shift[0, 2])
    inner = jnp.maximum(project(x_bf, ffn_w1, ffn_b1), 0.0).astype(jnp.bfloat16)
    hid_f32 = hid_f32 + project(inner, ffn_w2, ffn_b2)
    hid_f32, cache_b_new = self_block(hid_f32, cache_b, self_pos, ln_gain[1, 0], ln_shift[1, 0], attn_w[1], attn_b[1])
    hid_f32 = cross_block(hid_f32, cross_b, src_len, ln_gain[1, 1], ln_shift[1, 1], attn_w[1], attn_b[1])
    z_bf = layer_norm(hid_f32, ln_gain[1, 2], ln_shift[1, 2])
    return hid_f32, z_bf, cache_a_new, cache_b_new


def peer(index):
    return dict(device_id={'ep': index}, device_id_type=pl.DeviceIdType.MESH)


def neighbours():
    me = lax.axis_index('ep')
    core, x, y = me % 2, (me // 2) % 2, me // 4
    at = lambda yy, xx, cc: (yy * 2 + xx) * 2 + cc
    return me, core, x, y, at


def entry_barrier(others):
    barrier = pltpu.get_barrier_semaphore()
    for other in others:
        pl.semaphore_signal(barrier, inc=1, **peer(other))
    pl.semaphore_wait(barrier, len(others))


def gather_kernel(z_ref, ids_ref, zall_ref, idsall_ref, send_sem, recv_sem):
    me, core, x, y, at = neighbours()
    twin = at(y, x, 1 - core)
    chips = [(y, 1 - x), (1 - y, x), (1 - y, 1 - x)]
    entry_barrier([twin] + [at(cy, cx, core) for cy, cx in chips])

    def send(slot, src_z, src_ids, row, to):
        out = []
        for which, src, dst in ((0, src_z, zall_ref), (1, src_ids, idsall_ref)):
            cp = pltpu.make_async_remote_copy(
                src_ref=src, dst_ref=dst.at[row], send_sem=send_sem.at[slot, which], recv_sem=recv_sem.at[slot, which], **peer(to))
            cp.start()
            out.append(cp)
        return out

    sent = []
    for j in (2, 0, 1):
        sent.append((j, send(j, z_ref, ids_ref, me, at(*chips[j], core))))
    sent.append((3, send(3, z_ref, ids_ref, me, twin)))
    zall_ref[me] = z_ref[...]
    idsall_ref[me] = ids_ref[...]
    relays = []
    for j in (0, 1, 2):
        for cp in dict(sent)[j]:
            cp.wait_recv()
        row = at(*chips[j], core)
        relays += send(4 + j, zall_ref.at[row], idsall_ref.at[row], row, twin)
    for cp in dict(sent)[3]:
        cp.wait_recv()
    for cp in relays:
        cp.wait_recv()
    for _, cps in sent:
        for cp in cps:
            cp.wait_send()
    for cp in relays:
        cp.wait_send()


def gather_tokens(z_bf, ids_wide, group_n):
    tok, d_model = z_bf.shape
    return pl.pallas_call(
        gather_kernel,
        out_shape=[jax.ShapeDtypeStruct((group_n, tok, d_model), BF16), jax.ShapeDtypeStruct((group_n, tok, 128), jnp.int32)],
        in_specs=[pl.BlockSpec(memory_space=VMEM)] * 2,
        out_specs=[pl.BlockSpec(memory_space=VMEM)] * 2,
        scratch_shapes=[pltpu.SemaphoreType.DMA((7, 2)), pltpu.SemaphoreType.DMA((7, 2))],
        compiler_params=pltpu.CompilerParams(collective_id=0, has_side_effects=True),
        name='gather_tokens',
    )(z_bf, ids_wide)


def reduce_kernel(part_ref, hid_ref, out_ref, own, r1, s1, r2, s2, r3, send_sem, recv_sem):
    me, core, x, y, at = neighbours()
    twin, xn, yn = at(y, x, 1 - core), at(y, 1 - x, core), at(1 - y, x, core)
    entry_barrier([twin, xn, yn])
    half = hid_ref.shape[1] // 2
    cols = (pl.ds(0, half), pl.ds(half, half))

    def send(slot, src, dst, to):
        cp = pltpu.make_async_remote_copy(src_ref=src, dst_ref=dst, send_sem=send_sem.at[slot], recv_sem=recv_sem.at[slot], **peer(to))
        cp.start()
        return cp

    chips = [(1 - y, 1 - x), (y, 1 - x), (1 - y, x), (y, x)]
    first = [send(k, part_ref.at[at(cy, cx, 1 - core)], r1.at[k], twin) for k, (cy, cx) in enumerate(chips)]

    def sum1(k):
        first[k].wait_recv()
        cy, cx = chips[k]
        s1[k] = part_ref[at(cy, cx, core)] + r1[k]

    sum1(0)
    a0 = send(4, s1.at[0, :, cols[0]], r2.at[0, 0], xn)
    b0 = send(5, s1.at[0, :, cols[1]], r2.at[1, 0], yn)
    sum1(1)
    a1 = send(6, s1.at[1, :, cols[0]], r2.at[0, 1], xn)
    sum1(2)
    b1 = send(7, s1.at[2, :, cols[1]], r2.at[1, 1], yn)
    sum1(3)
    a0.wait_recv()
    s2[0] = s1[2, :, :half] + r2[0, 0]
    a2 = send(8, s2.at[0], r3.at[0], yn)
    b0.wait_recv()
    s2[1] = s1[1, :, half:] + r2[1, 0]
    b2 = send(9, s2.at[1], r3.at[1], xn)
    a1.wait_recv()
    own_a = hid_ref[:, :half] + s1[3, :, :half] + r2[0, 1]
    b1.wait_recv()
    own_b = hid_ref[:, half:] + s1[3, :, half:] + r2[1, 1]
    a2.wait_recv()
    out_ref[:, :half] = (own_a + r3[0]).astype(BF16)
    b2.wait_recv()
    out_ref[:, half:] = (own_b + r3[1]).astype(BF16)
    for cp in first + [a0, b0, a1, b1, a2, b2]:
        cp.wait_send()


def reduce_outputs(partial, hid_f32):
    group_n, tok, d_model = partial.shape
    half = d_model // 2
    return pl.pallas_call(
        reduce_kernel,
        out_shape=jax.ShapeDtypeStruct((tok, d_model), BF16),
        in_specs=[pl.BlockSpec(memory_space=VMEM)] * 2,
        out_specs=pl.BlockSpec(memory_space=VMEM),
        scratch_shapes=[
            VMEM((8, 128), F32),
            VMEM((4, tok, d_model), F32), VMEM((4, tok, d_model), F32),
            VMEM((2, 2, tok, half), F32), VMEM((2, tok, half), F32), VMEM((2, tok, half), F32),
            pltpu.SemaphoreType.DMA((10,)), pltpu.SemaphoreType.DMA((10,)),
        ],
        compiler_params=pltpu.CompilerParams(collective_id=1, has_side_effects=True),
        name='reduce_outputs',
    )(partial, hid_f32)


ROWS = 128
SPLIT = 2
SLOTS = 6


def expert_kernel(z_ref, ids_ref, rw_ref, b1_ref, b2_ref, w1_hbm, w2_hbm, out_ref,
                  w1_buf, w2_buf, rank_s, gate_s, cnt_v, cnt_s, list_s, x_s, o_s, sem1, sem2, csem):
    n_tok, d_model = z_ref.shape
    n_loc = w1_hbm.shape[0]
    ff = w1_hbm.shape[2]
    fc = ff // SPLIT
    n_blk = x_s.shape[0]
    me = lax.axis_index('ep')
    base = me * n_loc
    lane = lax.broadcasted_iota(jnp.int32, (n_tok, 128), 1)
    id0, id1 = ids_ref[:, 0:1], ids_ref[:, 1:2]
    hit_loc = jnp.logical_or(id0 - base == lane, id1 - base == lane)
    hit_loc = jnp.logical_and(hit_loc, lane < n_loc)
    hit_t = hit_loc.astype(F32)
    counts = jnp.sum(hit_t, axis=0, keepdims=True)
    cnt_v[...] = jnp.broadcast_to(counts, cnt_v.shape).astype(jnp.int32)
    cp = pltpu.make_async_copy(cnt_v, cnt_s, csem)
    cp.start()
    cp.wait()

    def scan_body(e, n_act):
        @pl.when(cnt_s[0, e] > 0)
        def _():
            list_s[n_act] = e
        return n_act + jnp.where(cnt_s[0, e] > 0, 1, 0)
    n_act = lax.fori_loop(0, n_loc, scan_body, 0)
    n_step = n_act * SPLIT

    def copies(step, slot):
        e = list_s[step // SPLIT]
        f0 = pl.multiple_of((step % SPLIT) * fc, fc)
        return (pltpu.make_async_copy(w1_hbm.at[e, :, pl.ds(f0, fc)], w1_buf.at[slot], sem1.at[slot]),
                pltpu.make_async_copy(w2_hbm.at[e, pl.ds(f0, fc), :], w2_buf.at[slot], sem2.at[slot]))

    for s in range(SLOTS):
        @pl.when(s < n_step)
        def _():
            for c in copies(s, s):
                c.start()

    hit_bf = hit_t.astype(BF16)
    row_i = lax.broadcasted_iota(jnp.int32, (n_tok, n_tok), 0)
    col_i = lax.broadcasted_iota(jnp.int32, (n_tok, n_tok), 1)
    before = (row_i < col_i).astype(BF16)
    hit = jnp.transpose(hit_t)
    rank = jnp.dot(hit.astype(BF16), before, preferred_element_type=F32)
    rank_s[...] = jnp.where(hit > 0.5, rank, -1.0)

    logits = jnp.dot(z_ref[...], rw_ref[...], preferred_element_type=F32)
    top = jnp.max(logits, axis=-1, keepdims=True)
    ex = jnp.exp(logits - top)
    probs = ex / jnp.sum(ex, axis=-1, keepdims=True)
    p0 = jnp.sum(jnp.where(lane == id0, probs, 0.0), axis=-1, keepdims=True)
    p1 = jnp.sum(jnp.where(lane == id1, probs, 0.0), axis=-1, keepdims=True)
    tot = p0 + p1
    g0, g1 = p0 / tot, p1 / tot
    gate_s[...] = jnp.where(lane == id0 - base, g0, jnp.where(lane == id1 - base, g1, 0.0))
    out_ref[...] = jnp.zeros_like(out_ref)

    def step_body(step, carry):
        slot = step % SLOTS
        e = list_s[step // SPLIT]
        part = step % SPLIT
        blocks = (cnt_s[0, e] + ROWS - 1) // ROWS
        slot_i = lax.broadcasted_iota(jnp.int32, (ROWS, n_tok), 0)

        def pick(j):
            want = (slot_i + j * ROWS).astype(F32)
            return (want == rank_s[pl.ds(e, 1), :]).astype(BF16)

        @pl.when(part == 0)
        def _():
            def gather_body(j, c):
                x_s[j] = jnp.dot(pick(j), z_ref[...], preferred_element_type=F32).astype(BF16)
                o_s[j] = jnp.broadcast_to(b2_ref[pl.ds(e, 1), :], (ROWS, d_model))
                return c
            lax.fori_loop(0, blocks, gather_body, 0)

        for c in copies(step, slot):
            c.wait()
        bias = b1_ref[pl.ds(e, 1), pl.ds(pl.multiple_of(part * fc, fc), fc)]

        def block_body(j, c):
            inner = jnp.dot(x_s[j], w1_buf[slot], preferred_element_type=F32) + bias
            inner = jnp.maximum(inner, 0.0).astype(BF16)
            o_s[j] += jnp.dot(inner, w2_buf[slot], preferred_element_type=F32)
            return c
        lax.fori_loop(0, blocks, block_body, 0)

        @pl.when(step + SLOTS < n_step)
        def _():
            for c in copies(step + SLOTS, slot):
                c.start()

        @pl.when(part == SPLIT - 1)
        def _():
            lane_g = lax.broadcasted_iota(jnp.int32, (n_tok, 128), 1)
            gate = jnp.sum(jnp.where(lane_g == e, gate_s[...], 0.0), axis=-1, keepdims=True)

            def scatter_body(j, c):
                back = lax.dot_general(pick(j), o_s[j].astype(BF16), (((0,), (0,)), ((), ())), preferred_element_type=F32)
                out_ref[...] += gate * back
                return c
            lax.fori_loop(0, blocks, scatter_body, 0)
        return carry

    lax.fori_loop(0, n_step, step_body, 0)


def run_experts(z_all, ids_all, router_w, exp_w1, exp_b1, exp_w2, exp_b2):
    n_tok, d_model = z_all.shape
    n_loc, _, ff = exp_w1.shape
    fc = ff // SPLIT
    n_blk = n_tok // ROWS
    vm = pl.BlockSpec(memory_space=VMEM)
    hbm = pl.BlockSpec(memory_space=pl.ANY)
    return pl.pallas_call(
        expert_kernel,
        out_shape=jax.ShapeDtypeStruct((n_tok, d_model), F32),
        in_specs=[vm] * 5 + [hbm] * 2,
        out_specs=vm,
        scratch_shapes=[
            VMEM((SLOTS, d_model, fc), BF16), VMEM((SLOTS, fc, d_model), BF16),
            VMEM((128, n_tok), F32), VMEM((n_tok, 128), F32),
            VMEM((8, 128), jnp.int32), pltpu.SMEM((8, 128), jnp.int32), pltpu.SMEM((n_loc,), jnp.int32),
            VMEM((n_blk, ROWS, d_model), BF16), VMEM((n_blk, ROWS, d_model), F32),
            pltpu.SemaphoreType.DMA((SLOTS,)), pltpu.SemaphoreType.DMA((SLOTS,)), pltpu.SemaphoreType.DMA,
        ],
        compiler_params=pltpu.CompilerParams(vmem_limit_bytes=60 * 1024 * 1024),
        name='run_experts',
    )(z_all, ids_all, router_w, exp_b1.astype(F32), exp_b2.astype(F32), exp_w1, exp_w2)


def solution(mesh):
    group_n = mesh.shape['ep']

    def local_step(hidden, self_pos, src_len, cache_a, cross_a, cache_b, cross_b, route_ids, ln_gain, ln_shift, attn_w, attn_b, ffn_w1, ffn_b1, ffn_w2, ffn_b2, router_w, exp_w1, exp_b1, exp_w2, exp_b2):
        hid_f32, z_bf, cache_a_new, cache_b_new = dense_layers(hidden, self_pos, src_len, cache_a, cross_a, cache_b, cross_b, ln_gain, ln_shift, attn_w, attn_b, ffn_w1, ffn_b1, ffn_w2, ffn_b2)
        tok, d_model = z_bf.shape
        ids_wide = jnp.pad(route_ids, ((0, 0), (0, 126)))
        z_all, ids_all = gather_tokens(z_bf, ids_wide, group_n)
        partial = run_experts(z_all.reshape(-1, d_model), ids_all.reshape(-1, 128), router_w, exp_w1, exp_b1, exp_w2, exp_b2)
        out = reduce_outputs(partial.reshape(group_n, tok, d_model), hid_f32)
        return out, cache_a_new, cache_b_new

    tok_spec = P(('dp', 'ep'))
    cache_spec = P(None, ('dp', 'ep'))
    rep_spec = P()
    exp_spec = P('ep')
    in_specs = (tok_spec, tok_spec, tok_spec, cache_spec, cache_spec, cache_spec, cache_spec, tok_spec) + (rep_spec,) * 9 + (exp_spec,) * 4
    out_specs = (tok_spec, cache_spec, cache_spec)
    return jax.shard_map(local_step, mesh=mesh, in_specs=in_specs, out_specs=out_specs, check_vma=False)
```

```python
import functools

import jax
import jax.numpy as jnp
from jax import lax
from jax.experimental import pallas as pl
from jax.experimental.pallas import tpu as pltpu
from jax.sharding import PartitionSpec as P

LN_EPS = 1e-5
F32 = jnp.float32
BF16 = jnp.bfloat16
VMEM = pltpu.VMEM


GROUP = 4
SELF_GROUP = 8
HEAD_PAD = 16


def norm_rows(x_val, gain_vec, shift_vec):
    mean_val = jnp.mean(x_val, axis=-1, keepdims=True)
    centered = x_val - mean_val
    var_val = jnp.mean(centered * centered, axis=-1, keepdims=True)
    return (centered * lax.rsqrt(var_val + LN_EPS) * gain_vec + shift_vec).astype(BF16)


def dense_kernel(pos_sm, len_sm, hid_ref, gain_ref, shift_ref, ab_ref, fb1_ref, fb2_ref,
                 cache_a, cross_a, cache_b, cross_b, aw_hbm, w1_hbm, w2_hbm,
                 hid_out, z_out, cache_a_out, cache_b_out,
                 w_buf, f1_buf, f2_buf, self_buf, cross_buf, q_s, k_s, v_s, ctx_s, cat_s, self_mask, cross_mask,
                 w_sem, f_sem, in_sem, out_sem, cross_sem):
    tok, d_model = hid_ref.shape
    n_heads, self_len, head_dim = self_buf.shape[2:]
    src = cross_buf.shape[3]
    ff = f1_buf.shape[1]
    scale = head_dim ** -0.5
    n_self = tok // SELF_GROUP

    def weight_copy(i):
        return pltpu.make_async_copy(aw_hbm.at[i // 6, i % 6], w_buf.at[i], w_sem.at[i])

    def ffn_copies():
        return (pltpu.make_async_copy(w1_hbm, f1_buf, f_sem.at[0]), pltpu.make_async_copy(w2_hbm, f2_buf, f_sem.at[1]))

    def self_in(cache, g):
        rows = pl.ds(g * SELF_GROUP, SELF_GROUP)
        return pltpu.make_async_copy(cache.at[:, rows], self_buf.at[:, rows], in_sem.at[g])

    def self_out(cache_out, g):
        rows = pl.ds(g * SELF_GROUP, SELF_GROUP)
        return pltpu.make_async_copy(self_buf.at[:, rows], cache_out.at[:, rows], out_sem.at[g])

    def cross_rows(b):
        return pl.multiple_of(((len_sm[b] + 15) // 16) * 16, 16)

    def cross_copy(cross, b):
        rows = pl.ds(0, cross_rows(b))
        return pltpu.make_async_copy(cross.at[:, b, :, rows, :], cross_buf.at[b, :, :, rows, :], cross_sem.at[b])

    for i in range(3):
        weight_copy(i).start()
    for g in range(n_self):
        self_in(cache_a, g).start()
    weight_copy(3).start()
    weight_copy(4).start()

    def first_cross(b, c):
        cross_copy(cross_a, b).start()
        return c
    lax.fori_loop(0, tok, first_cross, 0)
    weight_copy(5).start()
    for cp in ffn_copies():
        cp.start()
    for i in range(6, 12):
        weight_copy(i).start()

    def zero_tail(b, c):
        for part in range(1, src // 16):
            @pl.when(part * 16 >= cross_rows(b))
            def _():
                cross_buf[b, 1, :, part * 16:(part + 1) * 16, :] = jnp.zeros((n_heads, 16, head_dim), BF16)
        return c
    lax.fori_loop(0, tok, zero_tail, 0)

    def build_mask(ref, length):
        row = lax.broadcasted_iota(jnp.int32, ref.shape, 0)
        lane = lax.broadcasted_iota(jnp.int32, ref.shape, 1)
        ref[...] = jnp.where(lane // length == row, lane % length, 1 << 20)
    build_mask(self_mask, self_len)
    build_mask(cross_mask, src)

    def to_heads(ref, val):
        val = val.astype(BF16).astype(F32)
        for h in range(n_heads):
            ref[pl.ds(h, tok, stride=HEAD_PAD), :] = val[:, h * head_dim:(h + 1) * head_dim]

    def from_heads(ref):
        for h in range(0, n_heads, 2):
            two = [ref[pl.ds(h + k, tok, stride=HEAD_PAD), :] for k in range(2)]
            cat_s[:, h * head_dim:(h + 2) * head_dim] = jnp.concatenate(two, axis=1).astype(BF16)
        return cat_s[...]

    def softmax_rows(scores, mask_ref, limit):
        scores = jnp.where(mask_ref[...] < limit, scores * scale, -1e30)
        top = jnp.max(scores, axis=-1, keepdims=True)
        ex = jnp.exp(scores - top)
        return (ex * (1.0 / jnp.sum(ex, axis=-1, keepdims=True))).astype(BF16)

    def attend(q, keys, vals, mask_ref, limit):
        scores = lax.dot_general(q, keys, (((1,), (1,)), ((), ())), preferred_element_type=F32)
        probs = softmax_rows(scores, mask_ref, limit)
        return jnp.dot(probs, vals, preferred_element_type=F32)

    def proj(layer, i, x_bf):
        weight_copy(layer * 6 + i).wait()
        bias = ab_ref[layer, i:i + 1, :].astype(F32)
        return jnp.dot(x_bf, w_buf[layer * 6 + i], preferred_element_type=F32) + bias

    def self_layer(layer, h, cache, cache_out):
        x = norm_rows(h, gain_ref[0, layer:layer + 1, :], shift_ref[0, layer:layer + 1, :])
        to_heads(q_s, proj(layer, 0, x))
        to_heads(k_s, proj(layer, 1, x))
        to_heads(v_s, proj(layer, 2, x))
        row_i = lax.broadcasted_iota(jnp.int32, (self_len, head_dim), 0)

        def body(g, c):
            self_in(cache, g).wait()
            for u in range(SELF_GROUP):
                b = g * SELF_GROUP + u
                hit = row_i == pos_sm[b]
                kv = []
                for which, new in ((0, k_s), (1, v_s)):
                    tiles = []
                    for hd in range(n_heads):
                        row = new[pl.ds(b * HEAD_PAD + hd, self_len, stride=0), :]
                        tile = jnp.where(hit, row, self_buf[which, b, hd].astype(F32)).astype(BF16)
                        self_buf[which, b, hd] = tile
                        tiles.append(tile)
                    kv.append(jnp.concatenate(tiles, axis=0))
                q = q_s[pl.ds(pl.multiple_of(b * HEAD_PAD, HEAD_PAD), HEAD_PAD), :].astype(BF16)
                ctx_s[pl.ds(pl.multiple_of(b * HEAD_PAD, HEAD_PAD), HEAD_PAD), :] = attend(q, kv[0], kv[1], self_mask, pos_sm[b] + 1)
            self_out(cache_out, g).start()
            return c
        lax.fori_loop(0, n_self, body, 0)
        ctx = from_heads(ctx_s)
        return h + proj(layer, 3, ctx)

    def cross_layer(layer, h, cross, after):
        x = norm_rows(h, gain_ref[1, layer:layer + 1, :], shift_ref[1, layer:layer + 1, :])
        to_heads(q_s, proj(layer, 4, x))

        def body(g, c):
            for u in range(GROUP):
                cross_copy(cross, g * GROUP + u).wait()
            for u in range(GROUP):
                b = g * GROUP + u
                rows = pl.ds(pl.multiple_of(b * HEAD_PAD, HEAD_PAD), HEAD_PAD)
                q = q_s[rows, :].astype(BF16)
                keys = cross_buf[b, 0].reshape(n_heads * src, head_dim)
                vals = cross_buf[b, 1].reshape(n_heads * src, head_dim)
                ctx_s[rows, :] = attend(q, keys, vals, cross_mask, len_sm[b])
            if after is not None:
                for u in range(GROUP):
                    cross_copy(after, g * GROUP + u).start()
            return c
        lax.fori_loop(0, tok // GROUP, body, 0)
        ctx = from_heads(ctx_s)
        return h + proj(layer, 5, ctx)

    q_s[...] = jnp.zeros_like(q_s)
    h = hid_ref[...].astype(F32)
    h = self_layer(0, h, cache_a, cache_a_out)
    for g in range(n_self):
        self_out(cache_a_out, g).wait()
        self_in(cache_b, g).start()
    h = cross_layer(0, h, cross_a, cross_b)
    x = norm_rows(h, gain_ref[2, 0:1, :], shift_ref[2, 0:1, :])
    for cp in ffn_copies():
        cp.wait()
    acc = h + fb2_ref[...].astype(F32)
    for f in range(0, ff, d_model):
        inner = jnp.dot(x, f1_buf[:, f:f + d_model], preferred_element_type=F32) + fb1_ref[:, f:f + d_model].astype(F32)
        inner = jnp.maximum(inner, 0.0).astype(BF16)
        acc = acc + jnp.dot(inner, f2_buf[f:f + d_model, :], preferred_element_type=F32)
    h = acc
    h = self_layer(1, h, cache_b, cache_b_out)
    h = cross_layer(1, h, cross_b, None)
    hid_out[...] = h
    z_out[...] = norm_rows(h, gain_ref[2, 1:2, :], shift_ref[2, 1:2, :])
    for g in range(n_self):
        self_out(cache_b_out, g).wait()


def dense_layers(hidden, self_pos, src_len, cache_a, cross_a, cache_b, cross_b, ln_gain, ln_shift, attn_w, attn_b, ffn_w1, ffn_b1, ffn_w2, ffn_b2):
    tok, d_model = hidden.shape
    n_heads, head_dim = cache_a.shape[3:]
    self_len, src = cache_a.shape[2], cross_a.shape[2]
    ff = ffn_w1.shape[1]
    swap = lambda arr: jnp.swapaxes(arr, 2, 3)
    sm = pl.BlockSpec(memory_space=pltpu.SMEM)
    vm = pl.BlockSpec(memory_space=VMEM)
    hbm = pl.BlockSpec(memory_space=pl.ANY)
    cache_t = jax.ShapeDtypeStruct((2, tok, n_heads, self_len, head_dim), BF16)
    n_self = tok // SELF_GROUP
    heads = VMEM((tok * HEAD_PAD, head_dim), F32)
    hid, z, out_a, out_b = pl.pallas_call(
        dense_kernel,
        out_shape=[jax.ShapeDtypeStruct((tok, d_model), F32), jax.ShapeDtypeStruct((tok, d_model), BF16), cache_t, cache_t],
        in_specs=[sm] * 2 + [vm] * 6 + [hbm] * 7,
        out_specs=[vm] * 2 + [hbm] * 2,
        scratch_shapes=[
            VMEM((12, d_model, d_model), BF16), VMEM((d_model, ff), BF16), VMEM((ff, d_model), BF16),
            VMEM((2, tok, n_heads, self_len, head_dim), BF16), VMEM((tok, 2, n_heads, src, head_dim), BF16),
            heads, heads, heads, heads, VMEM((tok, d_model), BF16),
            VMEM((HEAD_PAD, n_heads * self_len), jnp.int32), VMEM((HEAD_PAD, n_heads * src), jnp.int32),
            pltpu.SemaphoreType.DMA((12,)), pltpu.SemaphoreType.DMA((2,)), pltpu.SemaphoreType.DMA((n_self,)),
            pltpu.SemaphoreType.DMA((n_self,)), pltpu.SemaphoreType.DMA((tok,)),
        ],
        compiler_params=pltpu.CompilerParams(vmem_limit_bytes=62 * 1024 * 1024),
        name='dense_layers',
    )(self_pos, src_len, hidden, jnp.swapaxes(ln_gain, 0, 1), jnp.swapaxes(ln_shift, 0, 1), attn_b, ffn_b1.reshape(1, -1), ffn_b2.reshape(1, -1),
      swap(cache_a), swap(cross_a), swap(cache_b), swap(cross_b), attn_w, ffn_w1, ffn_w2)
    return hid, z, swap(out_a), swap(out_b)


def peer(index):
    return dict(device_id={'ep': index}, device_id_type=pl.DeviceIdType.MESH)


def neighbours():
    me = lax.axis_index('ep')
    core, x, y = me % 2, (me // 2) % 2, me // 4
    at = lambda yy, xx, cc: (yy * 2 + xx) * 2 + cc
    return me, core, x, y, at


def entry_barrier(others):
    barrier = pltpu.get_barrier_semaphore()
    for other in others:
        pl.semaphore_signal(barrier, inc=1, **peer(other))
    pl.semaphore_wait(barrier, len(others))


def gather_kernel(z_ref, ids_ref, zall_ref, idsall_ref, send_sem, recv_sem):
    me, core, x, y, at = neighbours()
    twin = at(y, x, 1 - core)
    chips = [(y, 1 - x), (1 - y, x), (1 - y, 1 - x)]
    entry_barrier([twin] + [at(cy, cx, core) for cy, cx in chips])

    def send(slot, src_z, src_ids, row, to):
        out = []
        for which, src, dst in ((0, src_z, zall_ref), (1, src_ids, idsall_ref)):
            cp = pltpu.make_async_remote_copy(
                src_ref=src, dst_ref=dst.at[row], send_sem=send_sem.at[slot, which], recv_sem=recv_sem.at[slot, which], **peer(to))
            cp.start()
            out.append(cp)
        return out

    sent = []
    for j in (2, 0, 1):
        sent.append((j, send(j, z_ref, ids_ref, me, at(*chips[j], core))))
    sent.append((3, send(3, z_ref, ids_ref, me, twin)))
    zall_ref[me] = z_ref[...]
    idsall_ref[me] = ids_ref[...]
    relays = []
    for j in (0, 1, 2):
        for cp in dict(sent)[j]:
            cp.wait_recv()
        row = at(*chips[j], core)
        relays += send(4 + j, zall_ref.at[row], idsall_ref.at[row], row, twin)
    for cp in dict(sent)[3]:
        cp.wait_recv()
    for cp in relays:
        cp.wait_recv()
    for _, cps in sent:
        for cp in cps:
            cp.wait_send()
    for cp in relays:
        cp.wait_send()


def gather_tokens(z_bf, ids_wide, group_n):
    tok, d_model = z_bf.shape
    return pl.pallas_call(
        gather_kernel,
        out_shape=[jax.ShapeDtypeStruct((group_n, tok, d_model), BF16), jax.ShapeDtypeStruct((group_n, tok, 128), jnp.int32)],
        in_specs=[pl.BlockSpec(memory_space=VMEM)] * 2,
        out_specs=[pl.BlockSpec(memory_space=VMEM)] * 2,
        scratch_shapes=[pltpu.SemaphoreType.DMA((7, 2)), pltpu.SemaphoreType.DMA((7, 2))],
        compiler_params=pltpu.CompilerParams(collective_id=0, has_side_effects=True),
        name='gather_tokens',
    )(z_bf, ids_wide)


def reduce_kernel(part_ref, hid_ref, out_ref, own, r1, s1, r2, s2, r3, send_sem, recv_sem):
    me, core, x, y, at = neighbours()
    twin, xn, yn = at(y, x, 1 - core), at(y, 1 - x, core), at(1 - y, x, core)
    entry_barrier([twin, xn, yn])
    half = hid_ref.shape[1] // 2
    cols = (pl.ds(0, half), pl.ds(half, half))

    def send(slot, src, dst, to):
        cp = pltpu.make_async_remote_copy(src_ref=src, dst_ref=dst, send_sem=send_sem.at[slot], recv_sem=recv_sem.at[slot], **peer(to))
        cp.start()
        return cp

    chips = [(1 - y, 1 - x), (y, 1 - x), (1 - y, x), (y, x)]
    first = [send(k, part_ref.at[at(cy, cx, 1 - core)], r1.at[k], twin) for k, (cy, cx) in enumerate(chips)]

    def sum1(k):
        first[k].wait_recv()
        cy, cx = chips[k]
        s1[k] = part_ref[at(cy, cx, core)] + r1[k]

    sum1(0)
    a0 = send(4, s1.at[0, :, cols[0]], r2.at[0, 0], xn)
    b0 = send(5, s1.at[0, :, cols[1]], r2.at[1, 0], yn)
    sum1(1)
    a1 = send(6, s1.at[1, :, cols[0]], r2.at[0, 1], xn)
    sum1(2)
    b1 = send(7, s1.at[2, :, cols[1]], r2.at[1, 1], yn)
    sum1(3)
    a0.wait_recv()
    s2[0] = s1[2, :, :half] + r2[0, 0]
    a2 = send(8, s2.at[0], r3.at[0], yn)
    b0.wait_recv()
    s2[1] = s1[1, :, half:] + r2[1, 0]
    b2 = send(9, s2.at[1], r3.at[1], xn)
    a1.wait_recv()
    own_a = hid_ref[:, :half] + s1[3, :, :half] + r2[0, 1]
    b1.wait_recv()
    own_b = hid_ref[:, half:] + s1[3, :, half:] + r2[1, 1]
    a2.wait_recv()
    out_ref[:, :half] = (own_a + r3[0]).astype(BF16)
    b2.wait_recv()
    out_ref[:, half:] = (own_b + r3[1]).astype(BF16)
    for cp in first + [a0, b0, a1, b1, a2, b2]:
        cp.wait_send()


def reduce_outputs(partial, hid_f32):
    group_n, tok, d_model = partial.shape
    half = d_model // 2
    return pl.pallas_call(
        reduce_kernel,
        out_shape=jax.ShapeDtypeStruct((tok, d_model), BF16),
        in_specs=[pl.BlockSpec(memory_space=VMEM)] * 2,
        out_specs=pl.BlockSpec(memory_space=VMEM),
        scratch_shapes=[
            VMEM((8, 128), F32),
            VMEM((4, tok, d_model), F32), VMEM((4, tok, d_model), F32),
            VMEM((2, 2, tok, half), F32), VMEM((2, tok, half), F32), VMEM((2, tok, half), F32),
            pltpu.SemaphoreType.DMA((10,)), pltpu.SemaphoreType.DMA((10,)),
        ],
        compiler_params=pltpu.CompilerParams(collective_id=1, has_side_effects=True),
        name='reduce_outputs',
    )(partial, hid_f32)


ROWS = 128
SPLIT = 2
SLOTS = 6


def expert_kernel(z_ref, ids_ref, rw_ref, b1_ref, b2_ref, w1_hbm, w2_hbm, out_ref,
                  w1_buf, w2_buf, rank_s, gate_s, cnt_v, cnt_s, list_s, x_s, o_s, sem1, sem2, csem):
    n_tok, d_model = z_ref.shape
    n_loc = w1_hbm.shape[0]
    ff = w1_hbm.shape[2]
    fc = ff // SPLIT
    n_blk = x_s.shape[0]
    me = lax.axis_index('ep')
    base = me * n_loc
    lane = lax.broadcasted_iota(jnp.int32, (n_tok, 128), 1)
    id0, id1 = ids_ref[:, 0:1], ids_ref[:, 1:2]
    hit_loc = jnp.logical_or(id0 - base == lane, id1 - base == lane)
    hit_loc = jnp.logical_and(hit_loc, lane < n_loc)
    hit_t = hit_loc.astype(F32)
    counts = jnp.sum(hit_t, axis=0, keepdims=True)
    cnt_v[...] = jnp.broadcast_to(counts, cnt_v.shape).astype(jnp.int32)
    cp = pltpu.make_async_copy(cnt_v, cnt_s, csem)
    cp.start()
    cp.wait()

    def scan_body(e, n_act):
        @pl.when(cnt_s[0, e] > 0)
        def _():
            list_s[n_act] = e
        return n_act + jnp.where(cnt_s[0, e] > 0, 1, 0)
    n_act = lax.fori_loop(0, n_loc, scan_body, 0)
    n_step = n_act * SPLIT

    def copies(step, slot):
        e = list_s[step // SPLIT]
        f0 = pl.multiple_of((step % SPLIT) * fc, fc)
        return (pltpu.make_async_copy(w1_hbm.at[e, :, pl.ds(f0, fc)], w1_buf.at[slot], sem1.at[slot]),
                pltpu.make_async_copy(w2_hbm.at[e, pl.ds(f0, fc), :], w2_buf.at[slot], sem2.at[slot]))

    for s in range(SLOTS):
        @pl.when(s < n_step)
        def _():
            for c in copies(s, s):
                c.start()

    hit_bf = hit_t.astype(BF16)
    row_i = lax.broadcasted_iota(jnp.int32, (n_tok, n_tok), 0)
    col_i = lax.broadcasted_iota(jnp.int32, (n_tok, n_tok), 1)
    before = (row_i < col_i).astype(BF16)
    hit = jnp.transpose(hit_t)
    rank = jnp.dot(hit.astype(BF16), before, preferred_element_type=F32)
    rank_s[...] = jnp.where(hit > 0.5, rank, -1.0)

    logits = jnp.dot(z_ref[...], rw_ref[...], preferred_element_type=F32)
    top = jnp.max(logits, axis=-1, keepdims=True)
    ex = jnp.exp(logits - top)
    probs = ex / jnp.sum(ex, axis=-1, keepdims=True)
    p0 = jnp.sum(jnp.where(lane == id0, probs, 0.0), axis=-1, keepdims=True)
    p1 = jnp.sum(jnp.where(lane == id1, probs, 0.0), axis=-1, keepdims=True)
    tot = p0 + p1
    g0, g1 = p0 / tot, p1 / tot
    gate_s[...] = jnp.where(lane == id0 - base, g0, jnp.where(lane == id1 - base, g1, 0.0))
    out_ref[...] = jnp.zeros_like(out_ref)

    def step_body(step, carry):
        slot = step % SLOTS
        e = list_s[step // SPLIT]
        part = step % SPLIT
        blocks = (cnt_s[0, e] + ROWS - 1) // ROWS
        slot_i = lax.broadcasted_iota(jnp.int32, (ROWS, n_tok), 0)

        def pick(j):
            want = (slot_i + j * ROWS).astype(F32)
            return (want == rank_s[pl.ds(e, 1), :]).astype(BF16)

        @pl.when(part == 0)
        def _():
            def gather_body(j, c):
                x_s[j] = jnp.dot(pick(j), z_ref[...], preferred_element_type=F32).astype(BF16)
                o_s[j] = jnp.broadcast_to(b2_ref[pl.ds(e, 1), :], (ROWS, d_model))
                return c
            lax.fori_loop(0, blocks, gather_body, 0)

        for c in copies(step, slot):
            c.wait()
        bias = b1_ref[pl.ds(e, 1), pl.ds(pl.multiple_of(part * fc, fc), fc)]

        def block_body(j, c):
            inner = jnp.dot(x_s[j], w1_buf[slot], preferred_element_type=F32) + bias
            inner = jnp.maximum(inner, 0.0).astype(BF16)
            o_s[j] += jnp.dot(inner, w2_buf[slot], preferred_element_type=F32)
            return c
        lax.fori_loop(0, blocks, block_body, 0)

        @pl.when(step + SLOTS < n_step)
        def _():
            for c in copies(step + SLOTS, slot):
                c.start()

        @pl.when(part == SPLIT - 1)
        def _():
            lane_g = lax.broadcasted_iota(jnp.int32, (n_tok, 128), 1)
            gate = jnp.sum(jnp.where(lane_g == e, gate_s[...], 0.0), axis=-1, keepdims=True)

            def scatter_body(j, c):
                back = lax.dot_general(pick(j), o_s[j].astype(BF16), (((0,), (0,)), ((), ())), preferred_element_type=F32)
                out_ref[...] += gate * back
                return c
            lax.fori_loop(0, blocks, scatter_body, 0)
        return carry

    lax.fori_loop(0, n_step, step_body, 0)


def run_experts(z_all, ids_all, router_w, exp_w1, exp_b1, exp_w2, exp_b2):
    n_tok, d_model = z_all.shape
    n_loc, _, ff = exp_w1.shape
    fc = ff // SPLIT
    n_blk = n_tok // ROWS
    vm = pl.BlockSpec(memory_space=VMEM)
    hbm = pl.BlockSpec(memory_space=pl.ANY)
    return pl.pallas_call(
        expert_kernel,
        out_shape=jax.ShapeDtypeStruct((n_tok, d_model), F32),
        in_specs=[vm] * 5 + [hbm] * 2,
        out_specs=vm,
        scratch_shapes=[
            VMEM((SLOTS, d_model, fc), BF16), VMEM((SLOTS, fc, d_model), BF16),
            VMEM((128, n_tok), F32), VMEM((n_tok, 128), F32),
            VMEM((8, 128), jnp.int32), pltpu.SMEM((8, 128), jnp.int32), pltpu.SMEM((n_loc,), jnp.int32),
            VMEM((n_blk, ROWS, d_model), BF16), VMEM((n_blk, ROWS, d_model), F32),
            pltpu.SemaphoreType.DMA((SLOTS,)), pltpu.SemaphoreType.DMA((SLOTS,)), pltpu.SemaphoreType.DMA,
        ],
        compiler_params=pltpu.CompilerParams(vmem_limit_bytes=60 * 1024 * 1024),
        name='run_experts',
    )(z_all, ids_all, router_w, exp_b1.astype(F32), exp_b2.astype(F32), exp_w1, exp_w2)


def solution(mesh):
    group_n = mesh.shape['ep']

    def local_step(hidden, self_pos, src_len, cache_a, cross_a, cache_b, cross_b, route_ids, ln_gain, ln_shift, attn_w, attn_b, ffn_w1, ffn_b1, ffn_w2, ffn_b2, router_w, exp_w1, exp_b1, exp_w2, exp_b2):
        hid_f32, z_bf, cache_a_new, cache_b_new = dense_layers(hidden, self_pos, src_len, cache_a, cross_a, cache_b, cross_b, ln_gain, ln_shift, attn_w, attn_b, ffn_w1, ffn_b1, ffn_w2, ffn_b2)
        tok, d_model = z_bf.shape
        ids_wide = jnp.pad(route_ids, ((0, 0), (0, 126)))
        z_all, ids_all = gather_tokens(z_bf, ids_wide, group_n)
        partial = run_experts(z_all.reshape(-1, d_model), ids_all.reshape(-1, 128), router_w, exp_w1, exp_b1, exp_w2, exp_b2)
        out = reduce_outputs(partial.reshape(group_n, tok, d_model), hid_f32)
        return out, cache_a_new, cache_b_new

    tok_spec = P(('dp', 'ep'))
    cache_spec = P(None, ('dp', 'ep'))
    rep_spec = P()
    exp_spec = P('ep')
    in_specs = (tok_spec, tok_spec, tok_spec, cache_spec, cache_spec, cache_spec, cache_spec, tok_spec) + (rep_spec,) * 9 + (exp_spec,) * 4
    out_specs = (tok_spec, cache_spec, cache_spec)
    return jax.shard_map(local_step, mesh=mesh, in_specs=in_specs, out_specs=out_specs, check_vma=False)
```

```python
import functools

import jax
import jax.numpy as jnp
from jax import lax
from jax.experimental import pallas as pl
from jax.experimental.pallas import tpu as pltpu
from jax.sharding import PartitionSpec as P

LN_EPS = 1e-5
F32 = jnp.float32
BF16 = jnp.bfloat16
VMEM = pltpu.VMEM


GROUP = 4
SELF_GROUP = 8
HEAD_PAD = 16


def norm_rows(x_val, gain_vec, shift_vec):
    mean_val = jnp.mean(x_val, axis=-1, keepdims=True)
    centered = x_val - mean_val
    var_val = jnp.mean(centered * centered, axis=-1, keepdims=True)
    return (centered * lax.rsqrt(var_val + LN_EPS) * gain_vec + shift_vec).astype(BF16)


def dense_kernel(pos_sm, len_sm, pos_ref, hid_ref, gain_ref, shift_ref, ab_ref, fb1_ref, fb2_ref,
                 cache_a, cross_a, cache_b, cross_b, aw_hbm, w1_hbm, w2_hbm,
                 hid_out, z_out, cache_a_out, cache_b_out,
                 w_buf, f1_buf, f2_buf, self_buf, cross_buf, q_s, k_s, v_s, ctx_s, cat_s, lim_s, self_mask, cross_mask,
                 w_sem, f_sem, in_sem, out_sem, cross_sem):
    tok, d_model = hid_ref.shape
    n_heads, self_len, head_dim = self_buf.shape[2:]
    src = cross_buf.shape[3]
    ff = f1_buf.shape[1]
    scale = head_dim ** -0.5
    n_self = tok // SELF_GROUP

    def weight_copy(i):
        return pltpu.make_async_copy(aw_hbm.at[i // 6, i % 6], w_buf.at[i], w_sem.at[i])

    def ffn_copies():
        return (pltpu.make_async_copy(w1_hbm, f1_buf, f_sem.at[0]), pltpu.make_async_copy(w2_hbm, f2_buf, f_sem.at[1]))

    def self_in(cache, g):
        rows = pl.ds(g * SELF_GROUP, SELF_GROUP)
        return pltpu.make_async_copy(cache.at[:, rows], self_buf.at[:, rows], in_sem.at[g])

    def self_out(cache_out, g):
        rows = pl.ds(g * SELF_GROUP, SELF_GROUP)
        return pltpu.make_async_copy(self_buf.at[:, rows], cache_out.at[:, rows], out_sem.at[g])

    def cross_rows(b):
        return pl.multiple_of(((len_sm[b] + 15) // 16) * 16, 16)

    def cross_copy(cross, b):
        rows = pl.ds(0, cross_rows(b))
        return pltpu.make_async_copy(cross.at[:, b, :, rows, :], cross_buf.at[b, :, :, rows, :], cross_sem.at[b])

    for i in range(3):
        weight_copy(i).start()
    for g in range(n_self):
        self_in(cache_a, g).start()
    weight_copy(3).start()
    weight_copy(4).start()

    def first_cross(b, c):
        cross_copy(cross_a, b).start()
        return c
    lax.fori_loop(0, tok, first_cross, 0)
    weight_copy(5).start()
    for cp in ffn_copies():
        cp.start()
    for i in range(6, 12):
        weight_copy(i).start()

    def zero_tail(b, c):
        def zero_part(part, c2):
            cross_buf[b, 1, :, pl.ds(pl.multiple_of(part * 16, 16), 16), :] = jnp.zeros((n_heads, 16, head_dim), BF16)
            return c2
        return lax.fori_loop(cross_rows(b) // 16, src // 16, zero_part, c)
    lax.fori_loop(0, tok, zero_tail, 0)

    def build_mask(ref, length):
        row = lax.broadcasted_iota(jnp.int32, ref.shape, 0)
        lane = lax.broadcasted_iota(jnp.int32, ref.shape, 1)
        seq, head = lane // (n_heads * length), (lane // length) % n_heads
        ref[...] = jnp.where(seq * HEAD_PAD + head == row, lane % length, 1 << 20)
    build_mask(self_mask, self_len)
    build_mask(cross_mask, src)
    limit_col = jnp.broadcast_to(pos_ref[...] + 1, (tok, 128))
    for hd in range(HEAD_PAD):
        lim_s[pl.ds(hd, tok, stride=HEAD_PAD), :] = limit_col

    def to_heads(ref, val):
        val = val.astype(BF16).astype(F32)
        for h in range(n_heads):
            ref[pl.ds(h, tok, stride=HEAD_PAD), :] = val[:, h * head_dim:(h + 1) * head_dim]

    def from_heads(ref):
        for h in range(0, n_heads, 2):
            two = [ref[pl.ds(h + k, tok, stride=HEAD_PAD), :] for k in range(2)]
            cat_s[:, h * head_dim:(h + 2) * head_dim] = jnp.concatenate(two, axis=1).astype(BF16)
        return cat_s[...]

    def softmax_rows(scores, mask, limit):
        scores = jnp.where(mask < limit, scores * scale, -1e30)
        top = jnp.max(scores, axis=-1, keepdims=True)
        ex = jnp.exp(scores - top)
        return (ex * (1.0 / jnp.sum(ex, axis=-1, keepdims=True))).astype(BF16)

    def scores_of(q, keys):
        return lax.dot_general(q, keys, (((1,), (1,)), ((), ())), preferred_element_type=F32)

    def block_diag(blocks):
        rows = []
        for k, blk in enumerate(blocks):
            pad = jnp.zeros_like(blk)
            rows.append(jnp.concatenate([blk if j == k else pad for j in range(len(blocks))], axis=1))
        return jnp.concatenate(rows, axis=0)

    def head_rows(b, n):
        return pl.ds(pl.multiple_of(b * HEAD_PAD, HEAD_PAD), n * HEAD_PAD)

    def proj(layer, i, x_bf):
        weight_copy(layer * 6 + i).wait()
        bias = ab_ref[i].astype(F32)[layer:layer + 1, :]
        return jnp.dot(x_bf, w_buf[layer * 6 + i], preferred_element_type=F32) + bias

    def self_layer(layer, h, cache, cache_out):
        x = norm_rows(h, gain_ref[0, layer:layer + 1, :], shift_ref[0, layer:layer + 1, :])
        to_heads(q_s, proj(layer, 0, x))
        to_heads(k_s, proj(layer, 1, x))
        to_heads(v_s, proj(layer, 2, x))
        row_i = lax.broadcasted_iota(jnp.int32, (self_len, head_dim), 0)

        def body(g, c):
            self_in(cache, g).wait()
            sides = []
            for which, new in ((0, k_s), (1, v_s)):
                tiles = []
                for u in range(SELF_GROUP):
                    b = g * SELF_GROUP + u
                    hit = row_i == pos_sm[b]
                    for hd in range(n_heads):
                        row = new[pl.ds(b * HEAD_PAD + hd, self_len, stride=0), :]
                        tile = jnp.where(hit, row, self_buf[which, b, hd].astype(F32)).astype(BF16)
                        self_buf[which, b, hd] = tile
                        tiles.append(tile)
                sides.append(jnp.concatenate(tiles, axis=0))
                if which == 0:
                    q = q_s[head_rows(g * SELF_GROUP, SELF_GROUP), :].astype(BF16)
                    scores = scores_of(q, sides[0])
            two = 2 * n_heads * self_len
            blocks = []
            for p in range(SELF_GROUP // 2):
                lim = lim_s[head_rows(g * SELF_GROUP + 2 * p, 2), :]
                lim = jnp.concatenate([lim] * (two // 128), axis=1)
                blocks.append(softmax_rows(scores[p * 2 * HEAD_PAD:(p + 1) * 2 * HEAD_PAD, p * two:(p + 1) * two], self_mask[...], lim))
            ctx_s[head_rows(g * SELF_GROUP, SELF_GROUP), :] = jnp.dot(block_diag(blocks), sides[1], preferred_element_type=F32)
            self_out(cache_out, g).start()
            return c
        lax.fori_loop(0, n_self, body, 0)
        ctx = from_heads(ctx_s)
        return h + proj(layer, 3, ctx)

    def cross_layer(layer, h, cross, after):
        x = norm_rows(h, gain_ref[1, layer:layer + 1, :], shift_ref[1, layer:layer + 1, :])
        to_heads(q_s, proj(layer, 4, x))

        def body(g, c):
            first = g * (2 * GROUP)
            for u in range(2 * GROUP):
                cross_copy(cross, first + u).wait()
            halves = [first, first + GROUP]
            scores = []
            for at in halves:
                q = q_s[head_rows(at, GROUP), :].astype(BF16)
                scores.append(scores_of(q, cross_buf[pl.ds(at, GROUP), 0].reshape(GROUP * n_heads * src, head_dim)))
            wide = n_heads * src
            for at, sc in zip(halves, scores):
                blocks = [softmax_rows(sc[u * HEAD_PAD:(u + 1) * HEAD_PAD, u * wide:(u + 1) * wide], cross_mask[...], len_sm[at + u]) for u in range(GROUP)]
                vals = cross_buf[pl.ds(at, GROUP), 1].reshape(GROUP * wide, head_dim)
                ctx_s[head_rows(at, GROUP), :] = jnp.dot(block_diag(blocks), vals, preferred_element_type=F32)
            if after is not None:
                for u in range(2 * GROUP):
                    cross_copy(after, first + u).start()
            return c
        lax.fori_loop(0, tok // (2 * GROUP), body, 0)
        ctx = from_heads(ctx_s)
        return h + proj(layer, 5, ctx)

    q_s[...] = jnp.zeros_like(q_s)
    h = hid_ref[...].astype(F32)
    h = self_layer(0, h, cache_a, cache_a_out)
    for g in range(n_self):
        self_out(cache_a_out, g).wait()
        self_in(cache_b, g).start()
    h = cross_layer(0, h, cross_a, cross_b)
    x = norm_rows(h, gain_ref[2, 0:1, :], shift_ref[2, 0:1, :])
    for cp in ffn_copies():
        cp.wait()
    acc = h + fb2_ref[...].astype(F32).reshape(1, d_model)
    for f in range(0, ff, d_model):
        inner = jnp.dot(x, f1_buf[:, f:f + d_model], preferred_element_type=F32) + fb1_ref[f:f + d_model].astype(F32).reshape(1, d_model)
        inner = jnp.maximum(inner, 0.0).astype(BF16)
        acc = acc + jnp.dot(inner, f2_buf[f:f + d_model, :], preferred_element_type=F32)
    h = acc
    h = self_layer(1, h, cache_b, cache_b_out)
    h = cross_layer(1, h, cross_b, None)
    hid_out[...] = h
    z_out[...] = norm_rows(h, gain_ref[2, 1:2, :], shift_ref[2, 1:2, :])
    for g in range(n_self):
        self_out(cache_b_out, g).wait()


def dense_layers(hidden, self_pos, src_len, cache_a, cross_a, cache_b, cross_b, ln_gain, ln_shift, attn_w, attn_b, ffn_w1, ffn_b1, ffn_w2, ffn_b2):
    tok, d_model = hidden.shape
    n_heads, head_dim = cache_a.shape[3:]
    self_len, src = cache_a.shape[2], cross_a.shape[2]
    ff = ffn_w1.shape[1]
    swap = lambda arr: jnp.swapaxes(arr, 2, 3)
    sm = pl.BlockSpec(memory_space=pltpu.SMEM)
    vm = pl.BlockSpec(memory_space=VMEM)
    hbm = pl.BlockSpec(memory_space=pl.ANY)
    cache_t = jax.ShapeDtypeStruct((2, tok, n_heads, self_len, head_dim), BF16)
    n_self = tok // SELF_GROUP
    heads = VMEM((tok * HEAD_PAD, head_dim), F32)
    hid, z, out_a, out_b = pl.pallas_call(
        dense_kernel,
        out_shape=[jax.ShapeDtypeStruct((tok, d_model), F32), jax.ShapeDtypeStruct((tok, d_model), BF16), cache_t, cache_t],
        in_specs=[sm] * 2 + [vm] * 7 + [hbm] * 7,
        out_specs=[vm] * 2 + [hbm] * 2,
        scratch_shapes=[
            VMEM((12, d_model, d_model), BF16), VMEM((d_model, ff), BF16), VMEM((ff, d_model), BF16),
            VMEM((2, tok, n_heads, self_len, head_dim), BF16), VMEM((tok, 2, n_heads, src, head_dim), BF16),
            heads, heads, heads, heads, VMEM((tok, d_model), BF16), VMEM((tok * HEAD_PAD, 128), jnp.int32),
            VMEM((2 * HEAD_PAD, 2 * n_heads * self_len), jnp.int32), VMEM((HEAD_PAD, n_heads * src), jnp.int32),
            pltpu.SemaphoreType.DMA((12,)), pltpu.SemaphoreType.DMA((2,)), pltpu.SemaphoreType.DMA((n_self,)),
            pltpu.SemaphoreType.DMA((n_self,)), pltpu.SemaphoreType.DMA((tok,)),
        ],
        compiler_params=pltpu.CompilerParams(vmem_limit_bytes=62 * 1024 * 1024),
        name='dense_layers',
    )(self_pos, src_len, self_pos.reshape(-1, 1), hidden, jnp.swapaxes(ln_gain, 0, 1), jnp.swapaxes(ln_shift, 0, 1), jnp.swapaxes(attn_b, 0, 1), ffn_b1, ffn_b2,
      swap(cache_a), swap(cross_a), swap(cache_b), swap(cross_b), attn_w, ffn_w1, ffn_w2)
    return hid, z, swap(out_a), swap(out_b)


def peer(index):
    return dict(device_id={'ep': index}, device_id_type=pl.DeviceIdType.MESH)


def neighbours():
    me = lax.axis_index('ep')
    core, x, y = me % 2, (me // 2) % 2, me // 4
    at = lambda yy, xx, cc: (yy * 2 + xx) * 2 + cc
    return me, core, x, y, at


def entry_barrier(others):
    barrier = pltpu.get_barrier_semaphore()
    for other in others:
        pl.semaphore_signal(barrier, inc=1, **peer(other))
    pl.semaphore_wait(barrier, len(others))


def gather_kernel(z_ref, idst_ref, zall_ref, idsall_ref, flip, ids_ref, send_sem, recv_sem):
    me, core, x, y, at = neighbours()
    twin = at(y, x, 1 - core)
    chips = [(y, 1 - x), (1 - y, x), (1 - y, 1 - x)]
    tok = z_ref.shape[0]
    flip[...] = jnp.zeros_like(flip)
    flip[0:2, 0:tok] = idst_ref[...].astype(F32)
    ids_ref[...] = jnp.transpose(flip[...])[:tok]
    entry_barrier([twin] + [at(cy, cx, core) for cy, cx in chips])

    def send(slot, src_z, src_ids, row, to):
        out = []
        for which, src, dst in ((0, src_z, zall_ref), (1, src_ids, idsall_ref)):
            cp = pltpu.make_async_remote_copy(
                src_ref=src, dst_ref=dst.at[row], send_sem=send_sem.at[slot, which], recv_sem=recv_sem.at[slot, which], **peer(to))
            cp.start()
            out.append(cp)
        return out

    sent = []
    for j in (2, 0, 1):
        sent.append((j, send(j, z_ref, ids_ref, me, at(*chips[j], core))))
    sent.append((3, send(3, z_ref, ids_ref, me, twin)))
    zall_ref[me] = z_ref[...]
    idsall_ref[me] = ids_ref[...]
    relays = []
    for j in (0, 1, 2):
        for cp in dict(sent)[j]:
            cp.wait_recv()
        row = at(*chips[j], core)
        relays += send(4 + j, zall_ref.at[row], idsall_ref.at[row], row, twin)
    for cp in dict(sent)[3]:
        cp.wait_recv()
    for cp in relays:
        cp.wait_recv()
    for _, cps in sent:
        for cp in cps:
            cp.wait_send()
    for cp in relays:
        cp.wait_send()


def gather_tokens(z_bf, ids_t, group_n):
    tok, d_model = z_bf.shape
    return pl.pallas_call(
        gather_kernel,
        out_shape=[jax.ShapeDtypeStruct((group_n, tok, d_model), BF16), jax.ShapeDtypeStruct((group_n, tok, 128), F32)],
        in_specs=[pl.BlockSpec(memory_space=VMEM)] * 2,
        out_specs=[pl.BlockSpec(memory_space=VMEM)] * 2,
        scratch_shapes=[VMEM((128, 128), F32), VMEM((tok, 128), F32), pltpu.SemaphoreType.DMA((7, 2)), pltpu.SemaphoreType.DMA((7, 2))],
        compiler_params=pltpu.CompilerParams(collective_id=0, has_side_effects=True),
        name='gather_tokens',
    )(z_bf, ids_t)


def reduce_kernel(part_ref, hid_ref, out_ref, own, r1, s1, r2, s2, r3, send_sem, recv_sem):
    me, core, x, y, at = neighbours()
    twin, xn, yn = at(y, x, 1 - core), at(y, 1 - x, core), at(1 - y, x, core)
    entry_barrier([twin, xn, yn])
    half = hid_ref.shape[1] // 2
    cols = (pl.ds(0, half), pl.ds(half, half))

    def send(slot, src, dst, to):
        cp = pltpu.make_async_remote_copy(src_ref=src, dst_ref=dst, send_sem=send_sem.at[slot], recv_sem=recv_sem.at[slot], **peer(to))
        cp.start()
        return cp

    chips = [(1 - y, 1 - x), (y, 1 - x), (1 - y, x), (y, x)]
    first = [send(k, part_ref.at[at(cy, cx, 1 - core)], r1.at[k], twin) for k, (cy, cx) in enumerate(chips)]

    def sum1(k):
        first[k].wait_recv()
        cy, cx = chips[k]
        s1[k] = part_ref[at(cy, cx, core)] + r1[k]

    sum1(0)
    a0 = send(4, s1.at[0, :, cols[0]], r2.at[0, 0], xn)
    b0 = send(5, s1.at[0, :, cols[1]], r2.at[1, 0], yn)
    sum1(1)
    a1 = send(6, s1.at[1, :, cols[0]], r2.at[0, 1], xn)
    sum1(2)
    b1 = send(7, s1.at[2, :, cols[1]], r2.at[1, 1], yn)
    sum1(3)
    a0.wait_recv()
    s2[0] = s1[2, :, :half] + r2[0, 0]
    a2 = send(8, s2.at[0], r3.at[0], yn)
    b0.wait_recv()
    s2[1] = s1[1, :, half:] + r2[1, 0]
    b2 = send(9, s2.at[1], r3.at[1], xn)
    a1.wait_recv()
    own_a = hid_ref[:, :half] + s1[3, :, :half] + r2[0, 1]
    b1.wait_recv()
    own_b = hid_ref[:, half:] + s1[3, :, half:] + r2[1, 1]
    a2.wait_recv()
    out_ref[:, :half] = (own_a + r3[0]).astype(BF16)
    b2.wait_recv()
    out_ref[:, half:] = (own_b + r3[1]).astype(BF16)
    for cp in first + [a0, b0, a1, b1, a2, b2]:
        cp.wait_send()


def reduce_outputs(partial, hid_f32):
    group_n, tok, d_model = partial.shape
    half = d_model // 2
    return pl.pallas_call(
        reduce_kernel,
        out_shape=jax.ShapeDtypeStruct((tok, d_model), BF16),
        in_specs=[pl.BlockSpec(memory_space=VMEM)] * 2,
        out_specs=pl.BlockSpec(memory_space=VMEM),
        scratch_shapes=[
            VMEM((8, 128), F32),
            VMEM((4, tok, d_model), F32), VMEM((4, tok, d_model), F32),
            VMEM((2, 2, tok, half), F32), VMEM((2, tok, half), F32), VMEM((2, tok, half), F32),
            pltpu.SemaphoreType.DMA((10,)), pltpu.SemaphoreType.DMA((10,)),
        ],
        compiler_params=pltpu.CompilerParams(collective_id=1, has_side_effects=True),
        name='reduce_outputs',
    )(partial, hid_f32)


ROWS = 128
SPLIT = 2
SLOTS = 6


def expert_kernel(z_ref, ids_ref, rw_ref, b1_in, b2_in, w1_hbm, w2_hbm, out_ref,
                  b1_ref, b2_ref, w1_buf, w2_buf, rank_s, gate_s, cnt_v, cnt_s, list_s, x_s, o_s, sem1, sem2, csem):
    n_tok, d_model = z_ref.shape
    n_loc = w1_hbm.shape[0]
    ff = w1_hbm.shape[2]
    fc = ff // SPLIT
    n_blk = x_s.shape[0]
    me = lax.axis_index('ep')
    base = me * n_loc
    lane = lax.broadcasted_iota(jnp.int32, (n_tok, 128), 1)
    id0, id1 = ids_ref[:, 0:1].astype(jnp.int32), ids_ref[:, 1:2].astype(jnp.int32)
    hit_loc = jnp.logical_or(id0 - base == lane, id1 - base == lane)
    hit_loc = jnp.logical_and(hit_loc, lane < n_loc)
    hit_t = hit_loc.astype(F32)
    counts = jnp.sum(hit_t, axis=0, keepdims=True)
    cnt_v[...] = jnp.broadcast_to(counts, cnt_v.shape).astype(jnp.int32)
    cp = pltpu.make_async_copy(cnt_v, cnt_s, csem)
    cp.start()
    cp.wait()

    def scan_body(e, n_act):
        @pl.when(cnt_s[0, e] > 0)
        def _():
            list_s[n_act] = e
        return n_act + jnp.where(cnt_s[0, e] > 0, 1, 0)
    n_act = lax.fori_loop(0, n_loc, scan_body, 0)
    n_step = n_act * SPLIT

    def copies(step, slot):
        e = list_s[step // SPLIT]
        f0 = pl.multiple_of((step % SPLIT) * fc, fc)
        return (pltpu.make_async_copy(w1_hbm.at[e, :, pl.ds(f0, fc)], w1_buf.at[slot], sem1.at[slot]),
                pltpu.make_async_copy(w2_hbm.at[e, pl.ds(f0, fc), :], w2_buf.at[slot], sem2.at[slot]))

    for s in range(SLOTS):
        @pl.when(s < n_step)
        def _():
            for c in copies(s, s):
                c.start()

    b1_ref[...] = b1_in[...].astype(F32)
    b2_ref[...] = b2_in[...].astype(F32)
    hit_bf = hit_t.astype(BF16)
    row_i = lax.broadcasted_iota(jnp.int32, (n_tok, n_tok), 0)
    col_i = lax.broadcasted_iota(jnp.int32, (n_tok, n_tok), 1)
    before = (row_i < col_i).astype(BF16)
    hit = jnp.transpose(hit_t)
    rank = jnp.dot(hit.astype(BF16), before, preferred_element_type=F32)
    rank_s[...] = jnp.where(hit > 0.5, rank, -1.0)

    logits = jnp.dot(z_ref[...], rw_ref[...], preferred_element_type=F32)
    top = jnp.max(logits, axis=-1, keepdims=True)
    ex = jnp.exp(logits - top)
    probs = ex / jnp.sum(ex, axis=-1, keepdims=True)
    p0 = jnp.sum(jnp.where(lane == id0, probs, 0.0), axis=-1, keepdims=True)
    p1 = jnp.sum(jnp.where(lane == id1, probs, 0.0), axis=-1, keepdims=True)
    tot = p0 + p1
    g0, g1 = p0 / tot, p1 / tot
    gate_s[...] = jnp.where(lane == id0 - base, g0, jnp.where(lane == id1 - base, g1, 0.0))
    out_ref[...] = jnp.zeros_like(out_ref)

    def step_body(step, carry):
        slot = step % SLOTS
        e = list_s[step // SPLIT]
        part = step % SPLIT
        blocks = (cnt_s[0, e] + ROWS - 1) // ROWS
        slot_i = lax.broadcasted_iota(jnp.int32, (ROWS, n_tok), 0)

        def pick(j):
            want = (slot_i + j * ROWS).astype(F32)
            return (want == rank_s[pl.ds(e, 1), :]).astype(BF16)

        @pl.when(part == 0)
        def _():
            def gather_body(j, c):
                x_s[j] = jnp.dot(pick(j), z_ref[...], preferred_element_type=F32).astype(BF16)
                o_s[j] = jnp.broadcast_to(b2_ref[pl.ds(e, 1), :], (ROWS, d_model))
                return c
            lax.fori_loop(0, blocks, gather_body, 0)

        for c in copies(step, slot):
            c.wait()
        bias = b1_ref[pl.ds(e, 1), pl.ds(pl.multiple_of(part * fc, fc), fc)]

        def block_body(j, c):
            inner = jnp.dot(x_s[j], w1_buf[slot], preferred_element_type=F32) + bias
            inner = jnp.maximum(inner, 0.0).astype(BF16)
            o_s[j] += jnp.dot(inner, w2_buf[slot], preferred_element_type=F32)
            return c
        lax.fori_loop(0, blocks, block_body, 0)

        @pl.when(step + SLOTS < n_step)
        def _():
            for c in copies(step + SLOTS, slot):
                c.start()

        @pl.when(part == SPLIT - 1)
        def _():
            lane_g = lax.broadcasted_iota(jnp.int32, (n_tok, 128), 1)
            gate = jnp.sum(jnp.where(lane_g == e, gate_s[...], 0.0), axis=-1, keepdims=True)

            def scatter_body(j, c):
                back = lax.dot_general(pick(j), o_s[j].astype(BF16), (((0,), (0,)), ((), ())), preferred_element_type=F32)
                out_ref[...] += gate * back
                return c
            lax.fori_loop(0, blocks, scatter_body, 0)
        return carry

    lax.fori_loop(0, n_step, step_body, 0)


def run_experts(z_all, ids_all, router_w, exp_w1, exp_b1, exp_w2, exp_b2):
    n_tok, d_model = z_all.shape
    n_loc, _, ff = exp_w1.shape
    fc = ff // SPLIT
    n_blk = n_tok // ROWS
    vm = pl.BlockSpec(memory_space=VMEM)
    hbm = pl.BlockSpec(memory_space=pl.ANY)
    return pl.pallas_call(
        expert_kernel,
        out_shape=jax.ShapeDtypeStruct((n_tok, d_model), F32),
        in_specs=[vm] * 5 + [hbm] * 2,
        out_specs=vm,
        scratch_shapes=[
            VMEM((n_loc, ff), F32), VMEM((n_loc, d_model), F32),
            VMEM((SLOTS, d_model, fc), BF16), VMEM((SLOTS, fc, d_model), BF16),
            VMEM((128, n_tok), F32), VMEM((n_tok, 128), F32),
            VMEM((8, 128), jnp.int32), pltpu.SMEM((8, 128), jnp.int32), pltpu.SMEM((n_loc,), jnp.int32),
            VMEM((n_blk, ROWS, d_model), BF16), VMEM((n_blk, ROWS, d_model), F32),
            pltpu.SemaphoreType.DMA((SLOTS,)), pltpu.SemaphoreType.DMA((SLOTS,)), pltpu.SemaphoreType.DMA,
        ],
        compiler_params=pltpu.CompilerParams(vmem_limit_bytes=60 * 1024 * 1024),
        name='run_experts',
    )(z_all, ids_all, router_w, exp_b1, exp_b2, exp_w1, exp_w2)


def solution(mesh):
    group_n = mesh.shape['ep']

    def local_step(hidden, self_pos, src_len, cache_a, cross_a, cache_b, cross_b, route_ids, ln_gain, ln_shift, attn_w, attn_b, ffn_w1, ffn_b1, ffn_w2, ffn_b2, router_w, exp_w1, exp_b1, exp_w2, exp_b2):
        hid_f32, z_bf, cache_a_new, cache_b_new = dense_layers(hidden, self_pos, src_len, cache_a, cross_a, cache_b, cross_b, ln_gain, ln_shift, attn_w, attn_b, ffn_w1, ffn_b1, ffn_w2, ffn_b2)
        tok, d_model = z_bf.shape
        z_all, ids_all = gather_tokens(z_bf, route_ids.T, group_n)
        partial = run_experts(z_all.reshape(-1, d_model), ids_all.reshape(-1, 128), router_w, exp_w1, exp_b1, exp_w2, exp_b2)
        out = reduce_outputs(partial.reshape(group_n, tok, d_model), hid_f32)
        return out, cache_a_new, cache_b_new

    tok_spec = P(('dp', 'ep'))
    cache_spec = P(None, ('dp', 'ep'))
    rep_spec = P()
    exp_spec = P('ep')
    in_specs = (tok_spec, tok_spec, tok_spec, cache_spec, cache_spec, cache_spec, cache_spec, tok_spec) + (rep_spec,) * 9 + (exp_spec,) * 4
    out_specs = (tok_spec, cache_spec, cache_spec)
    return jax.shard_map(local_step, mesh=mesh, in_specs=in_specs, out_specs=out_specs, check_vma=False)
```

```python
import functools

import jax
import jax.numpy as jnp
from jax import lax
from jax.experimental import pallas as pl
from jax.experimental.pallas import tpu as pltpu
from jax.sharding import PartitionSpec as P

LN_EPS = 1e-5
F32 = jnp.float32
BF16 = jnp.bfloat16
VMEM = pltpu.VMEM


CROSS_GROUP = 16
CROSS_UNIT = 1
SELF_GROUP = 16
SELF_UNIT = 2
HEAD_PAD = 16


def norm_rows(x_val, gain_vec, shift_vec):
    mean_val = jnp.mean(x_val, axis=-1, keepdims=True)
    centered = x_val - mean_val
    var_val = jnp.mean(centered * centered, axis=-1, keepdims=True)
    return (centered * lax.rsqrt(var_val + LN_EPS) * gain_vec + shift_vec).astype(BF16)


def dense_kernel(pos_sm, len_sm, hid_ref, gain_ref, shift_ref, ab_ref, fb1_ref, fb2_ref,
                 cache_a, cross_a, cache_b, cross_b, aw_hbm, w1_hbm, w2_hbm,
                 hid_out, z_out, cache_a_out, cache_b_out,
                 w_buf, f1_buf, f2_buf, self_buf, cross_buf, q_s, k_s, v_s, ctx_s, cat_s, lim_s, self_mask, cross_mask,
                 w_sem, f_sem, in_sem, out_sem, cross_sem):
    tok, d_model = hid_ref.shape
    n_heads, self_len, head_dim = self_buf.shape[2:]
    src = cross_buf.shape[3]
    ff = f1_buf.shape[1]
    scale = head_dim ** -0.5
    n_self = tok // SELF_GROUP

    def head_rows(b, n):
        return pl.ds(pl.multiple_of(b * HEAD_PAD, HEAD_PAD), n * HEAD_PAD)

    def weight_copy(i):
        return pltpu.make_async_copy(aw_hbm.at[i // 6, i % 6], w_buf.at[i], w_sem.at[i])

    def ffn_copies():
        return (pltpu.make_async_copy(w1_hbm, f1_buf, f_sem.at[0]), pltpu.make_async_copy(w2_hbm, f2_buf, f_sem.at[1]))

    def self_in(cache, g):
        rows = pl.ds(g * SELF_GROUP, SELF_GROUP)
        return pltpu.make_async_copy(cache.at[:, rows], self_buf.at[:, rows], in_sem.at[g])

    def self_out(cache_out, g):
        rows = pl.ds(g * SELF_GROUP, SELF_GROUP)
        return pltpu.make_async_copy(self_buf.at[:, rows], cache_out.at[:, rows], out_sem.at[g])

    def cross_rows(b):
        return pl.multiple_of(((len_sm[b] + 15) // 16) * 16, 16)

    def cross_copy(cross, b):
        rows = pl.ds(0, cross_rows(b))
        return pltpu.make_async_copy(cross.at[:, b, :, rows, :], cross_buf.at[b, :, :, rows, :], cross_sem.at[b])

    for i in range(3):
        weight_copy(i).start()
    for g in range(n_self):
        self_in(cache_a, g).start()
    weight_copy(3).start()
    weight_copy(4).start()

    def first_cross(b, c):
        cross_copy(cross_a, b).start()
        return c
    lax.fori_loop(0, tok, first_cross, 0)
    weight_copy(5).start()
    for cp in ffn_copies():
        cp.start()
    for i in range(6, 12):
        weight_copy(i).start()

    def zero_tail(b, c):
        def zero_part(part, c2):
            cross_buf[b, 1, :, pl.ds(pl.multiple_of(part * 16, 16), 16), :] = jnp.zeros((n_heads, 16, head_dim), BF16)
            return c2
        return lax.fori_loop(cross_rows(b) // 16, src // 16, zero_part, c)
    lax.fori_loop(0, tok, zero_tail, 0)

    def build_mask(ref, length):
        row = lax.broadcasted_iota(jnp.int32, ref.shape, 0)
        lane = lax.broadcasted_iota(jnp.int32, ref.shape, 1)
        seq, head = lane // (n_heads * length), (lane // length) % n_heads
        ref[...] = jnp.where(seq * HEAD_PAD + head == row, lane % length, 1 << 20)
    build_mask(self_mask, self_len)
    build_mask(cross_mask, src)

    def fill_limit(b, c):
        lim_s[head_rows(b, 1), :] = jnp.full((HEAD_PAD, 128), pos_sm[b] + 1, jnp.int32)
        return c
    lax.fori_loop(0, tok, fill_limit, 0)

    def to_heads(ref, val):
        val = val.astype(BF16).astype(F32)
        for h in range(n_heads):
            ref[pl.ds(h, tok, stride=HEAD_PAD), :] = val[:, h * head_dim:(h + 1) * head_dim]

    def from_heads(ref):
        for h in range(0, n_heads, 2):
            two = [ref[pl.ds(h + k, tok, stride=HEAD_PAD), :] for k in range(2)]
            cat_s[:, h * head_dim:(h + 2) * head_dim] = jnp.concatenate(two, axis=1).astype(BF16)
        return cat_s[...]

    def softmax_rows(scores, mask, limit):
        scores = jnp.where(mask < limit, scores * scale, -1e30)
        top = jnp.max(scores, axis=-1, keepdims=True)
        ex = jnp.exp(scores - top)
        return (ex * (1.0 / jnp.sum(ex, axis=-1, keepdims=True))).astype(BF16)

    def scores_of(q, keys):
        return lax.dot_general(q, keys, (((1,), (1,)), ((), ())), preferred_element_type=F32)

    def block_diag(blocks):
        rows = []
        for k, blk in enumerate(blocks):
            pad = jnp.zeros_like(blk)
            rows.append(jnp.concatenate([blk if j == k else pad for j in range(len(blocks))], axis=1))
        return jnp.concatenate(rows, axis=0)

    def proj(layer, i, x_bf):
        weight_copy(layer * 6 + i).wait()
        bias = ab_ref[i].astype(F32)[layer:layer + 1, :]
        return jnp.dot(x_bf, w_buf[layer * 6 + i], preferred_element_type=F32) + bias

    def self_layer(layer, h, cache, cache_out):
        x = norm_rows(h, gain_ref[0, layer:layer + 1, :], shift_ref[0, layer:layer + 1, :])
        to_heads(q_s, proj(layer, 0, x))
        to_heads(k_s, proj(layer, 1, x))
        to_heads(v_s, proj(layer, 2, x))
        row_i = lax.broadcasted_iota(jnp.int32, (self_len, head_dim), 0)
        row_b = row_i.astype(F32).astype(BF16)

        def body(g, c):
            self_in(cache, g).wait()
            first = g * SELF_GROUP
            sides = []
            for which, new in ((0, k_s), (1, v_s)):
                tiles = []
                for u in range(SELF_GROUP):
                    b = first + u
                    hit = row_b == jnp.full(row_b.shape, pos_sm[b], jnp.int32).astype(F32).astype(BF16)
                    for hd in range(n_heads):
                        row = new[pl.ds(b * HEAD_PAD + hd, self_len, stride=0), :]
                        tile = jnp.where(hit, row.astype(BF16), self_buf[which, b, hd])
                        self_buf[which, b, hd] = tile
                        tiles.append(tile)
                sides.append(tiles)
            n = SELF_UNIT
            parts = range(0, SELF_GROUP, n)
            wide = n * n_heads * self_len
            stack = lambda tiles, p: jnp.concatenate(tiles[p * n_heads:(p + n) * n_heads], axis=0)
            scores = [scores_of(q_s[head_rows(first + p, n), :].astype(BF16), stack(sides[0], p)) for p in parts]
            probs = []
            for p, sc in zip(parts, scores):
                two = 2 * n_heads * self_len
                blocks = []
                for k in range(n // 2):
                    lim = lim_s[head_rows(first + p + 2 * k, 2), :]
                    lim = jnp.concatenate([lim] * (two // 128), axis=1)
                    blocks.append(softmax_rows(sc[k * 2 * HEAD_PAD:(k + 1) * 2 * HEAD_PAD, k * two:(k + 1) * two], self_mask[...], lim))
                probs.append(block_diag(blocks))
            for p, pr in zip(parts, probs):
                ctx_s[head_rows(first + p, n), :] = jnp.dot(pr, stack(sides[1], p), preferred_element_type=F32)
            self_out(cache_out, g).start()
            return c
        lax.fori_loop(0, n_self, body, 0)
        ctx = from_heads(ctx_s)
        return h + proj(layer, 3, ctx)

    def cross_layer(layer, h, cross, after):
        x = norm_rows(h, gain_ref[1, layer:layer + 1, :], shift_ref[1, layer:layer + 1, :])
        to_heads(q_s, proj(layer, 4, x))

        def body(g, c):
            first = g * CROSS_GROUP
            for u in range(CROSS_GROUP):
                cross_copy(cross, first + u).wait()
            n = CROSS_UNIT
            parts = [first + p for p in range(0, CROSS_GROUP, n)]
            wide = n_heads * src
            scores = [scores_of(q_s[head_rows(at, n), :].astype(BF16), cross_buf[pl.ds(at, n), 0].reshape(n * wide, head_dim)) for at in parts]
            probs = []
            for at, sc in zip(parts, scores):
                probs.append(block_diag([softmax_rows(sc[u * HEAD_PAD:(u + 1) * HEAD_PAD, u * wide:(u + 1) * wide], cross_mask[...], len_sm[at + u]) for u in range(n)]))
            for at, pr in zip(parts, probs):
                vals = cross_buf[pl.ds(at, n), 1].reshape(n * wide, head_dim)
                ctx_s[head_rows(at, n), :] = jnp.dot(pr, vals, preferred_element_type=F32)
            if after is not None:
                for u in range(CROSS_GROUP):
                    cross_copy(after, first + u).start()
            return c
        lax.fori_loop(0, tok // CROSS_GROUP, body, 0)
        ctx = from_heads(ctx_s)
        return h + proj(layer, 5, ctx)

    q_s[...] = jnp.zeros_like(q_s)
    h = hid_ref[...].astype(F32)
    h = self_layer(0, h, cache_a, cache_a_out)
    for g in range(n_self):
        self_out(cache_a_out, g).wait()
        self_in(cache_b, g).start()
    h = cross_layer(0, h, cross_a, cross_b)
    x = norm_rows(h, gain_ref[2, 0:1, :], shift_ref[2, 0:1, :])
    for cp in ffn_copies():
        cp.wait()
    acc = h + fb2_ref[...].astype(F32).reshape(1, d_model)
    for f in range(0, ff, d_model):
        inner = jnp.dot(x, f1_buf[:, f:f + d_model], preferred_element_type=F32) + fb1_ref[f:f + d_model].astype(F32).reshape(1, d_model)
        inner = jnp.maximum(inner, 0.0).astype(BF16)
        acc = acc + jnp.dot(inner, f2_buf[f:f + d_model, :], preferred_element_type=F32)
    h = acc
    h = self_layer(1, h, cache_b, cache_b_out)
    h = cross_layer(1, h, cross_b, None)
    hid_out[...] = h
    z_out[...] = norm_rows(h, gain_ref[2, 1:2, :], shift_ref[2, 1:2, :])
    for g in range(n_self):
        self_out(cache_b_out, g).wait()


def dense_layers(hidden, self_pos, src_len, cache_a, cross_a, cache_b, cross_b, ln_gain, ln_shift, attn_w, attn_b, ffn_w1, ffn_b1, ffn_w2, ffn_b2):
    tok, d_model = hidden.shape
    n_heads, head_dim = cache_a.shape[3:]
    self_len, src = cache_a.shape[2], cross_a.shape[2]
    ff = ffn_w1.shape[1]
    swap = lambda arr: jnp.swapaxes(arr, 2, 3)
    sm = pl.BlockSpec(memory_space=pltpu.SMEM)
    vm = pl.BlockSpec(memory_space=VMEM)
    hbm = pl.BlockSpec(memory_space=pl.ANY)
    cache_t = jax.ShapeDtypeStruct((2, tok, n_heads, self_len, head_dim), BF16)
    n_self = tok // SELF_GROUP
    heads = VMEM((tok * HEAD_PAD, head_dim), F32)
    hid, z, out_a, out_b = pl.pallas_call(
        dense_kernel,
        out_shape=[VMEM((tok, d_model), F32), VMEM((tok, d_model), BF16), cache_t, cache_t],
        in_specs=[sm] * 2 + [vm] * 6 + [hbm] * 7,
        out_specs=[vm] * 2 + [hbm] * 2,
        scratch_shapes=[
            VMEM((12, d_model, d_model), BF16), VMEM((d_model, ff), BF16), VMEM((ff, d_model), BF16),
            VMEM((2, tok, n_heads, self_len, head_dim), BF16), VMEM((tok, 2, n_heads, src, head_dim), BF16),
            heads, heads, heads, heads, VMEM((tok, d_model), BF16), VMEM((tok * HEAD_PAD, 128), jnp.int32),
            VMEM((2 * HEAD_PAD, 2 * n_heads * self_len), jnp.int32), VMEM((HEAD_PAD, n_heads * src), jnp.int32),
            pltpu.SemaphoreType.DMA((12,)), pltpu.SemaphoreType.DMA((2,)), pltpu.SemaphoreType.DMA((n_self,)),
            pltpu.SemaphoreType.DMA((n_self,)), pltpu.SemaphoreType.DMA((tok,)),
        ],
        compiler_params=pltpu.CompilerParams(vmem_limit_bytes=61 * 1024 * 1024),
        name='dense_layers',
    )(self_pos, src_len, hidden, jnp.swapaxes(ln_gain, 0, 1), jnp.swapaxes(ln_shift, 0, 1), jnp.swapaxes(attn_b, 0, 1), ffn_b1, ffn_b2,
      swap(cache_a), swap(cross_a), swap(cache_b), swap(cross_b), attn_w, ffn_w1, ffn_w2)
    return hid, z, swap(out_a), swap(out_b)


def peer(index):
    return dict(device_id={'ep': index}, device_id_type=pl.DeviceIdType.MESH)


def neighbours():
    me = lax.axis_index('ep')
    core, x, y = me % 2, (me // 2) % 2, me // 4
    at = lambda yy, xx, cc: (yy * 2 + xx) * 2 + cc
    return me, core, x, y, at


def entry_barrier(others):
    barrier = pltpu.get_barrier_semaphore()
    for other in others:
        pl.semaphore_signal(barrier, inc=1, **peer(other))
    pl.semaphore_wait(barrier, len(others))


def named_experts(ids_cols, base, n_loc):
    n_tok = ids_cols.shape[0]
    lane = lax.broadcasted_iota(jnp.int32, (n_tok, 128), 1)
    id0 = ids_cols[:, 0:1].astype(jnp.int32) - base
    id1 = ids_cols[:, 1:2].astype(jnp.int32) - base
    hit = jnp.logical_and(jnp.logical_or(id0 == lane, id1 == lane), lane < n_loc)
    return id0, id1, lane, hit.astype(F32)


def gather_kernel(n_loc, z_ref, idst_ref, zall_ref, cols_ref, meta_ref, flip, ids_ref, idsall, send_sem, recv_sem):
    me, core, x, y, at = neighbours()
    twin = at(y, x, 1 - core)
    chips = [(y, 1 - x), (1 - y, x), (1 - y, 1 - x)]
    tok = z_ref.shape[0]
    group_n = zall_ref.shape[0]
    ids_ref[...] = jnp.zeros_like(ids_ref)
    ids_ref[0:2, 0:tok] = idst_ref[...].astype(F32)
    entry_barrier([twin] + [at(cy, cx, core) for cy, cx in chips])

    def send(slot, which, src, row, to):
        dst = (idsall, zall_ref)[which]
        cp = pltpu.make_async_remote_copy(
            src_ref=src, dst_ref=dst.at[row], send_sem=send_sem.at[slot, which], recv_sem=recv_sem.at[slot, which], **peer(to))
        cp.start()
        return cp

    far = [at(cy, cx, core) for cy, cx in chips]
    ids_sent = [send(j, 0, ids_ref, me, far[j]) for j in range(3)] + [send(3, 0, ids_ref, me, twin)]
    z_sent = {j: send(j, 1, z_ref, me, far[j]) for j in (2, 0, 1)}
    z_sent[3] = send(3, 1, z_ref, me, twin)
    zall_ref[me] = z_ref[...]
    idsall[me] = ids_ref[...]
    relays = []
    for j in range(3):
        ids_sent[j].wait_recv()
        relays.append(send(4 + j, 0, idsall.at[far[j]], far[j], twin))
    ids_sent[3].wait_recv()
    for cp in relays:
        cp.wait_recv()

    flip[...] = jnp.zeros_like(flip)
    for d in range(group_n):
        flip[2 * d:2 * d + 2, :] = idsall[d, 0:2, :]
    cols = jnp.transpose(flip[...])[:tok]
    lane_b = lax.broadcasted_iota(jnp.int32, (tok, 128), 1)
    wide = [jnp.where(lane_b == 0, cols[:, 2 * d:2 * d + 1], cols[:, 2 * d + 1:2 * d + 2]) for d in range(group_n)]
    cols_ref[...] = jnp.concatenate(wide, axis=0)
    _, _, _, hit = named_experts(cols_ref[...], me * n_loc, n_loc)
    ones = jnp.ones((group_n * tok, 128), BF16)
    count = lax.dot_general(hit.astype(BF16), ones, (((0,), (0,)), ((), ())), preferred_element_type=F32)
    row_i = lax.broadcasted_iota(jnp.int32, (128, 128), 0)
    col_i = lax.broadcasted_iota(jnp.int32, (128, 128), 1)
    named = (count > 0.5).astype(F32)
    order = jnp.dot((row_i > col_i).astype(BF16), named.astype(BF16), preferred_element_type=F32)
    spot = jnp.where(order == col_i.astype(F32), named, 0.0)
    expert_list = jnp.sum(spot * row_i.astype(F32), axis=0, keepdims=True)
    counts = jnp.sum(hit, axis=0, keepdims=True)
    total = jnp.sum(named, axis=0, keepdims=True)
    meta_ref[...] = jnp.concatenate([counts, expert_list, total, jnp.zeros((5, 128), F32)], axis=0).astype(jnp.int32)

    z_relays = []
    for j in (0, 1, 2):
        z_sent[j].wait_recv()
        z_relays.append(send(4 + j, 1, zall_ref.at[far[j]], far[j], twin))
    z_sent[3].wait_recv()
    for cp in z_relays:
        cp.wait_recv()
    for cp in ids_sent + relays + list(z_sent.values()) + z_relays:
        cp.wait_send()


def in_vmem(arr):
    return pltpu.with_memory_space_constraint(arr, VMEM)


def gather_tokens(z_bf, ids_t, group_n, n_loc):
    tok, d_model = z_bf.shape
    return pl.pallas_call(
        functools.partial(gather_kernel, n_loc),
        out_shape=[VMEM((group_n, tok, d_model), BF16), VMEM((group_n * tok, 128), F32), jax.ShapeDtypeStruct((8, 128), jnp.int32)],
        in_specs=[pl.BlockSpec(memory_space=VMEM)] * 2,
        out_specs=[pl.BlockSpec(memory_space=VMEM)] * 3,
        scratch_shapes=[VMEM((128, 128), F32), VMEM((8, 128), F32), VMEM((group_n, 8, 128), F32),
                        pltpu.SemaphoreType.DMA((7, 2)), pltpu.SemaphoreType.DMA((7, 2))],
        compiler_params=pltpu.CompilerParams(collective_id=0, has_side_effects=True, vmem_limit_bytes=16 * 1024 * 1024),
        name='gather_tokens',
    )(in_vmem(z_bf), ids_t)


def reduce_kernel(part_ref, hid_ref, out_ref, r1, s1, r2, s2, r3, send_sem, recv_sem):
    me, core, x, y, at = neighbours()
    twin, xn, yn = at(y, x, 1 - core), at(y, 1 - x, core), at(1 - y, x, core)
    entry_barrier([twin, xn, yn])
    half = hid_ref.shape[1] // 2
    cols = (pl.ds(0, half), pl.ds(half, half))

    def send(slot, src, dst, to):
        cp = pltpu.make_async_remote_copy(src_ref=src, dst_ref=dst, send_sem=send_sem.at[slot], recv_sem=recv_sem.at[slot], **peer(to))
        cp.start()
        return cp

    chips = [(1 - y, 1 - x), (y, 1 - x), (1 - y, x), (y, x)]
    first = [send(k, part_ref.at[at(cy, cx, 1 - core)], r1.at[k], twin) for k, (cy, cx) in enumerate(chips)]

    def sum1(k):
        first[k].wait_recv()
        cy, cx = chips[k]
        s1[k] = part_ref[at(cy, cx, core)] + r1[k]

    sum1(0)
    a0 = send(4, s1.at[0, :, cols[0]], r2.at[0, 0], xn)
    b0 = send(5, s1.at[0, :, cols[1]], r2.at[1, 0], yn)
    sum1(1)
    a1 = send(6, s1.at[1, :, cols[0]], r2.at[0, 1], xn)
    sum1(2)
    b1 = send(7, s1.at[2, :, cols[1]], r2.at[1, 1], yn)
    sum1(3)
    a0.wait_recv()
    s2[0] = s1[2, :, :half] + r2[0, 0]
    a2 = send(8, s2.at[0], r3.at[0], yn)
    b0.wait_recv()
    s2[1] = s1[1, :, half:] + r2[1, 0]
    b2 = send(9, s2.at[1], r3.at[1], xn)
    a1.wait_recv()
    own_a = hid_ref[:, :half] + s1[3, :, :half] + r2[0, 1]
    b1.wait_recv()
    own_b = hid_ref[:, half:] + s1[3, :, half:] + r2[1, 1]
    a2.wait_recv()
    out_ref[:, :half] = (own_a + r3[0]).astype(BF16)
    b2.wait_recv()
    out_ref[:, half:] = (own_b + r3[1]).astype(BF16)
    for cp in first + [a0, b0, a1, b1, a2, b2]:
        cp.wait_send()


def reduce_outputs(partial, hid_f32):
    group_n, tok, d_model = partial.shape
    half = d_model // 2
    return pl.pallas_call(
        reduce_kernel,
        out_shape=VMEM((tok, d_model), BF16),
        in_specs=[pl.BlockSpec(memory_space=VMEM)] * 2,
        out_specs=pl.BlockSpec(memory_space=VMEM),
        scratch_shapes=[
            VMEM((4, tok, d_model), F32), VMEM((4, tok, d_model), F32),
            VMEM((2, 2, tok, half), F32), VMEM((2, tok, half), F32), VMEM((2, tok, half), F32),
            pltpu.SemaphoreType.DMA((10,)), pltpu.SemaphoreType.DMA((10,)),
        ],
        compiler_params=pltpu.CompilerParams(collective_id=1, has_side_effects=True, vmem_limit_bytes=16 * 1024 * 1024),
        name='reduce_outputs',
    )(in_vmem(partial), in_vmem(hid_f32))


ROWS = 128
SPLIT = 2
SLOTS = 6


def expert_kernel(meta_sm, z_ref, cols_ref, rw_ref, b1_in, b2_in, w1_hbm, w2_hbm, out_ref,
                  b1_ref, b2_ref, w1_buf, w2_buf, rank_s, gate_s, x_s, o_s, sem1, sem2):
    n_tok, d_model = cols_ref.shape[0], z_ref.shape[2]
    n_loc = w1_hbm.shape[0]
    ff = w1_hbm.shape[2]
    fc = ff // SPLIT
    n_step = meta_sm[2, 0] * SPLIT

    def copies(step, slot):
        e = meta_sm[1, step // SPLIT]
        f0 = pl.multiple_of((step % SPLIT) * fc, fc)
        return (pltpu.make_async_copy(w1_hbm.at[e, :, pl.ds(f0, fc)], w1_buf.at[slot], sem1.at[slot]),
                pltpu.make_async_copy(w2_hbm.at[e, pl.ds(f0, fc), :], w2_buf.at[slot], sem2.at[slot]))

    for s in range(SLOTS):
        @pl.when(s < n_step)
        def _():
            for c in copies(s, s):
                c.start()

    b1_ref[...] = b1_in[...].astype(F32)
    b2_ref[...] = b2_in[...].astype(F32)
    z_all = z_ref[...].reshape(n_tok, d_model)
    id0, id1, lane, hit_t = named_experts(cols_ref[...], lax.axis_index('ep') * n_loc, n_loc)
    base = lax.axis_index('ep') * n_loc
    row_i = lax.broadcasted_iota(jnp.int32, (n_tok, n_tok), 0)
    col_i = lax.broadcasted_iota(jnp.int32, (n_tok, n_tok), 1)
    before = (row_i < col_i).astype(BF16)
    hit = jnp.transpose(hit_t)
    rank = jnp.dot(hit.astype(BF16), before, preferred_element_type=F32)
    rank_s[...] = jnp.where(hit > 0.5, rank, -1.0)

    logits = jnp.dot(z_all, rw_ref[...], preferred_element_type=F32)
    top = jnp.max(logits, axis=-1, keepdims=True)
    ex = jnp.exp(logits - top)
    probs = ex / jnp.sum(ex, axis=-1, keepdims=True)
    p0 = jnp.sum(jnp.where(lane == id0 + base, probs, 0.0), axis=-1, keepdims=True)
    p1 = jnp.sum(jnp.where(lane == id1 + base, probs, 0.0), axis=-1, keepdims=True)
    tot = p0 + p1
    g0, g1 = p0 / tot, p1 / tot
    gate_s[...] = jnp.where(lane == id0, g0, jnp.where(lane == id1, g1, 0.0))
    out_ref[...] = jnp.zeros_like(out_ref)

    def step_body(step, carry):
        slot = step % SLOTS
        e = meta_sm[1, step // SPLIT]
        part = step % SPLIT
        blocks = (meta_sm[0, e] + ROWS - 1) // ROWS
        slot_i = lax.broadcasted_iota(jnp.int32, (ROWS, n_tok), 0)

        def pick(j):
            want = (slot_i + j * ROWS).astype(F32)
            return (want == rank_s[pl.ds(e, 1), :]).astype(BF16)

        @pl.when(part == 0)
        def _():
            def gather_body(j, c):
                x_s[j] = jnp.dot(pick(j), z_ref[...].reshape(n_tok, d_model), preferred_element_type=F32).astype(BF16)
                o_s[j] = jnp.broadcast_to(b2_ref[pl.ds(e, 1), :], (ROWS, d_model))
                return c
            lax.fori_loop(0, blocks, gather_body, 0)

        for c in copies(step, slot):
            c.wait()
        bias = b1_ref[pl.ds(e, 1), pl.ds(pl.multiple_of(part * fc, fc), fc)]

        def block_body(j, c):
            inner = jnp.dot(x_s[j], w1_buf[slot], preferred_element_type=F32) + bias
            inner = jnp.maximum(inner, 0.0).astype(BF16)
            o_s[j] += jnp.dot(inner, w2_buf[slot], preferred_element_type=F32)
            return c
        lax.fori_loop(0, blocks, block_body, 0)

        @pl.when(step + SLOTS < n_step)
        def _():
            for c in copies(step + SLOTS, slot):
                c.start()

        @pl.when(part == SPLIT - 1)
        def _():
            lane_g = lax.broadcasted_iota(jnp.int32, (n_tok, 128), 1)
            gate = jnp.sum(jnp.where(lane_g == e, gate_s[...], 0.0), axis=-1, keepdims=True)

            def scatter_body(j, c):
                back = lax.dot_general(pick(j), o_s[j].astype(BF16), (((0,), (0,)), ((), ())), preferred_element_type=F32)
                out_ref[...] += (gate * back).reshape(out_ref.shape)
                return c
            lax.fori_loop(0, blocks, scatter_body, 0)
        return carry

    lax.fori_loop(0, n_step, step_body, 0)


def run_experts(meta, z_all, cols, router_w, exp_w1, exp_b1, exp_w2, exp_b2):
    group_n, tok, d_model = z_all.shape
    n_tok = group_n * tok
    n_loc, _, ff = exp_w1.shape
    fc = ff // SPLIT
    n_blk = n_tok // ROWS
    vm = pl.BlockSpec(memory_space=VMEM)
    hbm = pl.BlockSpec(memory_space=pl.ANY)
    return pl.pallas_call(
        expert_kernel,
        out_shape=VMEM((group_n, tok, d_model), F32),
        in_specs=[pl.BlockSpec(memory_space=pltpu.SMEM)] + [vm] * 5 + [hbm] * 2,
        out_specs=vm,
        scratch_shapes=[
            VMEM((n_loc, ff), F32), VMEM((n_loc, d_model), F32),
            VMEM((SLOTS, d_model, fc), BF16), VMEM((SLOTS, fc, d_model), BF16),
            VMEM((128, n_tok), F32), VMEM((n_tok, 128), F32),
            VMEM((n_blk, ROWS, d_model), BF16), VMEM((n_blk, ROWS, d_model), F32),
            pltpu.SemaphoreType.DMA((SLOTS,)), pltpu.SemaphoreType.DMA((SLOTS,)),
        ],
        compiler_params=pltpu.CompilerParams(vmem_limit_bytes=48 * 1024 * 1024),
        name='run_experts',
    )(meta, in_vmem(z_all), in_vmem(cols), router_w, exp_b1, exp_b2, exp_w1, exp_w2)


def solution(mesh):
    group_n = mesh.shape['ep']

    def local_step(hidden, self_pos, src_len, cache_a, cross_a, cache_b, cross_b, route_ids, ln_gain, ln_shift, attn_w, attn_b, ffn_w1, ffn_b1, ffn_w2, ffn_b2, router_w, exp_w1, exp_b1, exp_w2, exp_b2):
        hid_f32, z_bf, cache_a_new, cache_b_new = dense_layers(hidden, self_pos, src_len, cache_a, cross_a, cache_b, cross_b, ln_gain, ln_shift, attn_w, attn_b, ffn_w1, ffn_b1, ffn_w2, ffn_b2)
        z_all, cols, meta = gather_tokens(z_bf, route_ids.T, group_n, exp_w1.shape[0])
        partial = run_experts(meta, z_all, cols, router_w, exp_w1, exp_b1, exp_w2, exp_b2)
        out = reduce_outputs(partial, hid_f32)
        return out, cache_a_new, cache_b_new

    tok_spec = P(('dp', 'ep'))
    cache_spec = P(None, ('dp', 'ep'))
    rep_spec = P()
    exp_spec = P('ep')
    in_specs = (tok_spec, tok_spec, tok_spec, cache_spec, cache_spec, cache_spec, cache_spec, tok_spec) + (rep_spec,) * 9 + (exp_spec,) * 4
    out_specs = (tok_spec, cache_spec, cache_spec)
    return jax.shard_map(local_step, mesh=mesh, in_specs=in_specs, out_specs=out_specs, check_vma=False)
```

```python
import functools

import jax
import jax.numpy as jnp
from jax import lax
from jax.experimental import pallas as pl
from jax.experimental.pallas import tpu as pltpu
from jax.sharding import PartitionSpec as P

LN_EPS = 1e-5
F32 = jnp.float32
BF16 = jnp.bfloat16
VMEM = pltpu.VMEM


CROSS_GROUP = 16
SELF_GROUP = 16
SELF_UNIT = 4
HEAD_PAD = 16
PAIR_PAD = 8


def norm_rows(x_val, gain_vec, shift_vec):
    mean_val = jnp.mean(x_val, axis=-1, keepdims=True)
    centered = x_val - mean_val
    var_val = jnp.mean(centered * centered, axis=-1, keepdims=True)
    return (centered * lax.rsqrt(var_val + LN_EPS) * gain_vec + shift_vec).astype(BF16)


def dense_kernel(pos_sm, len_sm, hid_ref, gain_ref, shift_ref, ab_ref, fb1_ref, fb2_ref,
                 cache_a, cross_a, cache_b, cross_b, aw_hbm, w1_hbm, w2_hbm,
                 hid_out, z_out, cache_a_out, cache_b_out,
                 w_buf, f1_buf, f2_buf, self_buf, cross_buf, q_s, k_s, v_s, ctx_s, cat_s, lim_s, self_mask, cross_mask,
                 w_sem, f_sem, in_sem, out_sem, cross_sem):
    tok, d_model = hid_ref.shape
    n_heads, self_len, head_dim = self_buf.shape[2:]
    src = cross_buf.shape[3]
    ff = f1_buf.shape[1]
    scale = head_dim ** -0.5
    n_self = tok // SELF_GROUP

    def head_rows(b, n):
        return pl.ds(pl.multiple_of(b * HEAD_PAD, HEAD_PAD), n * HEAD_PAD)

    def weight_copy(i):
        return pltpu.make_async_copy(aw_hbm.at[i // 6, i % 6], w_buf.at[i], w_sem.at[i])

    def ffn_copies():
        return (pltpu.make_async_copy(w1_hbm, f1_buf, f_sem.at[0]), pltpu.make_async_copy(w2_hbm, f2_buf, f_sem.at[1]))

    def self_in(cache, g):
        rows = pl.ds(g * SELF_GROUP, SELF_GROUP)
        return pltpu.make_async_copy(cache.at[:, rows], self_buf.at[:, rows], in_sem.at[g])

    def self_out(cache_out, g):
        rows = pl.ds(g * SELF_GROUP, SELF_GROUP)
        return pltpu.make_async_copy(self_buf.at[:, rows], cache_out.at[:, rows], out_sem.at[g])

    def cross_rows(b):
        return pl.multiple_of(((len_sm[b] + 15) // 16) * 16, 16)

    def cross_copy(cross, b):
        rows = pl.ds(0, cross_rows(b))
        return pltpu.make_async_copy(cross.at[:, b, :, rows, :], cross_buf.at[b, :, :, rows, :], cross_sem.at[b])

    for i in range(3):
        weight_copy(i).start()
    for g in range(n_self):
        self_in(cache_a, g).start()
    weight_copy(3).start()
    weight_copy(4).start()

    def first_cross(b, c):
        cross_copy(cross_a, b).start()
        return c
    lax.fori_loop(0, tok, first_cross, 0)
    weight_copy(5).start()
    for cp in ffn_copies():
        cp.start()
    for i in range(6, 12):
        weight_copy(i).start()

    def zero_tail(b, c):
        def zero_part(part, c2):
            cross_buf[b, 1, :, pl.ds(pl.multiple_of(part * 16, 16), 16), :] = jnp.zeros((n_heads, 16, head_dim), BF16)
            return c2
        return lax.fori_loop(cross_rows(b) // 16, src // 16, zero_part, c)
    lax.fori_loop(0, tok, zero_tail, 0)

    n_pairs = n_heads // 2
    wide = 2 * head_dim

    def build_mask(ref, length):
        row = lax.broadcasted_iota(jnp.int32, ref.shape, 0)
        lane = lax.broadcasted_iota(jnp.int32, ref.shape, 1)
        seq, pair = lane // (n_pairs * length), (lane // length) % n_pairs
        same = jnp.logical_and(seq == row // HEAD_PAD, pair == (row % HEAD_PAD) // 2)
        ref[...] = jnp.where(same, lane % length, 1 << 20)
    build_mask(self_mask, self_len)
    build_mask(cross_mask, src)

    def fill_limit(b, c):
        lim_s[head_rows(b, 1), :] = jnp.full((HEAD_PAD, 128), pos_sm[b] + 1, jnp.int32)
        return c
    lax.fori_loop(0, tok, fill_limit, 0)

    even_half = lax.broadcasted_iota(jnp.int32, (tok, wide), 1) < head_dim

    def pairs_of(val):
        val = val.astype(BF16).astype(F32)
        return [val[:, j * wide:(j + 1) * wide] for j in range(n_pairs)]

    def to_heads(ref, val):
        for j, two in enumerate(pairs_of(val)):
            ref[pl.ds(2 * j, tok, stride=HEAD_PAD), :] = jnp.where(even_half, two, 0.0)
            ref[pl.ds(2 * j + 1, tok, stride=HEAD_PAD), :] = jnp.where(even_half, 0.0, two)

    def to_pairs(ref, val):
        for j, two in enumerate(pairs_of(val)):
            ref[pl.ds(j, tok, stride=PAIR_PAD), :] = two

    def from_heads(ref):
        for j in range(n_pairs):
            two = jnp.where(even_half, ref[pl.ds(2 * j, tok, stride=HEAD_PAD), :], ref[pl.ds(2 * j + 1, tok, stride=HEAD_PAD), :])
            cat_s[:, j * wide:(j + 1) * wide] = two.astype(BF16)
        return cat_s[...]

    def softmax_rows(scores, mask, limit):
        scores = jnp.where(mask < limit, scores * scale, -1e30)
        top = jnp.max(scores, axis=-1, keepdims=True)
        ex = jnp.exp(scores - top)
        return (ex * (1.0 / jnp.sum(ex, axis=-1, keepdims=True))).astype(BF16)

    def scores_of(q, keys):
        return lax.dot_general(q, keys, (((1,), (1,)), ((), ())), preferred_element_type=F32)

    def proj(layer, i, x_bf):
        weight_copy(layer * 6 + i).wait()
        bias = ab_ref[i].astype(F32)[layer:layer + 1, :]
        return jnp.dot(x_bf, w_buf[layer * 6 + i], preferred_element_type=F32) + bias

    def self_layer(layer, h, cache, cache_out):
        x = norm_rows(h, gain_ref[0, layer:layer + 1, :], shift_ref[0, layer:layer + 1, :])
        to_heads(q_s, proj(layer, 0, x))
        to_pairs(k_s, proj(layer, 1, x))
        to_pairs(v_s, proj(layer, 2, x))
        row_i = lax.broadcasted_iota(jnp.int32, (self_len, wide), 0)
        row_b = row_i.astype(F32).astype(BF16)

        def body(g, c):
            self_in(cache, g).wait()
            first = g * SELF_GROUP
            sides = []
            for which, new in ((0, k_s), (1, v_s)):
                tiles = []
                for u in range(SELF_GROUP):
                    b = first + u
                    hit = row_b == jnp.full(row_b.shape, pos_sm[b], jnp.int32).astype(F32).astype(BF16)
                    for j in range(n_pairs):
                        row = new[pl.ds(b * PAIR_PAD + j, self_len, stride=0), :].astype(BF16)
                        two = jnp.concatenate([self_buf[which, b, 2 * j], self_buf[which, b, 2 * j + 1]], axis=1)
                        two = jnp.where(hit, row, two)
                        self_buf[which, b, 2 * j] = two[:, :head_dim]
                        self_buf[which, b, 2 * j + 1] = two[:, head_dim:]
                        tiles.append(two)
                sides.append(tiles)
            n = SELF_UNIT
            parts = range(0, SELF_GROUP, n)
            stack = lambda tiles, p: jnp.concatenate(tiles[p * n_pairs:(p + n) * n_pairs], axis=0)
            scores = [scores_of(q_s[head_rows(first + p, n), :].astype(BF16), stack(sides[0], p)) for p in parts]
            probs = []
            for p, sc in zip(parts, scores):
                lim = lim_s[head_rows(first + p, n), :]
                lim = jnp.concatenate([lim] * (sc.shape[1] // 128), axis=1)
                probs.append(softmax_rows(sc, self_mask[...], lim))
            for p, pr in zip(parts, probs):
                ctx_s[head_rows(first + p, n), :] = jnp.dot(pr, stack(sides[1], p), preferred_element_type=F32)
            self_out(cache_out, g).start()
            return c
        lax.fori_loop(0, n_self, body, 0)
        ctx = from_heads(ctx_s)
        return h + proj(layer, 3, ctx)

    def cross_layer(layer, h, cross, after):
        x = norm_rows(h, gain_ref[1, layer:layer + 1, :], shift_ref[1, layer:layer + 1, :])
        to_heads(q_s, proj(layer, 4, x))

        def body(g, c):
            first = g * CROSS_GROUP
            for u in range(CROSS_GROUP):
                cross_copy(cross, first + u).wait()
            def side(b, which):
                return jnp.concatenate([jnp.concatenate([cross_buf[b, which, 2 * j], cross_buf[b, which, 2 * j + 1]], axis=1) for j in range(n_pairs)], axis=0)

            group = [first + u for u in range(CROSS_GROUP)]
            scores = [scores_of(q_s[head_rows(b, 1), :].astype(BF16), side(b, 0)) for b in group]
            probs = [softmax_rows(sc, cross_mask[...], len_sm[b]) for b, sc in zip(group, scores)]
            for b, pr in zip(group, probs):
                ctx_s[head_rows(b, 1), :] = jnp.dot(pr, side(b, 1), preferred_element_type=F32)
            if after is not None:
                for u in range(CROSS_GROUP):
                    cross_copy(after, first + u).start()
            return c
        lax.fori_loop(0, tok // CROSS_GROUP, body, 0)
        ctx = from_heads(ctx_s)
        return h + proj(layer, 5, ctx)

    q_s[...] = jnp.zeros_like(q_s)
    h = hid_ref[...].astype(F32)
    h = self_layer(0, h, cache_a, cache_a_out)
    for g in range(n_self):
        self_out(cache_a_out, g).wait()
        self_in(cache_b, g).start()
    h = cross_layer(0, h, cross_a, cross_b)
    x = norm_rows(h, gain_ref[2, 0:1, :], shift_ref[2, 0:1, :])
    for cp in ffn_copies():
        cp.wait()
    acc = h + fb2_ref[...].astype(F32).reshape(1, d_model)
    for f in range(0, ff, d_model):
        inner = jnp.dot(x, f1_buf[:, f:f + d_model], preferred_element_type=F32) + fb1_ref[f:f + d_model].astype(F32).reshape(1, d_model)
        inner = jnp.maximum(inner, 0.0).astype(BF16)
        acc = acc + jnp.dot(inner, f2_buf[f:f + d_model, :], preferred_element_type=F32)
    h = acc
    h = self_layer(1, h, cache_b, cache_b_out)
    h = cross_layer(1, h, cross_b, None)
    hid_out[...] = h
    z_out[...] = norm_rows(h, gain_ref[2, 1:2, :], shift_ref[2, 1:2, :])
    for g in range(n_self):
        self_out(cache_b_out, g).wait()


def dense_layers(hidden, self_pos, src_len, cache_a, cross_a, cache_b, cross_b, ln_gain, ln_shift, attn_w, attn_b, ffn_w1, ffn_b1, ffn_w2, ffn_b2):
    tok, d_model = hidden.shape
    n_heads, head_dim = cache_a.shape[3:]
    self_len, src = cache_a.shape[2], cross_a.shape[2]
    ff = ffn_w1.shape[1]
    swap = lambda arr: jnp.swapaxes(arr, 2, 3)
    sm = pl.BlockSpec(memory_space=pltpu.SMEM)
    vm = pl.BlockSpec(memory_space=VMEM)
    hbm = pl.BlockSpec(memory_space=pl.ANY)
    cache_t = jax.ShapeDtypeStruct((2, tok, n_heads, self_len, head_dim), BF16)
    n_self = tok // SELF_GROUP
    heads = VMEM((tok * HEAD_PAD, 2 * head_dim), F32)
    pairs = VMEM((tok * PAIR_PAD, 2 * head_dim), F32)
    half = n_heads // 2
    hid, z, out_a, out_b = pl.pallas_call(
        dense_kernel,
        out_shape=[VMEM((tok, d_model), F32), VMEM((tok, d_model), BF16), cache_t, cache_t],
        in_specs=[sm] * 2 + [vm] * 6 + [hbm] * 7,
        out_specs=[vm] * 2 + [hbm] * 2,
        scratch_shapes=[
            VMEM((12, d_model, d_model), BF16), VMEM((d_model, ff), BF16), VMEM((ff, d_model), BF16),
            VMEM((2, tok, n_heads, self_len, head_dim), BF16), VMEM((tok, 2, n_heads, src, head_dim), BF16),
            heads, pairs, pairs, heads, VMEM((tok, d_model), BF16), VMEM((tok * HEAD_PAD, 128), jnp.int32),
            VMEM((SELF_UNIT * HEAD_PAD, SELF_UNIT * half * self_len), jnp.int32), VMEM((HEAD_PAD, half * src), jnp.int32),
            pltpu.SemaphoreType.DMA((12,)), pltpu.SemaphoreType.DMA((2,)), pltpu.SemaphoreType.DMA((n_self,)),
            pltpu.SemaphoreType.DMA((n_self,)), pltpu.SemaphoreType.DMA((tok,)),
        ],
        compiler_params=pltpu.CompilerParams(vmem_limit_bytes=61 * 1024 * 1024),
        name='dense_layers',
    )(self_pos, src_len, hidden, jnp.swapaxes(ln_gain, 0, 1), jnp.swapaxes(ln_shift, 0, 1), jnp.swapaxes(attn_b, 0, 1), ffn_b1, ffn_b2,
      swap(cache_a), swap(cross_a), swap(cache_b), swap(cross_b), attn_w, ffn_w1, ffn_w2)
    return hid, z, swap(out_a), swap(out_b)


def peer(index):
    return dict(device_id={'ep': index}, device_id_type=pl.DeviceIdType.MESH)


def neighbours():
    me = lax.axis_index('ep')
    core, x, y = me % 2, (me // 2) % 2, me // 4
    at = lambda yy, xx, cc: (yy * 2 + xx) * 2 + cc
    return me, core, x, y, at


def entry_barrier(others):
    barrier = pltpu.get_barrier_semaphore()
    for other in others:
        pl.semaphore_signal(barrier, inc=1, **peer(other))
    pl.semaphore_wait(barrier, len(others))


def named_experts(ids_cols, base, n_loc):
    n_tok = ids_cols.shape[0]
    lane = lax.broadcasted_iota(jnp.int32, (n_tok, 128), 1)
    id0 = ids_cols[:, 0:1].astype(jnp.int32) - base
    id1 = ids_cols[:, 1:2].astype(jnp.int32) - base
    hit = jnp.logical_and(jnp.logical_or(id0 == lane, id1 == lane), lane < n_loc)
    return id0, id1, lane, hit.astype(F32)


def gather_kernel(n_loc, z_ref, idst_ref, zall_ref, cols_ref, meta_ref, flip, ids_ref, idsall, send_sem, recv_sem):
    me, core, x, y, at = neighbours()
    twin = at(y, x, 1 - core)
    chips = [(y, 1 - x), (1 - y, x), (1 - y, 1 - x)]
    tok = z_ref.shape[0]
    group_n = zall_ref.shape[0]
    ids_ref[...] = jnp.zeros_like(ids_ref)
    ids_ref[0:2, 0:tok] = idst_ref[...].astype(F32)
    entry_barrier([twin] + [at(cy, cx, core) for cy, cx in chips])

    def send(slot, which, src, row, to):
        dst = (idsall, zall_ref)[which]
        cp = pltpu.make_async_remote_copy(
            src_ref=src, dst_ref=dst.at[row], send_sem=send_sem.at[slot, which], recv_sem=recv_sem.at[slot, which], **peer(to))
        cp.start()
        return cp

    far = [at(cy, cx, core) for cy, cx in chips]
    ids_sent = [send(j, 0, ids_ref, me, far[j]) for j in range(3)] + [send(3, 0, ids_ref, me, twin)]
    z_sent = {j: send(j, 1, z_ref, me, far[j]) for j in (2, 0, 1)}
    z_sent[3] = send(3, 1, z_ref, me, twin)
    zall_ref[me] = z_ref[...]
    idsall[me] = ids_ref[...]
    relays = []
    for j in range(3):
        ids_sent[j].wait_recv()
        relays.append(send(4 + j, 0, idsall.at[far[j]], far[j], twin))
    ids_sent[3].wait_recv()
    for cp in relays:
        cp.wait_recv()

    flip[...] = jnp.zeros_like(flip)
    for d in range(group_n):
        flip[2 * d:2 * d + 2, :] = idsall[d, 0:2, :]
    cols = jnp.transpose(flip[...])[:tok]
    lane_b = lax.broadcasted_iota(jnp.int32, (tok, 128), 1)
    wide = [jnp.where(lane_b == 0, cols[:, 2 * d:2 * d + 1], cols[:, 2 * d + 1:2 * d + 2]) for d in range(group_n)]
    cols_ref[...] = jnp.concatenate(wide, axis=0)
    _, _, _, hit = named_experts(cols_ref[...], me * n_loc, n_loc)
    ones = jnp.ones((group_n * tok, 128), BF16)
    count = lax.dot_general(hit.astype(BF16), ones, (((0,), (0,)), ((), ())), preferred_element_type=F32)
    row_i = lax.broadcasted_iota(jnp.int32, (128, 128), 0)
    col_i = lax.broadcasted_iota(jnp.int32, (128, 128), 1)
    named = (count > 0.5).astype(F32)
    order = jnp.dot((row_i > col_i).astype(BF16), named.astype(BF16), preferred_element_type=F32)
    spot = jnp.where(order == col_i.astype(F32), named, 0.0)
    expert_list = jnp.sum(spot * row_i.astype(F32), axis=0, keepdims=True)
    counts = jnp.sum(hit, axis=0, keepdims=True)
    total = jnp.sum(named, axis=0, keepdims=True)
    meta_ref[...] = jnp.concatenate([counts, expert_list, total, jnp.zeros((5, 128), F32)], axis=0).astype(jnp.int32)

    z_relays = []
    for j in (0, 1, 2):
        z_sent[j].wait_recv()
        z_relays.append(send(4 + j, 1, zall_ref.at[far[j]], far[j], twin))
    z_sent[3].wait_recv()
    for cp in z_relays:
        cp.wait_recv()
    for cp in ids_sent + relays + list(z_sent.values()) + z_relays:
        cp.wait_send()


def in_vmem(arr):
    return pltpu.with_memory_space_constraint(arr, VMEM)


def gather_tokens(z_bf, ids_t, group_n, n_loc):
    tok, d_model = z_bf.shape
    return pl.pallas_call(
        functools.partial(gather_kernel, n_loc),
        out_shape=[VMEM((group_n, tok, d_model), BF16), VMEM((group_n * tok, 128), F32), jax.ShapeDtypeStruct((8, 128), jnp.int32)],
        in_specs=[pl.BlockSpec(memory_space=VMEM)] * 2,
        out_specs=[pl.BlockSpec(memory_space=VMEM)] * 3,
        scratch_shapes=[VMEM((128, 128), F32), VMEM((8, 128), F32), VMEM((group_n, 8, 128), F32),
                        pltpu.SemaphoreType.DMA((7, 2)), pltpu.SemaphoreType.DMA((7, 2))],
        compiler_params=pltpu.CompilerParams(collective_id=0, has_side_effects=True, vmem_limit_bytes=16 * 1024 * 1024),
        name='gather_tokens',
    )(in_vmem(z_bf), ids_t)


def reduce_kernel(part_ref, hid_ref, out_ref, r1, s1, r2, s2, r3, send_sem, recv_sem):
    me, core, x, y, at = neighbours()
    twin, xn, yn = at(y, x, 1 - core), at(y, 1 - x, core), at(1 - y, x, core)
    entry_barrier([twin, xn, yn])
    half = hid_ref.shape[1] // 2
    cols = (pl.ds(0, half), pl.ds(half, half))

    def send(slot, src, dst, to):
        cp = pltpu.make_async_remote_copy(src_ref=src, dst_ref=dst, send_sem=send_sem.at[slot], recv_sem=recv_sem.at[slot], **peer(to))
        cp.start()
        return cp

    chips = [(1 - y, 1 - x), (y, 1 - x), (1 - y, x), (y, x)]
    first = [send(k, part_ref.at[at(cy, cx, 1 - core)], r1.at[k], twin) for k, (cy, cx) in enumerate(chips)]

    def sum1(k):
        first[k].wait_recv()
        cy, cx = chips[k]
        s1[k] = part_ref[at(cy, cx, core)] + r1[k]

    sum1(0)
    a0 = send(4, s1.at[0, :, cols[0]], r2.at[0, 0], xn)
    b0 = send(5, s1.at[0, :, cols[1]], r2.at[1, 0], yn)
    sum1(1)
    a1 = send(6, s1.at[1, :, cols[0]], r2.at[0, 1], xn)
    sum1(2)
    b1 = send(7, s1.at[2, :, cols[1]], r2.at[1, 1], yn)
    sum1(3)
    a0.wait_recv()
    s2[0] = s1[2, :, :half] + r2[0, 0]
    a2 = send(8, s2.at[0], r3.at[0], yn)
    b0.wait_recv()
    s2[1] = s1[1, :, half:] + r2[1, 0]
    b2 = send(9, s2.at[1], r3.at[1], xn)
    a1.wait_recv()
    own_a = hid_ref[:, :half] + s1[3, :, :half] + r2[0, 1]
    b1.wait_recv()
    own_b = hid_ref[:, half:] + s1[3, :, half:] + r2[1, 1]
    a2.wait_recv()
    out_ref[:, :half] = (own_a + r3[0]).astype(BF16)
    b2.wait_recv()
    out_ref[:, half:] = (own_b + r3[1]).astype(BF16)
    for cp in first + [a0, b0, a1, b1, a2, b2]:
        cp.wait_send()


def reduce_outputs(partial, hid_f32):
    group_n, tok, d_model = partial.shape
    half = d_model // 2
    return pl.pallas_call(
        reduce_kernel,
        out_shape=VMEM((tok, d_model), BF16),
        in_specs=[pl.BlockSpec(memory_space=VMEM)] * 2,
        out_specs=pl.BlockSpec(memory_space=VMEM),
        scratch_shapes=[
            VMEM((4, tok, d_model), F32), VMEM((4, tok, d_model), F32),
            VMEM((2, 2, tok, half), F32), VMEM((2, tok, half), F32), VMEM((2, tok, half), F32),
            pltpu.SemaphoreType.DMA((10,)), pltpu.SemaphoreType.DMA((10,)),
        ],
        compiler_params=pltpu.CompilerParams(collective_id=1, has_side_effects=True, vmem_limit_bytes=16 * 1024 * 1024),
        name='reduce_outputs',
    )(in_vmem(partial), in_vmem(hid_f32))


ROWS = 128
SPLIT = 2
SLOTS = 6


def expert_kernel(meta_sm, z_ref, cols_ref, rw_ref, b1_in, b2_in, w1_hbm, w2_hbm, out_ref,
                  b1_ref, b2_ref, w1_buf, w2_buf, rank_s, gate_s, x_s, o_s, sem1, sem2):
    n_tok, d_model = cols_ref.shape[0], z_ref.shape[2]
    n_loc = w1_hbm.shape[0]
    ff = w1_hbm.shape[2]
    fc = ff // SPLIT
    n_step = meta_sm[2, 0] * SPLIT

    def copies(step, slot):
        e = meta_sm[1, step // SPLIT]
        f0 = pl.multiple_of((step % SPLIT) * fc, fc)
        return (pltpu.make_async_copy(w1_hbm.at[e, :, pl.ds(f0, fc)], w1_buf.at[slot], sem1.at[slot]),
                pltpu.make_async_copy(w2_hbm.at[e, pl.ds(f0, fc), :], w2_buf.at[slot], sem2.at[slot]))

    for s in range(SLOTS):
        @pl.when(s < n_step)
        def _():
            for c in copies(s, s):
                c.start()

    b1_ref[...] = b1_in[...].astype(F32)
    b2_ref[...] = b2_in[...].astype(F32)
    z_all = z_ref[...].reshape(n_tok, d_model)
    id0, id1, lane, hit_t = named_experts(cols_ref[...], lax.axis_index('ep') * n_loc, n_loc)
    base = lax.axis_index('ep') * n_loc
    row_i = lax.broadcasted_iota(jnp.int32, (n_tok, n_tok), 0)
    col_i = lax.broadcasted_iota(jnp.int32, (n_tok, n_tok), 1)
    before = (row_i < col_i).astype(BF16)
    hit = jnp.transpose(hit_t)
    rank = jnp.dot(hit.astype(BF16), before, preferred_element_type=F32)
    rank_s[...] = jnp.where(hit > 0.5, rank, -1.0)

    logits = jnp.dot(z_all, rw_ref[...], preferred_element_type=F32)
    top = jnp.max(logits, axis=-1, keepdims=True)
    ex = jnp.exp(logits - top)
    probs = ex / jnp.sum(ex, axis=-1, keepdims=True)
    p0 = jnp.sum(jnp.where(lane == id0 + base, probs, 0.0), axis=-1, keepdims=True)
    p1 = jnp.sum(jnp.where(lane == id1 + base, probs, 0.0), axis=-1, keepdims=True)
    tot = p0 + p1
    g0, g1 = p0 / tot, p1 / tot
    gate_s[...] = jnp.where(lane == id0, g0, jnp.where(lane == id1, g1, 0.0))
    out_ref[...] = jnp.zeros_like(out_ref)

    def step_body(step, carry):
        slot = step % SLOTS
        e = meta_sm[1, step // SPLIT]
        part = step % SPLIT
        blocks = (meta_sm[0, e] + ROWS - 1) // ROWS
        slot_i = lax.broadcasted_iota(jnp.int32, (ROWS, n_tok), 0)

        def pick(j):
            want = (slot_i + j * ROWS).astype(F32)
            return (want == rank_s[pl.ds(e, 1), :]).astype(BF16)

        @pl.when(part == 0)
        def _():
            def gather_body(j, c):
                x_s[j] = jnp.dot(pick(j), z_ref[...].reshape(n_tok, d_model), preferred_element_type=F32).astype(BF16)
                o_s[j] = jnp.broadcast_to(b2_ref[pl.ds(e, 1), :], (ROWS, d_model))
                return c
            lax.fori_loop(0, blocks, gather_body, 0)

        for c in copies(step, slot):
            c.wait()
        bias = b1_ref[pl.ds(e, 1), pl.ds(pl.multiple_of(part * fc, fc), fc)]

        def block_body(j, c):
            inner = jnp.dot(x_s[j], w1_buf[slot], preferred_element_type=F32) + bias
            inner = jnp.maximum(inner, 0.0).astype(BF16)
            o_s[j] += jnp.dot(inner, w2_buf[slot], preferred_element_type=F32)
            return c
        lax.fori_loop(0, blocks, block_body, 0)

        @pl.when(step + SLOTS < n_step)
        def _():
            for c in copies(step + SLOTS, slot):
                c.start()

        @pl.when(part == SPLIT - 1)
        def _():
            lane_g = lax.broadcasted_iota(jnp.int32, (n_tok, 128), 1)
            gate = jnp.sum(jnp.where(lane_g == e, gate_s[...], 0.0), axis=-1, keepdims=True)

            def scatter_body(j, c):
                back = lax.dot_general(pick(j), o_s[j].astype(BF16), (((0,), (0,)), ((), ())), preferred_element_type=F32)
                out_ref[...] += (gate * back).reshape(out_ref.shape)
                return c
            lax.fori_loop(0, blocks, scatter_body, 0)
        return carry

    lax.fori_loop(0, n_step, step_body, 0)


def run_experts(meta, z_all, cols, router_w, exp_w1, exp_b1, exp_w2, exp_b2):
    group_n, tok, d_model = z_all.shape
    n_tok = group_n * tok
    n_loc, _, ff = exp_w1.shape
    fc = ff // SPLIT
    n_blk = n_tok // ROWS
    vm = pl.BlockSpec(memory_space=VMEM)
    hbm = pl.BlockSpec(memory_space=pl.ANY)
    return pl.pallas_call(
        expert_kernel,
        out_shape=VMEM((group_n, tok, d_model), F32),
        in_specs=[pl.BlockSpec(memory_space=pltpu.SMEM)] + [vm] * 5 + [hbm] * 2,
        out_specs=vm,
        scratch_shapes=[
            VMEM((n_loc, ff), F32), VMEM((n_loc, d_model), F32),
            VMEM((SLOTS, d_model, fc), BF16), VMEM((SLOTS, fc, d_model), BF16),
            VMEM((128, n_tok), F32), VMEM((n_tok, 128), F32),
            VMEM((n_blk, ROWS, d_model), BF16), VMEM((n_blk, ROWS, d_model), F32),
            pltpu.SemaphoreType.DMA((SLOTS,)), pltpu.SemaphoreType.DMA((SLOTS,)),
        ],
        compiler_params=pltpu.CompilerParams(vmem_limit_bytes=48 * 1024 * 1024),
        name='run_experts',
    )(meta, in_vmem(z_all), in_vmem(cols), router_w, exp_b1, exp_b2, exp_w1, exp_w2)


def solution(mesh):
    group_n = mesh.shape['ep']

    def local_step(hidden, self_pos, src_len, cache_a, cross_a, cache_b, cross_b, route_ids, ln_gain, ln_shift, attn_w, attn_b, ffn_w1, ffn_b1, ffn_w2, ffn_b2, router_w, exp_w1, exp_b1, exp_w2, exp_b2):
        hid_f32, z_bf, cache_a_new, cache_b_new = dense_layers(hidden, self_pos, src_len, cache_a, cross_a, cache_b, cross_b, ln_gain, ln_shift, attn_w, attn_b, ffn_w1, ffn_b1, ffn_w2, ffn_b2)
        z_all, cols, meta = gather_tokens(z_bf, route_ids.T, group_n, exp_w1.shape[0])
        partial = run_experts(meta, z_all, cols, router_w, exp_w1, exp_b1, exp_w2, exp_b2)
        out = reduce_outputs(partial, hid_f32)
        return out, cache_a_new, cache_b_new

    tok_spec = P(('dp', 'ep'))
    cache_spec = P(None, ('dp', 'ep'))
    rep_spec = P()
    exp_spec = P('ep')
    in_specs = (tok_spec, tok_spec, tok_spec, cache_spec, cache_spec, cache_spec, cache_spec, tok_spec) + (rep_spec,) * 9 + (exp_spec,) * 4
    out_specs = (tok_spec, cache_spec, cache_spec)
    return jax.shard_map(local_step, mesh=mesh, in_specs=in_specs, out_specs=out_specs, check_vma=False)
```

```python
import functools

import jax
import jax.numpy as jnp
from jax import lax
from jax.experimental import pallas as pl
from jax.experimental.pallas import tpu as pltpu
from jax.sharding import PartitionSpec as P

LN_EPS = 1e-5
F32 = jnp.float32
BF16 = jnp.bfloat16
VMEM = pltpu.VMEM


CROSS_GROUP = 16
ROW_STEP = 16
SELF_GROUP = 16
SELF_UNIT = 2
HEAD_PAD = 16


def norm_rows(x_val, gain_vec, shift_vec):
    mean_val = jnp.mean(x_val, axis=-1, keepdims=True)
    centered = x_val - mean_val
    var_val = jnp.mean(centered * centered, axis=-1, keepdims=True)
    return (centered * lax.rsqrt(var_val + LN_EPS) * gain_vec + shift_vec).astype(BF16)


def dense_kernel(pos_sm, len_sm, hid_ref, gain_ref, shift_ref, ab_ref, fb1_ref, fb2_ref,
                 cache_a, cross_a, cache_b, cross_b, aw_hbm, w1_hbm, w2_hbm,
                 hid_out, z_out, cache_a_out, cache_b_out,
                 w_buf, f1_buf, f2_buf, self_buf, cross_buf, q_s, k_s, v_s, ctx_s, cat_s, lim_s, self_mask, mask_1, mask_2, mask_3, mask_4, order_sm, place_sm,
                 w_sem, f_sem, in_sem, out_sem, cross_sem):
    tok, d_model = hid_ref.shape
    n_heads, self_len, head_dim = self_buf.shape[2:]
    src = cross_buf.shape[3]
    ff = f1_buf.shape[1]
    scale = head_dim ** -0.5
    cross_masks = (mask_1, mask_2, mask_3, mask_4)
    n_class = len(cross_masks)
    n_self = tok // SELF_GROUP

    def head_rows(b, n):
        return pl.ds(pl.multiple_of(b * HEAD_PAD, HEAD_PAD), n * HEAD_PAD)

    def weight_copy(i):
        return pltpu.make_async_copy(aw_hbm.at[i // 6, i % 6], w_buf.at[i], w_sem.at[i])

    def ffn_copies():
        return (pltpu.make_async_copy(w1_hbm, f1_buf, f_sem.at[0]), pltpu.make_async_copy(w2_hbm, f2_buf, f_sem.at[1]))

    def self_in(cache, g):
        rows = pl.ds(g * SELF_GROUP, SELF_GROUP)
        return pltpu.make_async_copy(cache.at[:, rows], self_buf.at[:, rows], in_sem.at[g])

    def self_out(cache_out, g):
        rows = pl.ds(g * SELF_GROUP, SELF_GROUP)
        return pltpu.make_async_copy(self_buf.at[:, rows], cache_out.at[:, rows], out_sem.at[g])

    def cross_rows(b):
        return pl.multiple_of(((len_sm[b] + 15) // 16) * 16, 16)

    def length_class(b):
        return (len_sm[b] + (ROW_STEP - 1)) // ROW_STEP - 1

    def sort_by_length():
        for k in range(n_class):
            place_sm[k] = 0

        def count(b, c):
            k = length_class(b)
            place_sm[k] = place_sm[k] + 1
            return c
        lax.fori_loop(0, tok, count, 0)
        start = 0
        for k in range(n_class):
            here = place_sm[k]
            place_sm[k] = start
            start = start + here

        def put(b, c):
            k = length_class(b)
            order_sm[place_sm[k]] = b
            place_sm[k] = place_sm[k] + 1
            return c
        lax.fori_loop(0, tok, put, 0)

    def cross_copy(cross, b):
        rows = pl.ds(0, cross_rows(b))
        return pltpu.make_async_copy(cross.at[:, b, :, rows, :], cross_buf.at[b, :, :, rows, :], cross_sem.at[b])

    for i in range(3):
        weight_copy(i).start()
    for g in range(n_self):
        self_in(cache_a, g).start()
    weight_copy(3).start()
    weight_copy(4).start()

    sort_by_length()

    def first_cross(i, c):
        cross_copy(cross_a, order_sm[i]).start()
        return c
    lax.fori_loop(0, tok, first_cross, 0)
    weight_copy(5).start()
    for cp in ffn_copies():
        cp.start()
    for i in range(6, 12):
        weight_copy(i).start()

    def zero_tail(b, c):
        def zero_part(part, c2):
            cross_buf[b, 1, :, pl.ds(pl.multiple_of(part * 16, 16), 16), :] = jnp.zeros((n_heads, 16, head_dim), BF16)
            return c2
        return lax.fori_loop(cross_rows(b) // 16, src // 16, zero_part, c)
    lax.fori_loop(0, tok, zero_tail, 0)

    def build_mask(ref, length):
        row = lax.broadcasted_iota(jnp.int32, ref.shape, 0)
        lane = lax.broadcasted_iota(jnp.int32, ref.shape, 1)
        seq, head = lane // (n_heads * length), (lane // length) % n_heads
        ref[...] = jnp.where(seq * HEAD_PAD + head == row, lane % length, 1 << 20)
    build_mask(self_mask, self_len)
    for mask in cross_masks:
        build_mask(mask, mask.shape[1] // n_heads)

    def fill_limit(b, c):
        lim_s[head_rows(b, 1), :] = jnp.full((HEAD_PAD, 128), pos_sm[b] + 1, jnp.int32)
        return c
    lax.fori_loop(0, tok, fill_limit, 0)

    def to_heads(ref, val):
        val = val.astype(BF16).astype(F32)
        for h in range(n_heads):
            ref[pl.ds(h, tok, stride=HEAD_PAD), :] = val[:, h * head_dim:(h + 1) * head_dim]

    def from_heads(ref):
        for h in range(0, n_heads, 2):
            two = [ref[pl.ds(h + k, tok, stride=HEAD_PAD), :] for k in range(2)]
            cat_s[:, h * head_dim:(h + 2) * head_dim] = jnp.concatenate(two, axis=1).astype(BF16)
        return cat_s[...]

    def softmax_rows(scores, mask, limit):
        scores = jnp.where(mask < limit, scores * scale, -1e30)
        top = jnp.max(scores, axis=-1, keepdims=True)
        ex = jnp.exp(scores - top)
        return (ex * (1.0 / jnp.sum(ex, axis=-1, keepdims=True))).astype(BF16)

    def scores_of(q, keys):
        return lax.dot_general(q, keys, (((1,), (1,)), ((), ())), preferred_element_type=F32)

    def block_diag(blocks):
        rows = []
        for k, blk in enumerate(blocks):
            pad = jnp.zeros_like(blk)
            rows.append(jnp.concatenate([blk if j == k else pad for j in range(len(blocks))], axis=1))
        return jnp.concatenate(rows, axis=0)

    def proj(layer, i, x_bf):
        weight_copy(layer * 6 + i).wait()
        bias = ab_ref[i].astype(F32)[layer:layer + 1, :]
        return jnp.dot(x_bf, w_buf[layer * 6 + i], preferred_element_type=F32) + bias

    def self_layer(layer, h, cache, cache_out):
        x = norm_rows(h, gain_ref[0, layer:layer + 1, :], shift_ref[0, layer:layer + 1, :])
        to_heads(q_s, proj(layer, 0, x))
        to_heads(k_s, proj(layer, 1, x))
        to_heads(v_s, proj(layer, 2, x))
        row_i = lax.broadcasted_iota(jnp.int32, (self_len, head_dim), 0)
        row_b = row_i.astype(F32).astype(BF16)

        def body(g, c):
            self_in(cache, g).wait()
            first = g * SELF_GROUP
            sides = []
            for which, new in ((0, k_s), (1, v_s)):
                tiles = []
                for u in range(SELF_GROUP):
                    b = first + u
                    hit = row_b == jnp.full(row_b.shape, pos_sm[b], jnp.int32).astype(F32).astype(BF16)
                    for hd in range(n_heads):
                        row = new[pl.ds(b * HEAD_PAD + hd, self_len, stride=0), :]
                        tile = jnp.where(hit, row.astype(BF16), self_buf[which, b, hd])
                        self_buf[which, b, hd] = tile
                        tiles.append(tile)
                sides.append(tiles)
            n = SELF_UNIT
            parts = range(0, SELF_GROUP, n)
            wide = n * n_heads * self_len
            stack = lambda tiles, p: jnp.concatenate(tiles[p * n_heads:(p + n) * n_heads], axis=0)
            scores = [scores_of(q_s[head_rows(first + p, n), :].astype(BF16), stack(sides[0], p)) for p in parts]
            probs = []
            for p, sc in zip(parts, scores):
                two = 2 * n_heads * self_len
                blocks = []
                for k in range(n // 2):
                    lim = lim_s[head_rows(first + p + 2 * k, 2), :]
                    lim = jnp.concatenate([lim] * (two // 128), axis=1)
                    blocks.append(softmax_rows(sc[k * 2 * HEAD_PAD:(k + 1) * 2 * HEAD_PAD, k * two:(k + 1) * two], self_mask[...], lim))
                probs.append(block_diag(blocks))
            for p, pr in zip(parts, probs):
                ctx_s[head_rows(first + p, n), :] = jnp.dot(pr, stack(sides[1], p), preferred_element_type=F32)
            self_out(cache_out, g).start()
            return c
        lax.fori_loop(0, n_self, body, 0)
        ctx = from_heads(ctx_s)
        return h + proj(layer, 3, ctx)

    def cross_layer(layer, h, cross, after):
        x = norm_rows(h, gain_ref[1, layer:layer + 1, :], shift_ref[1, layer:layer + 1, :])
        to_heads(q_s, proj(layer, 4, x))

        def body(g, c):
            group = [order_sm[g * CROSS_GROUP + u] for u in range(CROSS_GROUP)]
            longest = length_class(group[-1])
            for b in group:
                cross_copy(cross, b).wait()
            for k, mask in enumerate(cross_masks):
                @pl.when(longest == k)
                def _():
                    rows = mask.shape[1] // n_heads
                    side = lambda b, which: cross_buf[b, which, :, 0:rows, :].reshape(n_heads * rows, head_dim)
                    scores = [scores_of(q_s[head_rows(b, 1), :].astype(BF16), side(b, 0)) for b in group]
                    probs = [softmax_rows(sc, mask[...], len_sm[b]) for b, sc in zip(group, scores)]
                    for b, pr in zip(group, probs):
                        ctx_s[head_rows(b, 1), :] = jnp.dot(pr, side(b, 1), preferred_element_type=F32)
            if after is not None:
                for b in group:
                    cross_copy(after, b).start()
            return c
        lax.fori_loop(0, tok // CROSS_GROUP, body, 0)
        ctx = from_heads(ctx_s)
        return h + proj(layer, 5, ctx)

    q_s[...] = jnp.zeros_like(q_s)
    h = hid_ref[...].astype(F32)
    h = self_layer(0, h, cache_a, cache_a_out)
    for g in range(n_self):
        self_out(cache_a_out, g).wait()
        self_in(cache_b, g).start()
    h = cross_layer(0, h, cross_a, cross_b)
    x = norm_rows(h, gain_ref[2, 0:1, :], shift_ref[2, 0:1, :])
    for cp in ffn_copies():
        cp.wait()
    acc = h + fb2_ref[...].astype(F32).reshape(1, d_model)
    for f in range(0, ff, d_model):
        inner = jnp.dot(x, f1_buf[:, f:f + d_model], preferred_element_type=F32) + fb1_ref[f:f + d_model].astype(F32).reshape(1, d_model)
        inner = jnp.maximum(inner, 0.0).astype(BF16)
        acc = acc + jnp.dot(inner, f2_buf[f:f + d_model, :], preferred_element_type=F32)
    h = acc
    h = self_layer(1, h, cache_b, cache_b_out)
    h = cross_layer(1, h, cross_b, None)
    hid_out[...] = h
    z_out[...] = norm_rows(h, gain_ref[2, 1:2, :], shift_ref[2, 1:2, :])
    for g in range(n_self):
        self_out(cache_b_out, g).wait()


def dense_layers(hidden, self_pos, src_len, cache_a, cross_a, cache_b, cross_b, ln_gain, ln_shift, attn_w, attn_b, ffn_w1, ffn_b1, ffn_w2, ffn_b2):
    tok, d_model = hidden.shape
    n_heads, head_dim = cache_a.shape[3:]
    self_len, src = cache_a.shape[2], cross_a.shape[2]
    ff = ffn_w1.shape[1]
    swap = lambda arr: jnp.swapaxes(arr, 2, 3)
    sm = pl.BlockSpec(memory_space=pltpu.SMEM)
    vm = pl.BlockSpec(memory_space=VMEM)
    hbm = pl.BlockSpec(memory_space=pl.ANY)
    cache_t = jax.ShapeDtypeStruct((2, tok, n_heads, self_len, head_dim), BF16)
    n_self = tok // SELF_GROUP
    heads = VMEM((tok * HEAD_PAD, head_dim), F32)
    hid, z, out_a, out_b = pl.pallas_call(
        dense_kernel,
        out_shape=[VMEM((tok, d_model), F32), VMEM((tok, d_model), BF16), cache_t, cache_t],
        in_specs=[sm] * 2 + [vm] * 6 + [hbm] * 7,
        out_specs=[vm] * 2 + [hbm] * 2,
        scratch_shapes=[
            VMEM((12, d_model, d_model), BF16), VMEM((d_model, ff), BF16), VMEM((ff, d_model), BF16),
            VMEM((2, tok, n_heads, self_len, head_dim), BF16), VMEM((tok, 2, n_heads, src, head_dim), BF16),
            heads, heads, heads, heads, VMEM((tok, d_model), BF16), VMEM((tok * HEAD_PAD, 128), jnp.int32),
            VMEM((2 * HEAD_PAD, 2 * n_heads * self_len), jnp.int32), ] + [VMEM((HEAD_PAD, n_heads * rows), jnp.int32) for rows in range(ROW_STEP, src + 1, ROW_STEP)] + [
            pltpu.SMEM((tok,), jnp.int32), pltpu.SMEM((8,), jnp.int32),
            pltpu.SemaphoreType.DMA((12,)), pltpu.SemaphoreType.DMA((2,)), pltpu.SemaphoreType.DMA((n_self,)),
            pltpu.SemaphoreType.DMA((n_self,)), pltpu.SemaphoreType.DMA((tok,)),
        ],
        compiler_params=pltpu.CompilerParams(vmem_limit_bytes=61 * 1024 * 1024),
        name='dense_layers',
    )(self_pos, src_len, hidden, jnp.swapaxes(ln_gain, 0, 1), jnp.swapaxes(ln_shift, 0, 1), jnp.swapaxes(attn_b, 0, 1), ffn_b1, ffn_b2,
      swap(cache_a), swap(cross_a), swap(cache_b), swap(cross_b), attn_w, ffn_w1, ffn_w2)
    return hid, z, swap(out_a), swap(out_b)


def peer(index):
    return dict(device_id={'ep': index}, device_id_type=pl.DeviceIdType.MESH)


def neighbours():
    me = lax.axis_index('ep')
    core, x, y = me % 2, (me // 2) % 2, me // 4
    at = lambda yy, xx, cc: (yy * 2 + xx) * 2 + cc
    return me, core, x, y, at


def entry_barrier(others):
    barrier = pltpu.get_barrier_semaphore()
    for other in others:
        pl.semaphore_signal(barrier, inc=1, **peer(other))
    pl.semaphore_wait(barrier, len(others))


def named_experts(ids_cols, base, n_loc):
    n_tok = ids_cols.shape[0]
    lane = lax.broadcasted_iota(jnp.int32, (n_tok, 128), 1)
    id0 = ids_cols[:, 0:1].astype(jnp.int32) - base
    id1 = ids_cols[:, 1:2].astype(jnp.int32) - base
    hit = jnp.logical_and(jnp.logical_or(id0 == lane, id1 == lane), lane < n_loc)
    return id0, id1, lane, hit.astype(F32)


def gather_kernel(n_loc, z_ref, idst_ref, zall_ref, cols_ref, meta_ref, flip, ids_ref, idsall, send_sem, recv_sem):
    me, core, x, y, at = neighbours()
    twin = at(y, x, 1 - core)
    chips = [(y, 1 - x), (1 - y, x), (1 - y, 1 - x)]
    tok = z_ref.shape[0]
    group_n = zall_ref.shape[0]
    ids_ref[...] = jnp.zeros_like(ids_ref)
    ids_ref[0:2, 0:tok] = idst_ref[...].astype(F32)
    entry_barrier([twin] + [at(cy, cx, core) for cy, cx in chips])

    def send(slot, which, src, row, to):
        dst = (idsall, zall_ref)[which]
        cp = pltpu.make_async_remote_copy(
            src_ref=src, dst_ref=dst.at[row], send_sem=send_sem.at[slot, which], recv_sem=recv_sem.at[slot, which], **peer(to))
        cp.start()
        return cp

    far = [at(cy, cx, core) for cy, cx in chips]
    ids_sent = [send(j, 0, ids_ref, me, far[j]) for j in range(3)] + [send(3, 0, ids_ref, me, twin)]
    z_sent = {j: send(j, 1, z_ref, me, far[j]) for j in (2, 0, 1)}
    z_sent[3] = send(3, 1, z_ref, me, twin)
    zall_ref[me] = z_ref[...]
    idsall[me] = ids_ref[...]
    relays = []
    for j in range(3):
        ids_sent[j].wait_recv()
        relays.append(send(4 + j, 0, idsall.at[far[j]], far[j], twin))
    ids_sent[3].wait_recv()
    for cp in relays:
        cp.wait_recv()

    flip[...] = jnp.zeros_like(flip)
    for d in range(group_n):
        flip[2 * d:2 * d + 2, :] = idsall[d, 0:2, :]
    cols = jnp.transpose(flip[...])[:tok]
    lane_b = lax.broadcasted_iota(jnp.int32, (tok, 128), 1)
    wide = [jnp.where(lane_b == 0, cols[:, 2 * d:2 * d + 1], cols[:, 2 * d + 1:2 * d + 2]) for d in range(group_n)]
    cols_ref[...] = jnp.concatenate(wide, axis=0)
    _, _, _, hit = named_experts(cols_ref[...], me * n_loc, n_loc)
    ones = jnp.ones((group_n * tok, 128), BF16)
    count = lax.dot_general(hit.astype(BF16), ones, (((0,), (0,)), ((), ())), preferred_element_type=F32)
    row_i = lax.broadcasted_iota(jnp.int32, (128, 128), 0)
    col_i = lax.broadcasted_iota(jnp.int32, (128, 128), 1)
    named = (count > 0.5).astype(F32)
    order = jnp.dot((row_i > col_i).astype(BF16), named.astype(BF16), preferred_element_type=F32)
    spot = jnp.where(order == col_i.astype(F32), named, 0.0)
    expert_list = jnp.sum(spot * row_i.astype(F32), axis=0, keepdims=True)
    counts = jnp.sum(hit, axis=0, keepdims=True)
    total = jnp.sum(named, axis=0, keepdims=True)
    meta_ref[...] = jnp.concatenate([counts, expert_list, total, jnp.zeros((5, 128), F32)], axis=0).astype(jnp.int32)

    z_relays = []
    for j in (0, 1, 2):
        z_sent[j].wait_recv()
        z_relays.append(send(4 + j, 1, zall_ref.at[far[j]], far[j], twin))
    z_sent[3].wait_recv()
    for cp in z_relays:
        cp.wait_recv()
    for cp in ids_sent + relays + list(z_sent.values()) + z_relays:
        cp.wait_send()


def in_vmem(arr):
    return pltpu.with_memory_space_constraint(arr, VMEM)


def gather_tokens(z_bf, ids_t, group_n, n_loc):
    tok, d_model = z_bf.shape
    return pl.pallas_call(
        functools.partial(gather_kernel, n_loc),
        out_shape=[VMEM((group_n, tok, d_model), BF16), VMEM((group_n * tok, 128), F32), jax.ShapeDtypeStruct((8, 128), jnp.int32)],
        in_specs=[pl.BlockSpec(memory_space=VMEM)] * 2,
        out_specs=[pl.BlockSpec(memory_space=VMEM)] * 3,
        scratch_shapes=[VMEM((128, 128), F32), VMEM((8, 128), F32), VMEM((group_n, 8, 128), F32),
                        pltpu.SemaphoreType.DMA((7, 2)), pltpu.SemaphoreType.DMA((7, 2))],
        compiler_params=pltpu.CompilerParams(collective_id=0, has_side_effects=True, vmem_limit_bytes=16 * 1024 * 1024),
        name='gather_tokens',
    )(in_vmem(z_bf), ids_t)


def reduce_kernel(part_ref, hid_ref, out_ref, r1, s1, r2, s2, r3, send_sem, recv_sem):
    me, core, x, y, at = neighbours()
    twin, xn, yn = at(y, x, 1 - core), at(y, 1 - x, core), at(1 - y, x, core)
    entry_barrier([twin, xn, yn])
    half = hid_ref.shape[1] // 2
    cols = (pl.ds(0, half), pl.ds(half, half))

    def send(slot, src, dst, to):
        cp = pltpu.make_async_remote_copy(src_ref=src, dst_ref=dst, send_sem=send_sem.at[slot], recv_sem=recv_sem.at[slot], **peer(to))
        cp.start()
        return cp

    chips = [(1 - y, 1 - x), (y, 1 - x), (1 - y, x), (y, x)]
    first = [send(k, part_ref.at[at(cy, cx, 1 - core)], r1.at[k], twin) for k, (cy, cx) in enumerate(chips)]

    def sum1(k):
        first[k].wait_recv()
        cy, cx = chips[k]
        s1[k] = part_ref[at(cy, cx, core)] + r1[k]

    sum1(0)
    a0 = send(4, s1.at[0, :, cols[0]], r2.at[0, 0], xn)
    b0 = send(5, s1.at[0, :, cols[1]], r2.at[1, 0], yn)
    sum1(1)
    a1 = send(6, s1.at[1, :, cols[0]], r2.at[0, 1], xn)
    sum1(2)
    b1 = send(7, s1.at[2, :, cols[1]], r2.at[1, 1], yn)
    sum1(3)
    a0.wait_recv()
    s2[0] = s1[2, :, :half] + r2[0, 0]
    a2 = send(8, s2.at[0], r3.at[0], yn)
    b0.wait_recv()
    s2[1] = s1[1, :, half:] + r2[1, 0]
    b2 = send(9, s2.at[1], r3.at[1], xn)
    a1.wait_recv()
    own_a = hid_ref[:, :half] + s1[3, :, :half] + r2[0, 1]
    b1.wait_recv()
    own_b = hid_ref[:, half:] + s1[3, :, half:] + r2[1, 1]
    a2.wait_recv()
    out_ref[:, :half] = (own_a + r3[0]).astype(BF16)
    b2.wait_recv()
    out_ref[:, half:] = (own_b + r3[1]).astype(BF16)
    for cp in first + [a0, b0, a1, b1, a2, b2]:
        cp.wait_send()


def reduce_outputs(partial, hid_f32):
    group_n, tok, d_model = partial.shape
    half = d_model // 2
    return pl.pallas_call(
        reduce_kernel,
        out_shape=VMEM((tok, d_model), BF16),
        in_specs=[pl.BlockSpec(memory_space=VMEM)] * 2,
        out_specs=pl.BlockSpec(memory_space=VMEM),
        scratch_shapes=[
            VMEM((4, tok, d_model), F32), VMEM((4, tok, d_model), F32),
            VMEM((2, 2, tok, half), F32), VMEM((2, tok, half), F32), VMEM((2, tok, half), F32),
            pltpu.SemaphoreType.DMA((10,)), pltpu.SemaphoreType.DMA((10,)),
        ],
        compiler_params=pltpu.CompilerParams(collective_id=1, has_side_effects=True, vmem_limit_bytes=16 * 1024 * 1024),
        name='reduce_outputs',
    )(in_vmem(partial), in_vmem(hid_f32))


ROWS = 128
SPLIT = 2
SLOTS = 6


def expert_kernel(meta_sm, z_ref, cols_ref, rw_ref, b1_in, b2_in, w1_hbm, w2_hbm, out_ref,
                  b1_ref, b2_ref, w1_buf, w2_buf, rank_s, gate_s, x_s, o_s, sem1, sem2):
    n_tok, d_model = cols_ref.shape[0], z_ref.shape[2]
    n_loc = w1_hbm.shape[0]
    ff = w1_hbm.shape[2]
    fc = ff // SPLIT
    n_step = meta_sm[2, 0] * SPLIT

    def copies(step, slot):
        e = meta_sm[1, step // SPLIT]
        f0 = pl.multiple_of((step % SPLIT) * fc, fc)
        return (pltpu.make_async_copy(w1_hbm.at[e, :, pl.ds(f0, fc)], w1_buf.at[slot], sem1.at[slot]),
                pltpu.make_async_copy(w2_hbm.at[e, pl.ds(f0, fc), :], w2_buf.at[slot], sem2.at[slot]))

    for s in range(SLOTS):
        @pl.when(s < n_step)
        def _():
            for c in copies(s, s):
                c.start()

    b1_ref[...] = b1_in[...].astype(F32)
    b2_ref[...] = b2_in[...].astype(F32)
    z_all = z_ref[...].reshape(n_tok, d_model)
    id0, id1, lane, hit_t = named_experts(cols_ref[...], lax.axis_index('ep') * n_loc, n_loc)
    base = lax.axis_index('ep') * n_loc
    row_i = lax.broadcasted_iota(jnp.int32, (n_tok, n_tok), 0)
    col_i = lax.broadcasted_iota(jnp.int32, (n_tok, n_tok), 1)
    before = (row_i < col_i).astype(BF16)
    hit = jnp.transpose(hit_t)
    rank = jnp.dot(hit.astype(BF16), before, preferred_element_type=F32)
    rank_s[...] = jnp.where(hit > 0.5, rank, -1.0)

    logits = jnp.dot(z_all, rw_ref[...], preferred_element_type=F32)
    top = jnp.max(logits, axis=-1, keepdims=True)
    ex = jnp.exp(logits - top)
    probs = ex / jnp.sum(ex, axis=-1, keepdims=True)
    p0 = jnp.sum(jnp.where(lane == id0 + base, probs, 0.0), axis=-1, keepdims=True)
    p1 = jnp.sum(jnp.where(lane == id1 + base, probs, 0.0), axis=-1, keepdims=True)
    tot = p0 + p1
    g0, g1 = p0 / tot, p1 / tot
    gate_s[...] = jnp.where(lane == id0, g0, jnp.where(lane == id1, g1, 0.0))
    out_ref[...] = jnp.zeros_like(out_ref)

    def step_body(step, carry):
        slot = step % SLOTS
        e = meta_sm[1, step // SPLIT]
        part = step % SPLIT
        blocks = (meta_sm[0, e] + ROWS - 1) // ROWS
        slot_i = lax.broadcasted_iota(jnp.int32, (ROWS, n_tok), 0)

        def pick(j):
            want = (slot_i + j * ROWS).astype(F32)
            return (want == rank_s[pl.ds(e, 1), :]).astype(BF16)

        @pl.when(part == 0)
        def _():
            def gather_body(j, c):
                x_s[j] = jnp.dot(pick(j), z_ref[...].reshape(n_tok, d_model), preferred_element_type=F32).astype(BF16)
                o_s[j] = jnp.broadcast_to(b2_ref[pl.ds(e, 1), :], (ROWS, d_model))
                return c
            lax.fori_loop(0, blocks, gather_body, 0)

        for c in copies(step, slot):
            c.wait()
        bias = b1_ref[pl.ds(e, 1), pl.ds(pl.multiple_of(part * fc, fc), fc)]

        def block_body(j, c):
            inner = jnp.dot(x_s[j], w1_buf[slot], preferred_element_type=F32) + bias
            inner = jnp.maximum(inner, 0.0).astype(BF16)
            o_s[j] += jnp.dot(inner, w2_buf[slot], preferred_element_type=F32)
            return c
        lax.fori_loop(0, blocks, block_body, 0)

        @pl.when(step + SLOTS < n_step)
        def _():
            for c in copies(step + SLOTS, slot):
                c.start()

        @pl.when(part == SPLIT - 1)
        def _():
            lane_g = lax.broadcasted_iota(jnp.int32, (n_tok, 128), 1)
            gate = jnp.sum(jnp.where(lane_g == e, gate_s[...], 0.0), axis=-1, keepdims=True)

            def scatter_body(j, c):
                back = lax.dot_general(pick(j), o_s[j].astype(BF16), (((0,), (0,)), ((), ())), preferred_element_type=F32)
                out_ref[...] += (gate * back).reshape(out_ref.shape)
                return c
            lax.fori_loop(0, blocks, scatter_body, 0)
        return carry

    lax.fori_loop(0, n_step, step_body, 0)


def run_experts(meta, z_all, cols, router_w, exp_w1, exp_b1, exp_w2, exp_b2):
    group_n, tok, d_model = z_all.shape
    n_tok = group_n * tok
    n_loc, _, ff = exp_w1.shape
    fc = ff // SPLIT
    n_blk = n_tok // ROWS
    vm = pl.BlockSpec(memory_space=VMEM)
    hbm = pl.BlockSpec(memory_space=pl.ANY)
    return pl.pallas_call(
        expert_kernel,
        out_shape=VMEM((group_n, tok, d_model), F32),
        in_specs=[pl.BlockSpec(memory_space=pltpu.SMEM)] + [vm] * 5 + [hbm] * 2,
        out_specs=vm,
        scratch_shapes=[
            VMEM((n_loc, ff), F32), VMEM((n_loc, d_model), F32),
            VMEM((SLOTS, d_model, fc), BF16), VMEM((SLOTS, fc, d_model), BF16),
            VMEM((128, n_tok), F32), VMEM((n_tok, 128), F32),
            VMEM((n_blk, ROWS, d_model), BF16), VMEM((n_blk, ROWS, d_model), F32),
            pltpu.SemaphoreType.DMA((SLOTS,)), pltpu.SemaphoreType.DMA((SLOTS,)),
        ],
        compiler_params=pltpu.CompilerParams(vmem_limit_bytes=48 * 1024 * 1024),
        name='run_experts',
    )(meta, in_vmem(z_all), in_vmem(cols), router_w, exp_b1, exp_b2, exp_w1, exp_w2)


def solution(mesh):
    group_n = mesh.shape['ep']

    def local_step(hidden, self_pos, src_len, cache_a, cross_a, cache_b, cross_b, route_ids, ln_gain, ln_shift, attn_w, attn_b, ffn_w1, ffn_b1, ffn_w2, ffn_b2, router_w, exp_w1, exp_b1, exp_w2, exp_b2):
        hid_f32, z_bf, cache_a_new, cache_b_new = dense_layers(hidden, self_pos, src_len, cache_a, cross_a, cache_b, cross_b, ln_gain, ln_shift, attn_w, attn_b, ffn_w1, ffn_b1, ffn_w2, ffn_b2)
        z_all, cols, meta = gather_tokens(z_bf, route_ids.T, group_n, exp_w1.shape[0])
        partial = run_experts(meta, z_all, cols, router_w, exp_w1, exp_b1, exp_w2, exp_b2)
        out = reduce_outputs(partial, hid_f32)
        return out, cache_a_new, cache_b_new

    tok_spec = P(('dp', 'ep'))
    cache_spec = P(None, ('dp', 'ep'))
    rep_spec = P()
    exp_spec = P('ep')
    in_specs = (tok_spec, tok_spec, tok_spec, cache_spec, cache_spec, cache_spec, cache_spec, tok_spec) + (rep_spec,) * 9 + (exp_spec,) * 4
    out_specs = (tok_spec, cache_spec, cache_spec)
    return jax.shard_map(local_step, mesh=mesh, in_specs=in_specs, out_specs=out_specs, check_vma=False)
```

```python
import functools

import jax
import jax.numpy as jnp
from jax import lax
from jax.experimental import pallas as pl
from jax.experimental.pallas import tpu as pltpu
from jax.sharding import PartitionSpec as P

LN_EPS = 1e-5
F32 = jnp.float32
BF16 = jnp.bfloat16
VMEM = pltpu.VMEM


CROSS_GROUP = 16
ROW_STEP = 16
ROW_SHIFT = 4
SELF_GROUP = 16
SELF_UNIT = 2
HEAD_PAD = 16


def norm_rows(x_val, gain_vec, shift_vec):
    mean_val = jnp.mean(x_val, axis=-1, keepdims=True)
    centered = x_val - mean_val
    var_val = jnp.mean(centered * centered, axis=-1, keepdims=True)
    return (centered * lax.rsqrt(var_val + LN_EPS) * gain_vec + shift_vec).astype(BF16)


def dense_kernel(pos_sm, len_sm, hid_ref, gain_ref, shift_ref, ab_ref, fb1_ref, fb2_ref,
                 cache_a, cross_a, cache_b, cross_b, aw_hbm, w1_hbm, w2_hbm,
                 hid_out, z_out, cache_a_out, cache_b_out,
                 w_buf, f1_buf, f2_buf, self_buf, cross_buf, q_s, k_s, v_s, ctx_s, cat_s, lim_s, self_mask, mask_1, mask_2, mask_3, mask_4, order_sm, lists_sm,
                 w_sem, f_sem, in_sem, out_sem, cross_sem):
    tok, d_model = hid_ref.shape
    n_heads, self_len, head_dim = self_buf.shape[2:]
    src = cross_buf.shape[3]
    ff = f1_buf.shape[1]
    scale = head_dim ** -0.5
    cross_masks = (mask_1, mask_2, mask_3, mask_4)
    n_class = len(cross_masks)
    n_self = tok // SELF_GROUP

    def head_rows(b, n):
        return pl.ds(pl.multiple_of(b * HEAD_PAD, HEAD_PAD), n * HEAD_PAD)

    def weight_copy(i):
        return pltpu.make_async_copy(aw_hbm.at[i // 6, i % 6], w_buf.at[i], w_sem.at[i])

    def ffn_copies():
        return (pltpu.make_async_copy(w1_hbm, f1_buf, f_sem.at[0]), pltpu.make_async_copy(w2_hbm, f2_buf, f_sem.at[1]))

    def self_in(cache, g):
        rows = pl.ds(g * SELF_GROUP, SELF_GROUP)
        return pltpu.make_async_copy(cache.at[:, rows], self_buf.at[:, rows], in_sem.at[g])

    def self_out(cache_out, g):
        rows = pl.ds(g * SELF_GROUP, SELF_GROUP)
        return pltpu.make_async_copy(self_buf.at[:, rows], cache_out.at[:, rows], out_sem.at[g])

    def cross_rows(b):
        return pl.multiple_of((lax.shift_right_logical(len_sm[b] - 1, ROW_SHIFT) + 1) * ROW_STEP, ROW_STEP)

    def length_class(b):
        return lax.shift_right_logical(len_sm[b] - 1, ROW_SHIFT)

    def cross_copy(cross, b):
        rows = pl.ds(0, cross_rows(b))
        return pltpu.make_async_copy(cross.at[:, b, :, rows, :], cross_buf.at[b, :, :, rows, :], cross_sem.at[b])

    for i in range(3):
        weight_copy(i).start()
    for g in range(n_self):
        self_in(cache_a, g).start()
    weight_copy(3).start()
    weight_copy(4).start()

    def first_cross(b, sizes):
        cross_copy(cross_a, b).start()
        k = length_class(b)
        size = sizes[0]
        for j in range(1, n_class):
            size = jnp.where(k == j, sizes[j], size)
        lists_sm[k * tok + size] = b
        return tuple(n + jnp.where(k == j, 1, 0) for j, n in enumerate(sizes))
    sizes = lax.fori_loop(0, tok, first_cross, (jnp.int32(0),) * n_class)

    def place(i, c):
        at, end = i, jnp.int32(0)
        for j in range(n_class - 1):
            end = end + sizes[j]
            at = jnp.where(i >= end, (j + 1) * tok + i - end, at)
        order_sm[i] = lists_sm[at]
        return c
    lax.fori_loop(0, tok, place, 0)

    def zero_tail(b, c):
        def zero_part(part, c2):
            cross_buf[b, 1, :, pl.ds(pl.multiple_of(part * 16, 16), 16), :] = jnp.zeros((n_heads, 16, head_dim), BF16)
            return c2
        return lax.fori_loop(length_class(b) + 1, n_class, zero_part, c)
    lax.fori_loop(0, tok, zero_tail, 0)

    def issue_rest():
        weight_copy(5).start()
        for cp in ffn_copies():
            cp.start()
        for i in range(6, 12):
            weight_copy(i).start()

    def build_mask(ref, length):
        row = lax.broadcasted_iota(jnp.int32, ref.shape, 0)
        lane = lax.broadcasted_iota(jnp.int32, ref.shape, 1)
        seq, head = lane // (n_heads * length), (lane // length) % n_heads
        ref[...] = jnp.where(seq * HEAD_PAD + head == row, lane % length, 1 << 20)
    build_mask(self_mask, self_len)
    for mask in cross_masks:
        build_mask(mask, mask.shape[1] // n_heads)

    def fill_limit(b, c):
        lim_s[head_rows(b, 1), :] = jnp.full((HEAD_PAD, 128), pos_sm[b] + 1, jnp.int32)
        return c
    lax.fori_loop(0, tok, fill_limit, 0)

    def to_heads(ref, val):
        val = val.astype(BF16).astype(F32)
        for h in range(n_heads):
            ref[pl.ds(h, tok, stride=HEAD_PAD), :] = val[:, h * head_dim:(h + 1) * head_dim]

    def from_heads(ref):
        for h in range(0, n_heads, 2):
            two = [ref[pl.ds(h + k, tok, stride=HEAD_PAD), :] for k in range(2)]
            cat_s[:, h * head_dim:(h + 2) * head_dim] = jnp.concatenate(two, axis=1).astype(BF16)
        return cat_s[...]

    def softmax_rows(scores, mask, limit):
        scores = jnp.where(mask < limit, scores * scale, -1e30)
        top = jnp.max(scores, axis=-1, keepdims=True)
        ex = jnp.exp(scores - top)
        return (ex * (1.0 / jnp.sum(ex, axis=-1, keepdims=True))).astype(BF16)

    def scores_of(q, keys):
        return lax.dot_general(q, keys, (((1,), (1,)), ((), ())), preferred_element_type=F32)

    def block_diag(blocks):
        rows = []
        for k, blk in enumerate(blocks):
            pad = jnp.zeros_like(blk)
            rows.append(jnp.concatenate([blk if j == k else pad for j in range(len(blocks))], axis=1))
        return jnp.concatenate(rows, axis=0)

    def proj(layer, i, x_bf):
        weight_copy(layer * 6 + i).wait()
        bias = ab_ref[i].astype(F32)[layer:layer + 1, :]
        return jnp.dot(x_bf, w_buf[layer * 6 + i], preferred_element_type=F32) + bias

    def self_layer(layer, h, cache, cache_out):
        x = norm_rows(h, gain_ref[0, layer:layer + 1, :], shift_ref[0, layer:layer + 1, :])
        to_heads(q_s, proj(layer, 0, x))
        to_heads(k_s, proj(layer, 1, x))
        to_heads(v_s, proj(layer, 2, x))
        if layer == 0:
            issue_rest()
        row_i = lax.broadcasted_iota(jnp.int32, (self_len, head_dim), 0)
        row_b = row_i.astype(F32).astype(BF16)

        def body(g, c):
            self_in(cache, g).wait()
            first = g * SELF_GROUP
            sides = []
            for which, new in ((0, k_s), (1, v_s)):
                tiles = []
                for u in range(SELF_GROUP):
                    b = first + u
                    hit = row_b == jnp.full(row_b.shape, pos_sm[b], jnp.int32).astype(F32).astype(BF16)
                    for hd in range(n_heads):
                        row = new[pl.ds(b * HEAD_PAD + hd, self_len, stride=0), :]
                        tile = jnp.where(hit, row.astype(BF16), self_buf[which, b, hd])
                        self_buf[which, b, hd] = tile
                        tiles.append(tile)
                sides.append(tiles)
            n = SELF_UNIT
            parts = range(0, SELF_GROUP, n)
            wide = n * n_heads * self_len
            stack = lambda tiles, p: jnp.concatenate(tiles[p * n_heads:(p + n) * n_heads], axis=0)
            scores = [scores_of(q_s[head_rows(first + p, n), :].astype(BF16), stack(sides[0], p)) for p in parts]
            probs = []
            for p, sc in zip(parts, scores):
                two = 2 * n_heads * self_len
                blocks = []
                for k in range(n // 2):
                    lim = lim_s[head_rows(first + p + 2 * k, 2), :]
                    lim = jnp.concatenate([lim] * (two // 128), axis=1)
                    blocks.append(softmax_rows(sc[k * 2 * HEAD_PAD:(k + 1) * 2 * HEAD_PAD, k * two:(k + 1) * two], self_mask[...], lim))
                probs.append(block_diag(blocks))
            for p, pr in zip(parts, probs):
                ctx_s[head_rows(first + p, n), :] = jnp.dot(pr, stack(sides[1], p), preferred_element_type=F32)
            self_out(cache_out, g).start()
            return c
        lax.fori_loop(0, n_self, body, 0)
        ctx = from_heads(ctx_s)
        return h + proj(layer, 3, ctx)

    def cross_layer(layer, h, cross, after):
        x = norm_rows(h, gain_ref[1, layer:layer + 1, :], shift_ref[1, layer:layer + 1, :])
        to_heads(q_s, proj(layer, 4, x))

        def body(g, c):
            group = [order_sm[g * CROSS_GROUP + u] for u in range(CROSS_GROUP)]
            longest = length_class(group[-1])
            for b in group:
                cross_copy(cross, b).wait()
            for k, mask in enumerate(cross_masks):
                @pl.when(longest == k)
                def _():
                    rows = mask.shape[1] // n_heads
                    side = lambda b, which: cross_buf[b, which, :, 0:rows, :].reshape(n_heads * rows, head_dim)
                    scores = [scores_of(q_s[head_rows(b, 1), :].astype(BF16), side(b, 0)) for b in group]
                    probs = [softmax_rows(sc, mask[...], len_sm[b]) for b, sc in zip(group, scores)]
                    for b, pr in zip(group, probs):
                        ctx_s[head_rows(b, 1), :] = jnp.dot(pr, side(b, 1), preferred_element_type=F32)
            if after is not None:
                for b in group:
                    cross_copy(after, b).start()
            return c
        lax.fori_loop(0, tok // CROSS_GROUP, body, 0)
        ctx = from_heads(ctx_s)
        return h + proj(layer, 5, ctx)

    q_s[...] = jnp.zeros_like(q_s)
    h = hid_ref[...].astype(F32)
    h = self_layer(0, h, cache_a, cache_a_out)
    for g in range(n_self):
        self_out(cache_a_out, g).wait()
        self_in(cache_b, g).start()
    h = cross_layer(0, h, cross_a, cross_b)
    x = norm_rows(h, gain_ref[2, 0:1, :], shift_ref[2, 0:1, :])
    for cp in ffn_copies():
        cp.wait()
    acc = h + fb2_ref[...].astype(F32).reshape(1, d_model)
    for f in range(0, ff, d_model):
        inner = jnp.dot(x, f1_buf[:, f:f + d_model], preferred_element_type=F32) + fb1_ref[f:f + d_model].astype(F32).reshape(1, d_model)
        inner = jnp.maximum(inner, 0.0).astype(BF16)
        acc = acc + jnp.dot(inner, f2_buf[f:f + d_model, :], preferred_element_type=F32)
    h = acc
    h = self_layer(1, h, cache_b, cache_b_out)
    h = cross_layer(1, h, cross_b, None)
    hid_out[...] = h
    z_out[...] = norm_rows(h, gain_ref[2, 1:2, :], shift_ref[2, 1:2, :])
    for g in range(n_self):
        self_out(cache_b_out, g).wait()


def dense_layers(hidden, self_pos, src_len, cache_a, cross_a, cache_b, cross_b, ln_gain, ln_shift, attn_w, attn_b, ffn_w1, ffn_b1, ffn_w2, ffn_b2):
    tok, d_model = hidden.shape
    n_heads, head_dim = cache_a.shape[3:]
    self_len, src = cache_a.shape[2], cross_a.shape[2]
    ff = ffn_w1.shape[1]
    swap = lambda arr: jnp.swapaxes(arr, 2, 3)
    sm = pl.BlockSpec(memory_space=pltpu.SMEM)
    vm = pl.BlockSpec(memory_space=VMEM)
    hbm = pl.BlockSpec(memory_space=pl.ANY)
    cache_t = jax.ShapeDtypeStruct((2, tok, n_heads, self_len, head_dim), BF16)
    n_self = tok // SELF_GROUP
    heads = VMEM((tok * HEAD_PAD, head_dim), F32)
    hid, z, out_a, out_b = pl.pallas_call(
        dense_kernel,
        out_shape=[VMEM((tok, d_model), F32), VMEM((tok, d_model), BF16), cache_t, cache_t],
        in_specs=[sm] * 2 + [vm] * 6 + [hbm] * 7,
        out_specs=[vm] * 2 + [hbm] * 2,
        scratch_shapes=[
            VMEM((12, d_model, d_model), BF16), VMEM((d_model, ff), BF16), VMEM((ff, d_model), BF16),
            VMEM((2, tok, n_heads, self_len, head_dim), BF16), VMEM((tok, 2, n_heads, src, head_dim), BF16),
            heads, heads, heads, heads, VMEM((tok, d_model), BF16), VMEM((tok * HEAD_PAD, 128), jnp.int32),
            VMEM((2 * HEAD_PAD, 2 * n_heads * self_len), jnp.int32), ] + [VMEM((HEAD_PAD, n_heads * rows), jnp.int32) for rows in range(ROW_STEP, src + 1, ROW_STEP)] + [
            pltpu.SMEM((tok,), jnp.int32), pltpu.SMEM((src // ROW_STEP * tok,), jnp.int32),
            pltpu.SemaphoreType.DMA((12,)), pltpu.SemaphoreType.DMA((2,)), pltpu.SemaphoreType.DMA((n_self,)),
            pltpu.SemaphoreType.DMA((n_self,)), pltpu.SemaphoreType.DMA((tok,)),
        ],
        compiler_params=pltpu.CompilerParams(vmem_limit_bytes=61 * 1024 * 1024),
        name='dense_layers',
    )(self_pos, src_len, hidden, jnp.swapaxes(ln_gain, 0, 1), jnp.swapaxes(ln_shift, 0, 1), jnp.swapaxes(attn_b, 0, 1), ffn_b1, ffn_b2,
      swap(cache_a), swap(cross_a), swap(cache_b), swap(cross_b), attn_w, ffn_w1, ffn_w2)
    return hid, z, swap(out_a), swap(out_b)


def peer(index):
    return dict(device_id={'ep': index}, device_id_type=pl.DeviceIdType.MESH)


def neighbours():
    me = lax.axis_index('ep')
    core, x, y = me % 2, (me // 2) % 2, me // 4
    at = lambda yy, xx, cc: (yy * 2 + xx) * 2 + cc
    return me, core, x, y, at


def entry_barrier(others):
    barrier = pltpu.get_barrier_semaphore()
    for other in others:
        pl.semaphore_signal(barrier, inc=1, **peer(other))
    pl.semaphore_wait(barrier, len(others))


def named_experts(ids_cols, base, n_loc):
    n_tok = ids_cols.shape[0]
    lane = lax.broadcasted_iota(jnp.int32, (n_tok, 128), 1)
    id0 = ids_cols[:, 0:1].astype(jnp.int32) - base
    id1 = ids_cols[:, 1:2].astype(jnp.int32) - base
    hit = jnp.logical_and(jnp.logical_or(id0 == lane, id1 == lane), lane < n_loc)
    return id0, id1, lane, hit.astype(F32)


def gather_kernel(n_loc, z_ref, idst_ref, zall_ref, cols_ref, meta_ref, flip, ids_ref, idsall, send_sem, recv_sem):
    me, core, x, y, at = neighbours()
    twin = at(y, x, 1 - core)
    chips = [(y, 1 - x), (1 - y, x), (1 - y, 1 - x)]
    tok = z_ref.shape[0]
    group_n = zall_ref.shape[0]
    ids_ref[...] = jnp.zeros_like(ids_ref)
    ids_ref[0:2, 0:tok] = idst_ref[...].astype(F32)
    entry_barrier([twin] + [at(cy, cx, core) for cy, cx in chips])

    def send(slot, which, src, row, to):
        dst = (idsall, zall_ref)[which]
        cp = pltpu.make_async_remote_copy(
            src_ref=src, dst_ref=dst.at[row], send_sem=send_sem.at[slot, which], recv_sem=recv_sem.at[slot, which], **peer(to))
        cp.start()
        return cp

    far = [at(cy, cx, core) for cy, cx in chips]
    ids_sent = [send(j, 0, ids_ref, me, far[j]) for j in range(3)] + [send(3, 0, ids_ref, me, twin)]
    z_sent = {j: send(j, 1, z_ref, me, far[j]) for j in (2, 0, 1)}
    z_sent[3] = send(3, 1, z_ref, me, twin)
    zall_ref[me] = z_ref[...]
    idsall[me] = ids_ref[...]
    relays = []
    for j in range(3):
        ids_sent[j].wait_recv()
        relays.append(send(4 + j, 0, idsall.at[far[j]], far[j], twin))
    ids_sent[3].wait_recv()
    for cp in relays:
        cp.wait_recv()

    flip[...] = jnp.zeros_like(flip)
    for d in range(group_n):
        flip[2 * d:2 * d + 2, :] = idsall[d, 0:2, :]
    cols = jnp.transpose(flip[...])[:tok]
    lane_b = lax.broadcasted_iota(jnp.int32, (tok, 128), 1)
    wide = [jnp.where(lane_b == 0, cols[:, 2 * d:2 * d + 1], cols[:, 2 * d + 1:2 * d + 2]) for d in range(group_n)]
    cols_ref[...] = jnp.concatenate(wide, axis=0)
    _, _, _, hit = named_experts(cols_ref[...], me * n_loc, n_loc)
    ones = jnp.ones((group_n * tok, 128), BF16)
    count = lax.dot_general(hit.astype(BF16), ones, (((0,), (0,)), ((), ())), preferred_element_type=F32)
    row_i = lax.broadcasted_iota(jnp.int32, (128, 128), 0)
    col_i = lax.broadcasted_iota(jnp.int32, (128, 128), 1)
    named = (count > 0.5).astype(F32)
    order = jnp.dot((row_i > col_i).astype(BF16), named.astype(BF16), preferred_element_type=F32)
    spot = jnp.where(order == col_i.astype(F32), named, 0.0)
    expert_list = jnp.sum(spot * row_i.astype(F32), axis=0, keepdims=True)
    counts = jnp.sum(hit, axis=0, keepdims=True)
    total = jnp.sum(named, axis=0, keepdims=True)
    meta_ref[...] = jnp.concatenate([counts, expert_list, total, jnp.zeros((5, 128), F32)], axis=0).astype(jnp.int32)

    z_relays = []
    for j in (0, 1, 2):
        z_sent[j].wait_recv()
        z_relays.append(send(4 + j, 1, zall_ref.at[far[j]], far[j], twin))
    z_sent[3].wait_recv()
    for cp in z_relays:
        cp.wait_recv()
    for cp in ids_sent + relays + list(z_sent.values()) + z_relays:
        cp.wait_send()


def in_vmem(arr):
    return pltpu.with_memory_space_constraint(arr, VMEM)


def gather_tokens(z_bf, ids_t, group_n, n_loc):
    tok, d_model = z_bf.shape
    return pl.pallas_call(
        functools.partial(gather_kernel, n_loc),
        out_shape=[VMEM((group_n, tok, d_model), BF16), VMEM((group_n * tok, 128), F32), jax.ShapeDtypeStruct((8, 128), jnp.int32)],
        in_specs=[pl.BlockSpec(memory_space=VMEM)] * 2,
        out_specs=[pl.BlockSpec(memory_space=VMEM)] * 3,
        scratch_shapes=[VMEM((128, 128), F32), VMEM((8, 128), F32), VMEM((group_n, 8, 128), F32),
                        pltpu.SemaphoreType.DMA((7, 2)), pltpu.SemaphoreType.DMA((7, 2))],
        compiler_params=pltpu.CompilerParams(collective_id=0, has_side_effects=True, vmem_limit_bytes=16 * 1024 * 1024),
        name='gather_tokens',
    )(in_vmem(z_bf), ids_t)


def reduce_kernel(part_ref, hid_ref, out_ref, r1, s1, r2, s2, r3, send_sem, recv_sem):
    me, core, x, y, at = neighbours()
    twin, xn, yn = at(y, x, 1 - core), at(y, 1 - x, core), at(1 - y, x, core)
    entry_barrier([twin, xn, yn])
    half = hid_ref.shape[1] // 2
    cols = (pl.ds(0, half), pl.ds(half, half))

    def send(slot, src, dst, to):
        cp = pltpu.make_async_remote_copy(src_ref=src, dst_ref=dst, send_sem=send_sem.at[slot], recv_sem=recv_sem.at[slot], **peer(to))
        cp.start()
        return cp

    chips = [(1 - y, 1 - x), (y, 1 - x), (1 - y, x), (y, x)]
    first = [send(k, part_ref.at[at(cy, cx, 1 - core)], r1.at[k], twin) for k, (cy, cx) in enumerate(chips)]

    def sum1(k):
        first[k].wait_recv()
        cy, cx = chips[k]
        s1[k] = part_ref[at(cy, cx, core)] + r1[k]

    sum1(0)
    a0 = send(4, s1.at[0, :, cols[0]], r2.at[0, 0], xn)
    b0 = send(5, s1.at[0, :, cols[1]], r2.at[1, 0], yn)
    sum1(1)
    a1 = send(6, s1.at[1, :, cols[0]], r2.at[0, 1], xn)
    sum1(2)
    b1 = send(7, s1.at[2, :, cols[1]], r2.at[1, 1], yn)
    sum1(3)
    a0.wait_recv()
    s2[0] = s1[2, :, :half] + r2[0, 0]
    a2 = send(8, s2.at[0], r3.at[0], yn)
    b0.wait_recv()
    s2[1] = s1[1, :, half:] + r2[1, 0]
    b2 = send(9, s2.at[1], r3.at[1], xn)
    a1.wait_recv()
    own_a = hid_ref[:, :half] + s1[3, :, :half] + r2[0, 1]
    b1.wait_recv()
    own_b = hid_ref[:, half:] + s1[3, :, half:] + r2[1, 1]
    a2.wait_recv()
    out_ref[:, :half] = (own_a + r3[0]).astype(BF16)
    b2.wait_recv()
    out_ref[:, half:] = (own_b + r3[1]).astype(BF16)
    for cp in first + [a0, b0, a1, b1, a2, b2]:
        cp.wait_send()


def reduce_outputs(partial, hid_f32):
    group_n, tok, d_model = partial.shape
    half = d_model // 2
    return pl.pallas_call(
        reduce_kernel,
        out_shape=VMEM((tok, d_model), BF16),
        in_specs=[pl.BlockSpec(memory_space=VMEM)] * 2,
        out_specs=pl.BlockSpec(memory_space=VMEM),
        scratch_shapes=[
            VMEM((4, tok, d_model), F32), VMEM((4, tok, d_model), F32),
            VMEM((2, 2, tok, half), F32), VMEM((2, tok, half), F32), VMEM((2, tok, half), F32),
            pltpu.SemaphoreType.DMA((10,)), pltpu.SemaphoreType.DMA((10,)),
        ],
        compiler_params=pltpu.CompilerParams(collective_id=1, has_side_effects=True, vmem_limit_bytes=16 * 1024 * 1024),
        name='reduce_outputs',
    )(in_vmem(partial), in_vmem(hid_f32))


ROWS = 128
SPLIT = 4
SLOTS = 12


def expert_kernel(meta_sm, z_ref, cols_ref, rw_ref, b1_in, b2_in, w1_hbm, w2_hbm, out_ref,
                  b1_ref, b2_ref, w1_buf, w2_buf, rank_s, gate_s, x_s, o_s, sem1, sem2):
    n_tok, d_model = cols_ref.shape[0], z_ref.shape[2]
    n_loc = w1_hbm.shape[0]
    ff = w1_hbm.shape[2]
    fc = ff // SPLIT
    n_step = meta_sm[2, 0] * SPLIT

    def copies(step, slot):
        e = meta_sm[1, step // SPLIT]
        f0 = pl.multiple_of((step % SPLIT) * fc, fc)
        return (pltpu.make_async_copy(w1_hbm.at[e, :, pl.ds(f0, fc)], w1_buf.at[slot], sem1.at[slot]),
                pltpu.make_async_copy(w2_hbm.at[e, pl.ds(f0, fc), :], w2_buf.at[slot], sem2.at[slot]))

    for s in range(SLOTS):
        @pl.when(s < n_step)
        def _():
            for c in copies(s, s):
                c.start()

    b1_ref[...] = b1_in[...].astype(F32)
    b2_ref[...] = b2_in[...].astype(F32)
    z_all = z_ref[...].reshape(n_tok, d_model)
    id0, id1, lane, hit_t = named_experts(cols_ref[...], lax.axis_index('ep') * n_loc, n_loc)
    base = lax.axis_index('ep') * n_loc
    row_i = lax.broadcasted_iota(jnp.int32, (n_tok, n_tok), 0)
    col_i = lax.broadcasted_iota(jnp.int32, (n_tok, n_tok), 1)
    before = (row_i < col_i).astype(BF16)
    hit = jnp.transpose(hit_t)
    rank = jnp.dot(hit.astype(BF16), before, preferred_element_type=F32)
    rank_s[...] = jnp.where(hit > 0.5, rank, -1.0)

    logits = jnp.dot(z_all, rw_ref[...], preferred_element_type=F32)
    top = jnp.max(logits, axis=-1, keepdims=True)
    ex = jnp.exp(logits - top)
    probs = ex / jnp.sum(ex, axis=-1, keepdims=True)
    p0 = jnp.sum(jnp.where(lane == id0 + base, probs, 0.0), axis=-1, keepdims=True)
    p1 = jnp.sum(jnp.where(lane == id1 + base, probs, 0.0), axis=-1, keepdims=True)
    tot = p0 + p1
    g0, g1 = p0 / tot, p1 / tot
    gate_s[...] = jnp.where(lane == id0, g0, jnp.where(lane == id1, g1, 0.0))
    out_ref[...] = jnp.zeros_like(out_ref)

    def step_body(step, carry):
        slot = step % SLOTS
        e = meta_sm[1, step // SPLIT]
        part = step % SPLIT
        blocks = (meta_sm[0, e] + ROWS - 1) // ROWS
        slot_i = lax.broadcasted_iota(jnp.int32, (ROWS, n_tok), 0)

        def pick(j):
            want = (slot_i + j * ROWS).astype(F32)
            return (want == rank_s[pl.ds(e, 1), :]).astype(BF16)

        @pl.when(part == 0)
        def _():
            def gather_body(j, c):
                x_s[j] = jnp.dot(pick(j), z_ref[...].reshape(n_tok, d_model), preferred_element_type=F32).astype(BF16)
                o_s[j] = jnp.broadcast_to(b2_ref[pl.ds(e, 1), :], (ROWS, d_model))
                return c
            lax.fori_loop(0, blocks, gather_body, 0)

        for c in copies(step, slot):
            c.wait()
        bias = b1_ref[pl.ds(e, 1), pl.ds(pl.multiple_of(part * fc, fc), fc)]

        def block_body(j, c):
            inner = jnp.dot(x_s[j], w1_buf[slot], preferred_element_type=F32) + bias
            inner = jnp.maximum(inner, 0.0).astype(BF16)
            o_s[j] += jnp.dot(inner, w2_buf[slot], preferred_element_type=F32)
            return c
        lax.fori_loop(0, blocks, block_body, 0)

        @pl.when(step + SLOTS < n_step)
        def _():
            for c in copies(step + SLOTS, slot):
                c.start()

        @pl.when(part == SPLIT - 1)
        def _():
            lane_g = lax.broadcasted_iota(jnp.int32, (n_tok, 128), 1)
            gate = jnp.sum(jnp.where(lane_g == e, gate_s[...], 0.0), axis=-1, keepdims=True)

            def scatter_body(j, c):
                back = lax.dot_general(pick(j), o_s[j].astype(BF16), (((0,), (0,)), ((), ())), preferred_element_type=F32)
                out_ref[...] += (gate * back).reshape(out_ref.shape)
                return c
            lax.fori_loop(0, blocks, scatter_body, 0)
        return carry

    lax.fori_loop(0, n_step, step_body, 0)


def run_experts(meta, z_all, cols, router_w, exp_w1, exp_b1, exp_w2, exp_b2):
    group_n, tok, d_model = z_all.shape
    n_tok = group_n * tok
    n_loc, _, ff = exp_w1.shape
    fc = ff // SPLIT
    n_blk = n_tok // ROWS
    vm = pl.BlockSpec(memory_space=VMEM)
    hbm = pl.BlockSpec(memory_space=pl.ANY)
    return pl.pallas_call(
        expert_kernel,
        out_shape=VMEM((group_n, tok, d_model), F32),
        in_specs=[pl.BlockSpec(memory_space=pltpu.SMEM)] + [vm] * 5 + [hbm] * 2,
        out_specs=vm,
        scratch_shapes=[
            VMEM((n_loc, ff), F32), VMEM((n_loc, d_model), F32),
            VMEM((SLOTS, d_model, fc), BF16), VMEM((SLOTS, fc, d_model), BF16),
            VMEM((128, n_tok), F32), VMEM((n_tok, 128), F32),
            VMEM((n_blk, ROWS, d_model), BF16), VMEM((n_blk, ROWS, d_model), F32),
            pltpu.SemaphoreType.DMA((SLOTS,)), pltpu.SemaphoreType.DMA((SLOTS,)),
        ],
        compiler_params=pltpu.CompilerParams(vmem_limit_bytes=48 * 1024 * 1024),
        name='run_experts',
    )(meta, in_vmem(z_all), in_vmem(cols), router_w, exp_b1, exp_b2, exp_w1, exp_w2)


def solution(mesh):
    group_n = mesh.shape['ep']

    def local_step(hidden, self_pos, src_len, cache_a, cross_a, cache_b, cross_b, route_ids, ln_gain, ln_shift, attn_w, attn_b, ffn_w1, ffn_b1, ffn_w2, ffn_b2, router_w, exp_w1, exp_b1, exp_w2, exp_b2):
        hid_f32, z_bf, cache_a_new, cache_b_new = dense_layers(hidden, self_pos, src_len, cache_a, cross_a, cache_b, cross_b, ln_gain, ln_shift, attn_w, attn_b, ffn_w1, ffn_b1, ffn_w2, ffn_b2)
        z_all, cols, meta = gather_tokens(z_bf, route_ids.T, group_n, exp_w1.shape[0])
        partial = run_experts(meta, z_all, cols, router_w, exp_w1, exp_b1, exp_w2, exp_b2)
        out = reduce_outputs(partial, hid_f32)
        return out, cache_a_new, cache_b_new

    tok_spec = P(('dp', 'ep'))
    cache_spec = P(None, ('dp', 'ep'))
    rep_spec = P()
    exp_spec = P('ep')
    in_specs = (tok_spec, tok_spec, tok_spec, cache_spec, cache_spec, cache_spec, cache_spec, tok_spec) + (rep_spec,) * 9 + (exp_spec,) * 4
    out_specs = (tok_spec, cache_spec, cache_spec)
    return jax.shard_map(local_step, mesh=mesh, in_specs=in_specs, out_specs=out_specs, check_vma=False)
```

```python
import functools

import jax
import jax.numpy as jnp
from jax import lax
from jax.experimental import pallas as pl
from jax.experimental.pallas import tpu as pltpu
from jax.sharding import PartitionSpec as P

LN_EPS = 1e-5
F32 = jnp.float32
BF16 = jnp.bfloat16
VMEM = pltpu.VMEM


CROSS_GROUP = 16
ROW_STEP = 16
ROW_SHIFT = 4
SELF_GROUP = 16
SELF_UNIT = 2
HEAD_PAD = 16


def norm_rows(x_val, gain_vec, shift_vec):
    mean_val = jnp.mean(x_val, axis=-1, keepdims=True)
    centered = x_val - mean_val
    var_val = jnp.mean(centered * centered, axis=-1, keepdims=True)
    return (centered * lax.rsqrt(var_val + LN_EPS) * gain_vec + shift_vec).astype(BF16)


def dense_kernel(pos_sm, len_sm, hid_ref, gain_ref, shift_ref, ab_ref, fb1_ref, fb2_ref,
                 cache_a, cross_a, cache_b, cross_b, aw_hbm, w1_hbm, w2_hbm,
                 hid_out, z_out, cache_a_out, cache_b_out,
                 w_buf, f1_buf, f2_buf, self_buf, cross_buf, q_s, k_s, v_s, ctx_s, cat_s, lim_s, self_mask, mask_1, mask_2, mask_3, mask_4, order_sm, lists_sm,
                 w_sem, f_sem, in_sem, out_sem, cross_sem):
    tok, d_model = hid_ref.shape
    n_heads, self_len, head_dim = self_buf.shape[2:]
    src = cross_buf.shape[3]
    ff = f1_buf.shape[1]
    scale = head_dim ** -0.5
    cross_masks = (mask_1, mask_2, mask_3, mask_4)
    n_class = len(cross_masks)
    n_self = tok // SELF_GROUP

    def head_rows(b, n):
        return pl.ds(pl.multiple_of(b * HEAD_PAD, HEAD_PAD), n * HEAD_PAD)

    def weight_copy(i):
        return pltpu.make_async_copy(aw_hbm.at[i // 6, i % 6], w_buf.at[i], w_sem.at[i])

    def ffn_copies():
        return (pltpu.make_async_copy(w1_hbm, f1_buf, f_sem.at[0]), pltpu.make_async_copy(w2_hbm, f2_buf, f_sem.at[1]))

    def self_in(cache, g):
        rows = pl.ds(g * SELF_GROUP, SELF_GROUP)
        return pltpu.make_async_copy(cache.at[:, rows], self_buf.at[:, rows], in_sem.at[g])

    def self_out(cache_out, g):
        rows = pl.ds(g * SELF_GROUP, SELF_GROUP)
        return pltpu.make_async_copy(self_buf.at[:, rows], cache_out.at[:, rows], out_sem.at[g])

    def cross_rows(b):
        return pl.multiple_of((lax.shift_right_logical(len_sm[b] - 1, ROW_SHIFT) + 1) * ROW_STEP, ROW_STEP)

    def length_class(b):
        return lax.shift_right_logical(len_sm[b] - 1, ROW_SHIFT)

    def cross_copy(cross, b):
        rows = pl.ds(0, cross_rows(b))
        return pltpu.make_async_copy(cross.at[:, b, :, rows, :], cross_buf.at[b, :, :, rows, :], cross_sem.at[b])

    for i in range(3):
        weight_copy(i).start()
    for g in range(n_self):
        self_in(cache_a, g).start()
    weight_copy(3).start()
    weight_copy(4).start()

    def first_cross(b, sizes):
        cross_copy(cross_a, b).start()
        k = length_class(b)
        size = sizes[0]
        for j in range(1, n_class):
            size = jnp.where(k == j, sizes[j], size)
        lists_sm[k * tok + size] = b
        return tuple(n + jnp.where(k == j, 1, 0) for j, n in enumerate(sizes))
    sizes = lax.fori_loop(0, tok, first_cross, (jnp.int32(0),) * n_class)

    def place(i, c):
        at, end = i, jnp.int32(0)
        for j in range(n_class - 1):
            end = end + sizes[j]
            at = jnp.where(i >= end, (j + 1) * tok + i - end, at)
        order_sm[i] = lists_sm[at]
        return c
    lax.fori_loop(0, tok, place, 0)

    def zero_tail(b, c):
        def zero_part(part, c2):
            cross_buf[b, 1, :, pl.ds(pl.multiple_of(part * 16, 16), 16), :] = jnp.zeros((n_heads, 16, head_dim), BF16)
            return c2
        return lax.fori_loop(length_class(b) + 1, n_class, zero_part, c)
    lax.fori_loop(0, tok, zero_tail, 0)

    def issue_rest():
        weight_copy(5).start()
        for cp in ffn_copies():
            cp.start()
        for i in range(6, 12):
            weight_copy(i).start()

    def build_mask(ref, length):
        row = lax.broadcasted_iota(jnp.int32, ref.shape, 0)
        lane = lax.broadcasted_iota(jnp.int32, ref.shape, 1)
        seq, head = lane // (n_heads * length), (lane // length) % n_heads
        ref[...] = jnp.where(seq * HEAD_PAD + head == row, lane % length, 1 << 20)
    build_mask(self_mask, self_len)
    for mask in cross_masks:
        build_mask(mask, mask.shape[1] // n_heads)

    def fill_limit(b, c):
        lim_s[head_rows(b, 1), :] = jnp.full((HEAD_PAD, 128), pos_sm[b] + 1, jnp.int32)
        return c
    lax.fori_loop(0, tok, fill_limit, 0)

    def to_heads(ref, val):
        val = val.astype(BF16).astype(F32)
        for h in range(n_heads):
            ref[pl.ds(h, tok, stride=HEAD_PAD), :] = val[:, h * head_dim:(h + 1) * head_dim]

    def from_heads(ref):
        for h in range(0, n_heads, 2):
            two = [ref[pl.ds(h + k, tok, stride=HEAD_PAD), :] for k in range(2)]
            cat_s[:, h * head_dim:(h + 2) * head_dim] = jnp.concatenate(two, axis=1).astype(BF16)
        return cat_s[...]

    def softmax_rows(scores, mask, limit):
        scores = jnp.where(mask < limit, scores * scale, -1e30)
        top = jnp.max(scores, axis=-1, keepdims=True)
        ex = jnp.exp(scores - top)
        return (ex * (1.0 / jnp.sum(ex, axis=-1, keepdims=True))).astype(BF16)

    def scores_of(q, keys):
        return lax.dot_general(q, keys, (((1,), (1,)), ((), ())), preferred_element_type=F32)

    def block_diag(blocks):
        rows = []
        for k, blk in enumerate(blocks):
            pad = jnp.zeros_like(blk)
            rows.append(jnp.concatenate([blk if j == k else pad for j in range(len(blocks))], axis=1))
        return jnp.concatenate(rows, axis=0)

    def proj(layer, i, x_bf):
        weight_copy(layer * 6 + i).wait()
        bias = ab_ref[i].astype(F32)[layer:layer + 1, :]
        return jnp.dot(x_bf, w_buf[layer * 6 + i], preferred_element_type=F32) + bias

    def self_layer(layer, h, cache, cache_out):
        x = norm_rows(h, gain_ref[0, layer:layer + 1, :], shift_ref[0, layer:layer + 1, :])
        to_heads(q_s, proj(layer, 0, x))
        to_heads(k_s, proj(layer, 1, x))
        to_heads(v_s, proj(layer, 2, x))
        if layer == 0:
            issue_rest()
        row_i = lax.broadcasted_iota(jnp.int32, (self_len, head_dim), 0)
        row_b = row_i.astype(F32).astype(BF16)

        def body(g, c):
            self_in(cache, g).wait()
            first = g * SELF_GROUP
            sides = []
            for which, new in ((0, k_s), (1, v_s)):
                tiles = []
                for u in range(SELF_GROUP):
                    b = first + u
                    hit = row_b == jnp.full(row_b.shape, pos_sm[b], jnp.int32).astype(F32).astype(BF16)
                    for hd in range(n_heads):
                        row = new[pl.ds(b * HEAD_PAD + hd, self_len, stride=0), :]
                        tile = jnp.where(hit, row.astype(BF16), self_buf[which, b, hd])
                        self_buf[which, b, hd] = tile
                        tiles.append(tile)
                sides.append(tiles)
            n = SELF_UNIT
            parts = range(0, SELF_GROUP, n)
            wide = n * n_heads * self_len
            stack = lambda tiles, p: jnp.concatenate(tiles[p * n_heads:(p + n) * n_heads], axis=0)
            scores = [scores_of(q_s[head_rows(first + p, n), :].astype(BF16), stack(sides[0], p)) for p in parts]
            probs = []
            for p, sc in zip(parts, scores):
                two = 2 * n_heads * self_len
                blocks = []
                for k in range(n // 2):
                    lim = lim_s[head_rows(first + p + 2 * k, 2), :]
                    lim = jnp.concatenate([lim] * (two // 128), axis=1)
                    blocks.append(softmax_rows(sc[k * 2 * HEAD_PAD:(k + 1) * 2 * HEAD_PAD, k * two:(k + 1) * two], self_mask[...], lim))
                probs.append(block_diag(blocks))
            for p, pr in zip(parts, probs):
                ctx_s[head_rows(first + p, n), :] = jnp.dot(pr, stack(sides[1], p), preferred_element_type=F32)
            self_out(cache_out, g).start()
            return c
        lax.fori_loop(0, n_self, body, 0)
        ctx = from_heads(ctx_s)
        return h + proj(layer, 3, ctx)

    def cross_layer(layer, h, cross, after):
        x = norm_rows(h, gain_ref[1, layer:layer + 1, :], shift_ref[1, layer:layer + 1, :])
        to_heads(q_s, proj(layer, 4, x))

        def body(g, c):
            group = [order_sm[g * CROSS_GROUP + u] for u in range(CROSS_GROUP)]
            longest = length_class(group[-1])
            for b in group:
                cross_copy(cross, b).wait()
            for k, mask in enumerate(cross_masks):
                @pl.when(longest == k)
                def _():
                    rows = mask.shape[1] // n_heads
                    side = lambda b, which: cross_buf[b, which, :, 0:rows, :].reshape(n_heads * rows, head_dim)
                    scores = [scores_of(q_s[head_rows(b, 1), :].astype(BF16), side(b, 0)) for b in group]
                    probs = [softmax_rows(sc, mask[...], len_sm[b]) for b, sc in zip(group, scores)]
                    for b, pr in zip(group, probs):
                        ctx_s[head_rows(b, 1), :] = jnp.dot(pr, side(b, 1), preferred_element_type=F32)
            if after is not None:
                for b in group:
                    cross_copy(after, b).start()
            return c
        lax.fori_loop(0, tok // CROSS_GROUP, body, 0)
        ctx = from_heads(ctx_s)
        return h + proj(layer, 5, ctx)

    q_s[...] = jnp.zeros_like(q_s)
    h = hid_ref[...].astype(F32)
    h = self_layer(0, h, cache_a, cache_a_out)
    for g in range(n_self):
        self_out(cache_a_out, g).wait()
        self_in(cache_b, g).start()
    h = cross_layer(0, h, cross_a, cross_b)
    x = norm_rows(h, gain_ref[2, 0:1, :], shift_ref[2, 0:1, :])
    for cp in ffn_copies():
        cp.wait()
    acc = h + fb2_ref[...].astype(F32).reshape(1, d_model)
    for f in range(0, ff, d_model):
        inner = jnp.dot(x, f1_buf[:, f:f + d_model], preferred_element_type=F32) + fb1_ref[f:f + d_model].astype(F32).reshape(1, d_model)
        inner = jnp.maximum(inner, 0.0).astype(BF16)
        acc = acc + jnp.dot(inner, f2_buf[f:f + d_model, :], preferred_element_type=F32)
    h = acc
    h = self_layer(1, h, cache_b, cache_b_out)
    h = cross_layer(1, h, cross_b, None)
    hid_out[...] = h
    z_out[...] = norm_rows(h, gain_ref[2, 1:2, :], shift_ref[2, 1:2, :])
    for g in range(n_self):
        self_out(cache_b_out, g).wait()


def dense_layers(hidden, self_pos, src_len, cache_a, cross_a, cache_b, cross_b, ln_gain, ln_shift, attn_w, attn_b, ffn_w1, ffn_b1, ffn_w2, ffn_b2):
    tok, d_model = hidden.shape
    n_heads, head_dim = cache_a.shape[3:]
    self_len, src = cache_a.shape[2], cross_a.shape[2]
    ff = ffn_w1.shape[1]
    swap = lambda arr: jnp.swapaxes(arr, 2, 3)
    sm = pl.BlockSpec(memory_space=pltpu.SMEM)
    vm = pl.BlockSpec(memory_space=VMEM)
    hbm = pl.BlockSpec(memory_space=pl.ANY)
    cache_t = jax.ShapeDtypeStruct((2, tok, n_heads, self_len, head_dim), BF16)
    n_self = tok // SELF_GROUP
    heads = VMEM((tok * HEAD_PAD, head_dim), F32)
    hid, z, out_a, out_b = pl.pallas_call(
        dense_kernel,
        out_shape=[VMEM((tok, d_model), F32), VMEM((tok, d_model), BF16), cache_t, cache_t],
        in_specs=[sm] * 2 + [vm] * 6 + [hbm] * 7,
        out_specs=[vm] * 2 + [hbm] * 2,
        scratch_shapes=[
            VMEM((12, d_model, d_model), BF16), VMEM((d_model, ff), BF16), VMEM((ff, d_model), BF16),
            VMEM((2, tok, n_heads, self_len, head_dim), BF16), VMEM((tok, 2, n_heads, src, head_dim), BF16),
            heads, heads, heads, heads, VMEM((tok, d_model), BF16), VMEM((tok * HEAD_PAD, 128), jnp.int32),
            VMEM((2 * HEAD_PAD, 2 * n_heads * self_len), jnp.int32), ] + [VMEM((HEAD_PAD, n_heads * rows), jnp.int32) for rows in range(ROW_STEP, src + 1, ROW_STEP)] + [
            pltpu.SMEM((tok,), jnp.int32), pltpu.SMEM((src // ROW_STEP * tok,), jnp.int32),
            pltpu.SemaphoreType.DMA((12,)), pltpu.SemaphoreType.DMA((2,)), pltpu.SemaphoreType.DMA((n_self,)),
            pltpu.SemaphoreType.DMA((n_self,)), pltpu.SemaphoreType.DMA((tok,)),
        ],
        compiler_params=pltpu.CompilerParams(vmem_limit_bytes=61 * 1024 * 1024),
        name='dense_layers',
    )(self_pos, src_len, hidden, jnp.swapaxes(ln_gain, 0, 1), jnp.swapaxes(ln_shift, 0, 1), jnp.swapaxes(attn_b, 0, 1), ffn_b1, ffn_b2,
      swap(cache_a), swap(cross_a), swap(cache_b), swap(cross_b), attn_w, ffn_w1, ffn_w2)
    return hid, z, swap(out_a), swap(out_b)


def peer(index):
    return dict(device_id={'ep': index}, device_id_type=pl.DeviceIdType.MESH)


def neighbours():
    me = lax.axis_index('ep')
    core, x, y = me % 2, (me // 2) % 2, me // 4
    at = lambda yy, xx, cc: (yy * 2 + xx) * 2 + cc
    return me, core, x, y, at


def entry_barrier(others):
    barrier = pltpu.get_barrier_semaphore()
    for other in others:
        pl.semaphore_signal(barrier, inc=1, **peer(other))
    pl.semaphore_wait(barrier, len(others))


def named_experts(ids_cols, base, n_loc):
    n_tok = ids_cols.shape[0]
    lane = lax.broadcasted_iota(jnp.int32, (n_tok, 128), 1)
    id0 = ids_cols[:, 0:1].astype(jnp.int32) - base
    id1 = ids_cols[:, 1:2].astype(jnp.int32) - base
    hit = jnp.logical_and(jnp.logical_or(id0 == lane, id1 == lane), lane < n_loc)
    return id0, id1, lane, hit.astype(F32)


def gather_kernel(n_loc, z_ref, idst_ref, zall_ref, cols_ref, meta_ref, flip, ids_ref, idsall, send_sem, recv_sem):
    me, core, x, y, at = neighbours()
    twin = at(y, x, 1 - core)
    chips = [(y, 1 - x), (1 - y, x), (1 - y, 1 - x)]
    tok = z_ref.shape[0]
    group_n = zall_ref.shape[0]
    ids_ref[...] = jnp.zeros_like(ids_ref)
    ids_ref[0:2, 0:tok] = idst_ref[...].astype(F32)
    entry_barrier([twin] + [at(cy, cx, core) for cy, cx in chips])

    def send(slot, which, src, row, to):
        dst = (idsall, zall_ref)[which]
        cp = pltpu.make_async_remote_copy(
            src_ref=src, dst_ref=dst.at[row], send_sem=send_sem.at[slot, which], recv_sem=recv_sem.at[slot, which], **peer(to))
        cp.start()
        return cp

    far = [at(cy, cx, core) for cy, cx in chips]
    ids_sent = [send(j, 0, ids_ref, me, far[j]) for j in range(3)] + [send(3, 0, ids_ref, me, twin)]
    z_sent = {j: send(j, 1, z_ref, me, far[j]) for j in (2, 0, 1)}
    z_sent[3] = send(3, 1, z_ref, me, twin)
    zall_ref[me] = z_ref[...]
    idsall[me] = ids_ref[...]
    relays = []
    for j in range(3):
        ids_sent[j].wait_recv()
        relays.append(send(4 + j, 0, idsall.at[far[j]], far[j], twin))
    ids_sent[3].wait_recv()
    for cp in relays:
        cp.wait_recv()

    flip[...] = jnp.zeros_like(flip)
    for d in range(group_n):
        flip[2 * d:2 * d + 2, :] = idsall[d, 0:2, :]
    cols = jnp.transpose(flip[...])[:tok]
    lane_b = lax.broadcasted_iota(jnp.int32, (tok, 128), 1)
    wide = [jnp.where(lane_b == 0, cols[:, 2 * d:2 * d + 1], cols[:, 2 * d + 1:2 * d + 2]) for d in range(group_n)]
    cols_ref[...] = jnp.concatenate(wide, axis=0)
    _, _, _, hit = named_experts(cols_ref[...], me * n_loc, n_loc)
    ones = jnp.ones((group_n * tok, 128), BF16)
    count = lax.dot_general(hit.astype(BF16), ones, (((0,), (0,)), ((), ())), preferred_element_type=F32)
    row_i = lax.broadcasted_iota(jnp.int32, (128, 128), 0)
    col_i = lax.broadcasted_iota(jnp.int32, (128, 128), 1)
    named = (count > 0.5).astype(F32)
    order = jnp.dot((row_i > col_i).astype(BF16), named.astype(BF16), preferred_element_type=F32)
    spot = jnp.where(order == col_i.astype(F32), named, 0.0)
    expert_list = jnp.sum(spot * row_i.astype(F32), axis=0, keepdims=True)
    counts = jnp.sum(hit, axis=0, keepdims=True)
    total = jnp.sum(named, axis=0, keepdims=True)
    meta_ref[...] = jnp.concatenate([counts, expert_list, total, jnp.zeros((5, 128), F32)], axis=0).astype(jnp.int32)

    z_relays = []
    for j in (0, 1, 2):
        z_sent[j].wait_recv()
        z_relays.append(send(4 + j, 1, zall_ref.at[far[j]], far[j], twin))
    z_sent[3].wait_recv()
    for cp in z_relays:
        cp.wait_recv()
    for cp in ids_sent + relays + list(z_sent.values()) + z_relays:
        cp.wait_send()


def in_vmem(arr):
    return pltpu.with_memory_space_constraint(arr, VMEM)


def gather_tokens(z_bf, ids_t, group_n, n_loc):
    tok, d_model = z_bf.shape
    return pl.pallas_call(
        functools.partial(gather_kernel, n_loc),
        out_shape=[VMEM((group_n, tok, d_model), BF16), VMEM((group_n * tok, 128), F32), jax.ShapeDtypeStruct((8, 128), jnp.int32)],
        in_specs=[pl.BlockSpec(memory_space=VMEM)] * 2,
        out_specs=[pl.BlockSpec(memory_space=VMEM)] * 3,
        scratch_shapes=[VMEM((128, 128), F32), VMEM((8, 128), F32), VMEM((group_n, 8, 128), F32),
                        pltpu.SemaphoreType.DMA((7, 2)), pltpu.SemaphoreType.DMA((7, 2))],
        compiler_params=pltpu.CompilerParams(collective_id=0, has_side_effects=True, vmem_limit_bytes=16 * 1024 * 1024),
        name='gather_tokens',
    )(in_vmem(z_bf), ids_t)


def reduce_kernel(part_ref, hid_ref, out_ref, r1, s1, r2, s2, r3, send_sem, recv_sem):
    me, core, x, y, at = neighbours()
    twin, xn, yn = at(y, x, 1 - core), at(y, 1 - x, core), at(1 - y, x, core)
    entry_barrier([twin, xn, yn])
    half = hid_ref.shape[1] // 2
    cols = (pl.ds(0, half), pl.ds(half, half))

    def send(slot, src, dst, to):
        cp = pltpu.make_async_remote_copy(src_ref=src, dst_ref=dst, send_sem=send_sem.at[slot], recv_sem=recv_sem.at[slot], **peer(to))
        cp.start()
        return cp

    chips = [(1 - y, 1 - x), (y, 1 - x), (1 - y, x), (y, x)]
    first = [send(k, part_ref.at[at(cy, cx, 1 - core)], r1.at[k], twin) for k, (cy, cx) in enumerate(chips)]

    def sum1(k):
        first[k].wait_recv()
        cy, cx = chips[k]
        s1[k] = part_ref[at(cy, cx, core)] + r1[k]

    sum1(0)
    a0 = send(4, s1.at[0, :, cols[0]], r2.at[0, 0], xn)
    b0 = send(5, s1.at[0, :, cols[1]], r2.at[1, 0], yn)
    sum1(1)
    a1 = send(6, s1.at[1, :, cols[0]], r2.at[0, 1], xn)
    sum1(2)
    b1 = send(7, s1.at[2, :, cols[1]], r2.at[1, 1], yn)
    sum1(3)
    a0.wait_recv()
    s2[0] = s1[2, :, :half] + r2[0, 0]
    a2 = send(8, s2.at[0], r3.at[0], yn)
    b0.wait_recv()
    s2[1] = s1[1, :, half:] + r2[1, 0]
    b2 = send(9, s2.at[1], r3.at[1], xn)
    a1.wait_recv()
    own_a = hid_ref[:, :half] + s1[3, :, :half] + r2[0, 1]
    b1.wait_recv()
    own_b = hid_ref[:, half:] + s1[3, :, half:] + r2[1, 1]
    a2.wait_recv()
    out_ref[:, :half] = (own_a + r3[0]).astype(BF16)
    b2.wait_recv()
    out_ref[:, half:] = (own_b + r3[1]).astype(BF16)
    for cp in first + [a0, b0, a1, b1, a2, b2]:
        cp.wait_send()


def reduce_outputs(partial, hid_f32):
    group_n, tok, d_model = partial.shape
    half = d_model // 2
    return pl.pallas_call(
        reduce_kernel,
        out_shape=VMEM((tok, d_model), BF16),
        in_specs=[pl.BlockSpec(memory_space=VMEM)] * 2,
        out_specs=pl.BlockSpec(memory_space=VMEM),
        scratch_shapes=[
            VMEM((4, tok, d_model), F32), VMEM((4, tok, d_model), F32),
            VMEM((2, 2, tok, half), F32), VMEM((2, tok, half), F32), VMEM((2, tok, half), F32),
            pltpu.SemaphoreType.DMA((10,)), pltpu.SemaphoreType.DMA((10,)),
        ],
        compiler_params=pltpu.CompilerParams(collective_id=1, has_side_effects=True, vmem_limit_bytes=16 * 1024 * 1024),
        name='reduce_outputs',
    )(in_vmem(partial), in_vmem(hid_f32))


ROWS = 64
SPLIT = 2
SLOTS = 6


def expert_kernel(meta_sm, z_ref, cols_ref, rw_ref, b1_in, b2_in, w1_hbm, w2_hbm, out_ref,
                  b1_ref, b2_ref, w1_buf, w2_buf, rank_s, gate_s, x_s, o_s, sem1, sem2):
    n_tok, d_model = cols_ref.shape[0], z_ref.shape[2]
    n_loc = w1_hbm.shape[0]
    ff = w1_hbm.shape[2]
    fc = ff // SPLIT
    n_step = meta_sm[2, 0] * SPLIT

    def copies(step, slot):
        e = meta_sm[1, step // SPLIT]
        f0 = pl.multiple_of((step % SPLIT) * fc, fc)
        return (pltpu.make_async_copy(w1_hbm.at[e, :, pl.ds(f0, fc)], w1_buf.at[slot], sem1.at[slot]),
                pltpu.make_async_copy(w2_hbm.at[e, pl.ds(f0, fc), :], w2_buf.at[slot], sem2.at[slot]))

    for s in range(SLOTS):
        @pl.when(s < n_step)
        def _():
            for c in copies(s, s):
                c.start()

    b1_ref[...] = b1_in[...].astype(F32)
    b2_ref[...] = b2_in[...].astype(F32)
    z_all = z_ref[...].reshape(n_tok, d_model)
    id0, id1, lane, hit_t = named_experts(cols_ref[...], lax.axis_index('ep') * n_loc, n_loc)
    base = lax.axis_index('ep') * n_loc
    row_i = lax.broadcasted_iota(jnp.int32, (n_tok, n_tok), 0)
    col_i = lax.broadcasted_iota(jnp.int32, (n_tok, n_tok), 1)
    before = (row_i < col_i).astype(BF16)
    hit = jnp.transpose(hit_t)
    rank = jnp.dot(hit.astype(BF16), before, preferred_element_type=F32)
    rank_s[...] = jnp.where(hit > 0.5, rank, -1.0)

    logits = jnp.dot(z_all, rw_ref[...], preferred_element_type=F32)
    top = jnp.max(logits, axis=-1, keepdims=True)
    ex = jnp.exp(logits - top)
    probs = ex / jnp.sum(ex, axis=-1, keepdims=True)
    p0 = jnp.sum(jnp.where(lane == id0 + base, probs, 0.0), axis=-1, keepdims=True)
    p1 = jnp.sum(jnp.where(lane == id1 + base, probs, 0.0), axis=-1, keepdims=True)
    tot = p0 + p1
    g0, g1 = p0 / tot, p1 / tot
    gate_s[...] = jnp.where(lane == id0, g0, jnp.where(lane == id1, g1, 0.0))
    out_ref[...] = jnp.zeros_like(out_ref)

    def step_body(step, carry):
        slot = step % SLOTS
        e = meta_sm[1, step // SPLIT]
        part = step % SPLIT
        blocks = (meta_sm[0, e] + ROWS - 1) // ROWS
        slot_i = lax.broadcasted_iota(jnp.int32, (ROWS, n_tok), 0)

        def pick(j):
            want = (slot_i + j * ROWS).astype(F32)
            return (want == rank_s[pl.ds(e, 1), :]).astype(BF16)

        @pl.when(part == 0)
        def _():
            def gather_body(j, c):
                x_s[j] = jnp.dot(pick(j), z_ref[...].reshape(n_tok, d_model), preferred_element_type=F32).astype(BF16)
                o_s[j] = jnp.broadcast_to(b2_ref[pl.ds(e, 1), :], (ROWS, d_model))
                return c
            lax.fori_loop(0, blocks, gather_body, 0)

        for c in copies(step, slot):
            c.wait()
        bias = b1_ref[pl.ds(e, 1), pl.ds(pl.multiple_of(part * fc, fc), fc)]

        def block_body(j, c):
            inner = jnp.dot(x_s[j], w1_buf[slot], preferred_element_type=F32) + bias
            inner = jnp.maximum(inner, 0.0).astype(BF16)
            o_s[j] += jnp.dot(inner, w2_buf[slot], preferred_element_type=F32)
            return c
        lax.fori_loop(0, blocks, block_body, 0)

        @pl.when(step + SLOTS < n_step)
        def _():
            for c in copies(step + SLOTS, slot):
                c.start()

        @pl.when(part == SPLIT - 1)
        def _():
            lane_g = lax.broadcasted_iota(jnp.int32, (n_tok, 128), 1)
            gate = jnp.sum(jnp.where(lane_g == e, gate_s[...], 0.0), axis=-1, keepdims=True)

            def scatter_body(j, c):
                back = lax.dot_general(pick(j), o_s[j].astype(BF16), (((0,), (0,)), ((), ())), preferred_element_type=F32)
                out_ref[...] += (gate * back).reshape(out_ref.shape)
                return c
            lax.fori_loop(0, blocks, scatter_body, 0)
        return carry

    lax.fori_loop(0, n_step, step_body, 0)


def run_experts(meta, z_all, cols, router_w, exp_w1, exp_b1, exp_w2, exp_b2):
    group_n, tok, d_model = z_all.shape
    n_tok = group_n * tok
    n_loc, _, ff = exp_w1.shape
    fc = ff // SPLIT
    n_blk = n_tok // ROWS
    vm = pl.BlockSpec(memory_space=VMEM)
    hbm = pl.BlockSpec(memory_space=pl.ANY)
    return pl.pallas_call(
        expert_kernel,
        out_shape=VMEM((group_n, tok, d_model), F32),
        in_specs=[pl.BlockSpec(memory_space=pltpu.SMEM)] + [vm] * 5 + [hbm] * 2,
        out_specs=vm,
        scratch_shapes=[
            VMEM((n_loc, ff), F32), VMEM((n_loc, d_model), F32),
            VMEM((SLOTS, d_model, fc), BF16), VMEM((SLOTS, fc, d_model), BF16),
            VMEM((128, n_tok), F32), VMEM((n_tok, 128), F32),
            VMEM((n_blk, ROWS, d_model), BF16), VMEM((n_blk, ROWS, d_model), F32),
            pltpu.SemaphoreType.DMA((SLOTS,)), pltpu.SemaphoreType.DMA((SLOTS,)),
        ],
        compiler_params=pltpu.CompilerParams(vmem_limit_bytes=48 * 1024 * 1024),
        name='run_experts',
    )(meta, in_vmem(z_all), in_vmem(cols), router_w, exp_b1, exp_b2, exp_w1, exp_w2)


def solution(mesh):
    group_n = mesh.shape['ep']

    def local_step(hidden, self_pos, src_len, cache_a, cross_a, cache_b, cross_b, route_ids, ln_gain, ln_shift, attn_w, attn_b, ffn_w1, ffn_b1, ffn_w2, ffn_b2, router_w, exp_w1, exp_b1, exp_w2, exp_b2):
        hid_f32, z_bf, cache_a_new, cache_b_new = dense_layers(hidden, self_pos, src_len, cache_a, cross_a, cache_b, cross_b, ln_gain, ln_shift, attn_w, attn_b, ffn_w1, ffn_b1, ffn_w2, ffn_b2)
        z_all, cols, meta = gather_tokens(z_bf, route_ids.T, group_n, exp_w1.shape[0])
        partial = run_experts(meta, z_all, cols, router_w, exp_w1, exp_b1, exp_w2, exp_b2)
        out = reduce_outputs(partial, hid_f32)
        return out, cache_a_new, cache_b_new

    tok_spec = P(('dp', 'ep'))
    cache_spec = P(None, ('dp', 'ep'))
    rep_spec = P()
    exp_spec = P('ep')
    in_specs = (tok_spec, tok_spec, tok_spec, cache_spec, cache_spec, cache_spec, cache_spec, tok_spec) + (rep_spec,) * 9 + (exp_spec,) * 4
    out_specs = (tok_spec, cache_spec, cache_spec)
    return jax.shard_map(local_step, mesh=mesh, in_specs=in_specs, out_specs=out_specs, check_vma=False)
```

```python
import functools

import jax
import jax.numpy as jnp
from jax import lax
from jax.experimental import pallas as pl
from jax.experimental.pallas import tpu as pltpu
from jax.sharding import PartitionSpec as P

LN_EPS = 1e-5
F32 = jnp.float32
BF16 = jnp.bfloat16
VMEM = pltpu.VMEM


CROSS_GROUP = 16
ROW_STEP = 16
ROW_SHIFT = 4
SELF_GROUP = 16
SELF_UNIT = 2
HEAD_PAD = 16


def norm_rows(x_val, gain_vec, shift_vec):
    mean_val = jnp.mean(x_val, axis=-1, keepdims=True)
    centered = x_val - mean_val
    var_val = jnp.mean(centered * centered, axis=-1, keepdims=True)
    return (centered * lax.rsqrt(var_val + LN_EPS) * gain_vec + shift_vec).astype(BF16)


def dense_kernel(pos_sm, len_sm, hid_ref, gain_ref, shift_ref, ab_ref, fb1_ref, fb2_ref,
                 cache_a, cross_a, cache_b, cross_b, aw_hbm, w1_hbm, w2_hbm,
                 hid_out, z_out, cache_a_out, cache_b_out,
                 w_buf, f1_buf, f2_buf, self_buf, cross_buf, q_s, k_s, v_s, ctx_s, cat_s, lim_s, self_mask, mask_1, mask_2, mask_3, mask_4, order_sm, lists_sm,
                 w_sem, f_sem, in_sem, out_sem, cross_sem):
    tok, d_model = hid_ref.shape
    n_heads, self_len, head_dim = self_buf.shape[2:]
    src = cross_buf.shape[3]
    ff = f1_buf.shape[1]
    scale = head_dim ** -0.5
    cross_masks = (mask_1, mask_2, mask_3, mask_4)
    n_class = len(cross_masks)
    n_self = tok // SELF_GROUP

    def head_rows(b, n):
        return pl.ds(pl.multiple_of(b * HEAD_PAD, HEAD_PAD), n * HEAD_PAD)

    def weight_copy(i):
        return pltpu.make_async_copy(aw_hbm.at[i // 6, i % 6], w_buf.at[i], w_sem.at[i])

    def ffn_copies():
        return (pltpu.make_async_copy(w1_hbm, f1_buf, f_sem.at[0]), pltpu.make_async_copy(w2_hbm, f2_buf, f_sem.at[1]))

    def self_in(cache, g):
        rows = pl.ds(g * SELF_GROUP, SELF_GROUP)
        return pltpu.make_async_copy(cache.at[:, rows], self_buf.at[:, rows], in_sem.at[g])

    def self_out(cache_out, g):
        rows = pl.ds(g * SELF_GROUP, SELF_GROUP)
        return pltpu.make_async_copy(self_buf.at[:, rows], cache_out.at[:, rows], out_sem.at[g])

    def cross_rows(b):
        return pl.multiple_of((lax.shift_right_logical(len_sm[b] - 1, ROW_SHIFT) + 1) * ROW_STEP, ROW_STEP)

    def length_class(b):
        return lax.shift_right_logical(len_sm[b] - 1, ROW_SHIFT)

    def cross_copy(cross, b):
        rows = pl.ds(0, cross_rows(b))
        return pltpu.make_async_copy(cross.at[:, b, :, rows, :], cross_buf.at[b, :, :, rows, :], cross_sem.at[b])

    for i in range(3):
        weight_copy(i).start()
    for g in range(n_self):
        self_in(cache_a, g).start()
    weight_copy(3).start()
    weight_copy(4).start()

    def first_cross(b, sizes):
        cross_copy(cross_a, b).start()
        k = length_class(b)
        size = sizes[0]
        for j in range(1, n_class):
            size = jnp.where(k == j, sizes[j], size)
        lists_sm[k * tok + size] = b
        return tuple(n + jnp.where(k == j, 1, 0) for j, n in enumerate(sizes))
    sizes = lax.fori_loop(0, tok, first_cross, (jnp.int32(0),) * n_class)

    def place(i, c):
        at, end = i, jnp.int32(0)
        for j in range(n_class - 1):
            end = end + sizes[j]
            at = jnp.where(i >= end, (j + 1) * tok + i - end, at)
        order_sm[i] = lists_sm[at]
        return c
    lax.fori_loop(0, tok, place, 0)

    def zero_tail(b, c):
        def zero_part(part, c2):
            cross_buf[b, 1, :, pl.ds(pl.multiple_of(part * 16, 16), 16), :] = jnp.zeros((n_heads, 16, head_dim), BF16)
            return c2
        return lax.fori_loop(length_class(b) + 1, n_class, zero_part, c)

    def issue_rest():
        weight_copy(5).start()
        for cp in ffn_copies():
            cp.start()
        for i in range(6, 12):
            weight_copy(i).start()
        lax.fori_loop(0, tok, zero_tail, 0)

    def build_mask(ref, length):
        row = lax.broadcasted_iota(jnp.int32, ref.shape, 0)
        lane = lax.broadcasted_iota(jnp.int32, ref.shape, 1)
        seq, head = lane // (n_heads * length), (lane // length) % n_heads
        ref[...] = jnp.where(seq * HEAD_PAD + head == row, lane % length, 1 << 20)
    build_mask(self_mask, self_len)
    for mask in cross_masks:
        build_mask(mask, mask.shape[1] // n_heads)

    def fill_limit(b, c):
        lim_s[head_rows(b, 1), :] = jnp.full((HEAD_PAD, 128), pos_sm[b] + 1, jnp.int32)
        return c
    lax.fori_loop(0, tok, fill_limit, 0)

    def to_heads(ref, val):
        val = val.astype(BF16).astype(F32)
        for h in range(n_heads):
            ref[pl.ds(h, tok, stride=HEAD_PAD), :] = val[:, h * head_dim:(h + 1) * head_dim]

    def from_heads(ref):
        for h in range(0, n_heads, 2):
            two = [ref[pl.ds(h + k, tok, stride=HEAD_PAD), :] for k in range(2)]
            cat_s[:, h * head_dim:(h + 2) * head_dim] = jnp.concatenate(two, axis=1).astype(BF16)
        return cat_s[...]

    def softmax_rows(scores, mask, limit):
        scores = jnp.where(mask < limit, scores * scale, -1e30)
        top = jnp.max(scores, axis=-1, keepdims=True)
        ex = jnp.exp(scores - top)
        return (ex * (1.0 / jnp.sum(ex, axis=-1, keepdims=True))).astype(BF16)

    def scores_of(q, keys):
        return lax.dot_general(q, keys, (((1,), (1,)), ((), ())), preferred_element_type=F32)

    def block_diag(blocks):
        rows = []
        for k, blk in enumerate(blocks):
            pad = jnp.zeros_like(blk)
            rows.append(jnp.concatenate([blk if j == k else pad for j in range(len(blocks))], axis=1))
        return jnp.concatenate(rows, axis=0)

    def proj(layer, i, x_bf):
        weight_copy(layer * 6 + i).wait()
        bias = ab_ref[i].astype(F32)[layer:layer + 1, :]
        return jnp.dot(x_bf, w_buf[layer * 6 + i], preferred_element_type=F32) + bias

    def self_layer(layer, h, cache, cache_out):
        x = norm_rows(h, gain_ref[0, layer:layer + 1, :], shift_ref[0, layer:layer + 1, :])
        to_heads(q_s, proj(layer, 0, x))
        to_heads(k_s, proj(layer, 1, x))
        to_heads(v_s, proj(layer, 2, x))
        if layer == 0:
            issue_rest()
        row_i = lax.broadcasted_iota(jnp.int32, (self_len, head_dim), 0)
        row_b = row_i.astype(F32).astype(BF16)

        def body(g, c):
            self_in(cache, g).wait()
            first = g * SELF_GROUP
            sides = []
            for which, new in ((0, k_s), (1, v_s)):
                tiles = []
                for u in range(SELF_GROUP):
                    b = first + u
                    hit = row_b == jnp.full(row_b.shape, pos_sm[b], jnp.int32).astype(F32).astype(BF16)
                    for hd in range(n_heads):
                        row = new[pl.ds(b * HEAD_PAD + hd, self_len, stride=0), :]
                        tile = jnp.where(hit, row.astype(BF16), self_buf[which, b, hd])
                        self_buf[which, b, hd] = tile
                        tiles.append(tile)
                sides.append(tiles)
            n = SELF_UNIT
            parts = range(0, SELF_GROUP, n)
            wide = n * n_heads * self_len
            stack = lambda tiles, p: jnp.concatenate(tiles[p * n_heads:(p + n) * n_heads], axis=0)
            scores = [scores_of(q_s[head_rows(first + p, n), :].astype(BF16), stack(sides[0], p)) for p in parts]
            probs = []
            for p, sc in zip(parts, scores):
                two = 2 * n_heads * self_len
                blocks = []
                for k in range(n // 2):
                    lim = lim_s[head_rows(first + p + 2 * k, 2), :]
                    lim = jnp.concatenate([lim] * (two // 128), axis=1)
                    blocks.append(softmax_rows(sc[k * 2 * HEAD_PAD:(k + 1) * 2 * HEAD_PAD, k * two:(k + 1) * two], self_mask[...], lim))
                probs.append(block_diag(blocks))
            for p, pr in zip(parts, probs):
                ctx_s[head_rows(first + p, n), :] = jnp.dot(pr, stack(sides[1], p), preferred_element_type=F32)
            self_out(cache_out, g).start()
            return c
        lax.fori_loop(0, n_self, body, 0)
        ctx = from_heads(ctx_s)
        return h + proj(layer, 3, ctx)

    def cross_layer(layer, h, cross, after):
        x = norm_rows(h, gain_ref[1, layer:layer + 1, :], shift_ref[1, layer:layer + 1, :])
        to_heads(q_s, proj(layer, 4, x))

        def body(g, c):
            group = [order_sm[g * CROSS_GROUP + u] for u in range(CROSS_GROUP)]
            longest = length_class(group[-1])
            for b in group:
                cross_copy(cross, b).wait()
            for k, mask in enumerate(cross_masks):
                @pl.when(longest == k)
                def _():
                    rows = mask.shape[1] // n_heads
                    side = lambda b, which: cross_buf[b, which, :, 0:rows, :].reshape(n_heads * rows, head_dim)
                    scores = [scores_of(q_s[head_rows(b, 1), :].astype(BF16), side(b, 0)) for b in group]
                    probs = [softmax_rows(sc, mask[...], len_sm[b]) for b, sc in zip(group, scores)]
                    for b, pr in zip(group, probs):
                        ctx_s[head_rows(b, 1), :] = jnp.dot(pr, side(b, 1), preferred_element_type=F32)
            if after is not None:
                for b in group:
                    cross_copy(after, b).start()
            return c
        lax.fori_loop(0, tok // CROSS_GROUP, body, 0)
        ctx = from_heads(ctx_s)
        return h + proj(layer, 5, ctx)

    q_s[...] = jnp.zeros_like(q_s)
    h = hid_ref[...].astype(F32)
    h = self_layer(0, h, cache_a, cache_a_out)
    for g in range(n_self):
        self_out(cache_a_out, g).wait()
        self_in(cache_b, g).start()
    h = cross_layer(0, h, cross_a, cross_b)
    x = norm_rows(h, gain_ref[2, 0:1, :], shift_ref[2, 0:1, :])
    for cp in ffn_copies():
        cp.wait()
    acc = h + fb2_ref[...].astype(F32).reshape(1, d_model)
    for f in range(0, ff, d_model):
        inner = jnp.dot(x, f1_buf[:, f:f + d_model], preferred_element_type=F32) + fb1_ref[f:f + d_model].astype(F32).reshape(1, d_model)
        inner = jnp.maximum(inner, 0.0).astype(BF16)
        acc = acc + jnp.dot(inner, f2_buf[f:f + d_model, :], preferred_element_type=F32)
    h = acc
    h = self_layer(1, h, cache_b, cache_b_out)
    h = cross_layer(1, h, cross_b, None)
    hid_out[...] = h
    z_out[...] = norm_rows(h, gain_ref[2, 1:2, :], shift_ref[2, 1:2, :])
    for g in range(n_self):
        self_out(cache_b_out, g).wait()


def dense_layers(hidden, self_pos, src_len, cache_a, cross_a, cache_b, cross_b, ln_gain, ln_shift, attn_w, attn_b, ffn_w1, ffn_b1, ffn_w2, ffn_b2):
    tok, d_model = hidden.shape
    n_heads, head_dim = cache_a.shape[3:]
    self_len, src = cache_a.shape[2], cross_a.shape[2]
    ff = ffn_w1.shape[1]
    swap = lambda arr: jnp.swapaxes(arr, 2, 3)
    sm = pl.BlockSpec(memory_space=pltpu.SMEM)
    vm = pl.BlockSpec(memory_space=VMEM)
    hbm = pl.BlockSpec(memory_space=pl.ANY)
    cache_t = jax.ShapeDtypeStruct((2, tok, n_heads, self_len, head_dim), BF16)
    n_self = tok // SELF_GROUP
    heads = VMEM((tok * HEAD_PAD, head_dim), F32)
    hid, z, out_a, out_b = pl.pallas_call(
        dense_kernel,
        out_shape=[VMEM((tok, d_model), F32), VMEM((tok, d_model), BF16), cache_t, cache_t],
        in_specs=[sm] * 2 + [vm] * 6 + [hbm] * 7,
        out_specs=[vm] * 2 + [hbm] * 2,
        scratch_shapes=[
            VMEM((12, d_model, d_model), BF16), VMEM((d_model, ff), BF16), VMEM((ff, d_model), BF16),
            VMEM((2, tok, n_heads, self_len, head_dim), BF16), VMEM((tok, 2, n_heads, src, head_dim), BF16),
            heads, heads, heads, heads, VMEM((tok, d_model), BF16), VMEM((tok * HEAD_PAD, 128), jnp.int32),
            VMEM((2 * HEAD_PAD, 2 * n_heads * self_len), jnp.int32), ] + [VMEM((HEAD_PAD, n_heads * rows), jnp.int32) for rows in range(ROW_STEP, src + 1, ROW_STEP)] + [
            pltpu.SMEM((tok,), jnp.int32), pltpu.SMEM((src // ROW_STEP * tok,), jnp.int32),
            pltpu.SemaphoreType.DMA((12,)), pltpu.SemaphoreType.DMA((2,)), pltpu.SemaphoreType.DMA((n_self,)),
            pltpu.SemaphoreType.DMA((n_self,)), pltpu.SemaphoreType.DMA((tok,)),
        ],
        compiler_params=pltpu.CompilerParams(vmem_limit_bytes=61 * 1024 * 1024),
        name='dense_layers',
    )(self_pos, src_len, hidden, jnp.swapaxes(ln_gain, 0, 1), jnp.swapaxes(ln_shift, 0, 1), jnp.swapaxes(attn_b, 0, 1), ffn_b1, ffn_b2,
      swap(cache_a), swap(cross_a), swap(cache_b), swap(cross_b), attn_w, ffn_w1, ffn_w2)
    return hid, z, swap(out_a), swap(out_b)


def peer(index):
    return dict(device_id={'ep': index}, device_id_type=pl.DeviceIdType.MESH)


def neighbours():
    me = lax.axis_index('ep')
    core, x, y = me % 2, (me // 2) % 2, me // 4
    at = lambda yy, xx, cc: (yy * 2 + xx) * 2 + cc
    return me, core, x, y, at


def entry_barrier(others):
    barrier = pltpu.get_barrier_semaphore()
    for other in others:
        pl.semaphore_signal(barrier, inc=1, **peer(other))
    pl.semaphore_wait(barrier, len(others))


def named_experts(ids_cols, base, n_loc):
    n_tok = ids_cols.shape[0]
    lane = lax.broadcasted_iota(jnp.int32, (n_tok, 128), 1)
    id0 = ids_cols[:, 0:1].astype(jnp.int32) - base
    id1 = ids_cols[:, 1:2].astype(jnp.int32) - base
    hit = jnp.logical_and(jnp.logical_or(id0 == lane, id1 == lane), lane < n_loc)
    return id0, id1, lane, hit.astype(F32)


def gather_kernel(n_loc, z_ref, idst_ref, zall_ref, cols_ref, meta_ref, flip, ids_ref, idsall, send_sem, recv_sem):
    me, core, x, y, at = neighbours()
    twin = at(y, x, 1 - core)
    chips = [(y, 1 - x), (1 - y, x), (1 - y, 1 - x)]
    tok = z_ref.shape[0]
    group_n = zall_ref.shape[0]
    ids_ref[...] = jnp.zeros_like(ids_ref)
    ids_ref[0:2, 0:tok] = idst_ref[...].astype(F32)
    entry_barrier([twin] + [at(cy, cx, core) for cy, cx in chips])

    def send(slot, which, src, row, to):
        dst = (idsall, zall_ref)[which]
        cp = pltpu.make_async_remote_copy(
            src_ref=src, dst_ref=dst.at[row], send_sem=send_sem.at[slot, which], recv_sem=recv_sem.at[slot, which], **peer(to))
        cp.start()
        return cp

    far = [at(cy, cx, core) for cy, cx in chips]
    ids_sent = [send(j, 0, ids_ref, me, far[j]) for j in range(3)] + [send(3, 0, ids_ref, me, twin)]
    z_sent = {j: send(j, 1, z_ref, me, far[j]) for j in (2, 0, 1)}
    z_sent[3] = send(3, 1, z_ref, me, twin)
    zall_ref[me] = z_ref[...]
    idsall[me] = ids_ref[...]
    relays = []
    for j in range(3):
        ids_sent[j].wait_recv()
        relays.append(send(4 + j, 0, idsall.at[far[j]], far[j], twin))
    ids_sent[3].wait_recv()
    for cp in relays:
        cp.wait_recv()

    flip[...] = jnp.zeros_like(flip)
    for d in range(group_n):
        flip[2 * d:2 * d + 2, :] = idsall[d, 0:2, :]
    cols = jnp.transpose(flip[...])[:tok]
    lane_b = lax.broadcasted_iota(jnp.int32, (tok, 128), 1)
    wide = [jnp.where(lane_b == 0, cols[:, 2 * d:2 * d + 1], cols[:, 2 * d + 1:2 * d + 2]) for d in range(group_n)]
    cols_ref[...] = jnp.concatenate(wide, axis=0)
    _, _, _, hit = named_experts(cols_ref[...], me * n_loc, n_loc)
    ones = jnp.ones((group_n * tok, 128), BF16)
    count = lax.dot_general(hit.astype(BF16), ones, (((0,), (0,)), ((), ())), preferred_element_type=F32)
    row_i = lax.broadcasted_iota(jnp.int32, (128, 128), 0)
    col_i = lax.broadcasted_iota(jnp.int32, (128, 128), 1)
    named = (count > 0.5).astype(F32)
    order = jnp.dot((row_i > col_i).astype(BF16), named.astype(BF16), preferred_element_type=F32)
    spot = jnp.where(order == col_i.astype(F32), named, 0.0)
    expert_list = jnp.sum(spot * row_i.astype(F32), axis=0, keepdims=True)
    counts = jnp.sum(hit, axis=0, keepdims=True)
    total = jnp.sum(named, axis=0, keepdims=True)
    meta_ref[...] = jnp.concatenate([counts, expert_list, total, jnp.zeros((5, 128), F32)], axis=0).astype(jnp.int32)

    z_relays = []
    for j in (0, 1, 2):
        z_sent[j].wait_recv()
        z_relays.append(send(4 + j, 1, zall_ref.at[far[j]], far[j], twin))
    z_sent[3].wait_recv()
    for cp in z_relays:
        cp.wait_recv()
    for cp in ids_sent + relays + list(z_sent.values()) + z_relays:
        cp.wait_send()


def in_vmem(arr):
    return pltpu.with_memory_space_constraint(arr, VMEM)


def gather_tokens(z_bf, ids_t, group_n, n_loc):
    tok, d_model = z_bf.shape
    return pl.pallas_call(
        functools.partial(gather_kernel, n_loc),
        out_shape=[VMEM((group_n, tok, d_model), BF16), VMEM((group_n * tok, 128), F32), jax.ShapeDtypeStruct((8, 128), jnp.int32)],
        in_specs=[pl.BlockSpec(memory_space=VMEM)] * 2,
        out_specs=[pl.BlockSpec(memory_space=VMEM)] * 3,
        scratch_shapes=[VMEM((128, 128), F32), VMEM((8, 128), F32), VMEM((group_n, 8, 128), F32),
                        pltpu.SemaphoreType.DMA((7, 2)), pltpu.SemaphoreType.DMA((7, 2))],
        compiler_params=pltpu.CompilerParams(collective_id=0, has_side_effects=True, vmem_limit_bytes=16 * 1024 * 1024),
        name='gather_tokens',
    )(in_vmem(z_bf), ids_t)


def reduce_kernel(part_ref, hid_ref, out_ref, r1, s1, r2, s2, r3, send_sem, recv_sem):
    me, core, x, y, at = neighbours()
    twin, xn, yn = at(y, x, 1 - core), at(y, 1 - x, core), at(1 - y, x, core)
    entry_barrier([twin, xn, yn])
    half = hid_ref.shape[1] // 2
    cols = (pl.ds(0, half), pl.ds(half, half))

    def send(slot, src, dst, to):
        cp = pltpu.make_async_remote_copy(src_ref=src, dst_ref=dst, send_sem=send_sem.at[slot], recv_sem=recv_sem.at[slot], **peer(to))
        cp.start()
        return cp

    chips = [(1 - y, 1 - x), (y, 1 - x), (1 - y, x), (y, x)]
    first = [send(k, part_ref.at[at(cy, cx, 1 - core)], r1.at[k], twin) for k, (cy, cx) in enumerate(chips)]

    def sum1(k):
        first[k].wait_recv()
        cy, cx = chips[k]
        s1[k] = part_ref[at(cy, cx, core)] + r1[k]

    sum1(0)
    a0 = send(4, s1.at[0, :, cols[0]], r2.at[0, 0], xn)
    b0 = send(5, s1.at[0, :, cols[1]], r2.at[1, 0], yn)
    sum1(1)
    a1 = send(6, s1.at[1, :, cols[0]], r2.at[0, 1], xn)
    sum1(2)
    b1 = send(7, s1.at[2, :, cols[1]], r2.at[1, 1], yn)
    sum1(3)
    a0.wait_recv()
    s2[0] = s1[2, :, :half] + r2[0, 0]
    a2 = send(8, s2.at[0], r3.at[0], yn)
    b0.wait_recv()
    s2[1] = s1[1, :, half:] + r2[1, 0]
    b2 = send(9, s2.at[1], r3.at[1], xn)
    a1.wait_recv()
    own_a = hid_ref[:, :half] + s1[3, :, :half] + r2[0, 1]
    b1.wait_recv()
    own_b = hid_ref[:, half:] + s1[3, :, half:] + r2[1, 1]
    a2.wait_recv()
    out_ref[:, :half] = (own_a + r3[0]).astype(BF16)
    b2.wait_recv()
    out_ref[:, half:] = (own_b + r3[1]).astype(BF16)
    for cp in first + [a0, b0, a1, b1, a2, b2]:
        cp.wait_send()


def reduce_outputs(partial, hid_f32):
    group_n, tok, d_model = partial.shape
    half = d_model // 2
    return pl.pallas_call(
        reduce_kernel,
        out_shape=VMEM((tok, d_model), BF16),
        in_specs=[pl.BlockSpec(memory_space=VMEM)] * 2,
        out_specs=pl.BlockSpec(memory_space=VMEM),
        scratch_shapes=[
            VMEM((4, tok, d_model), F32), VMEM((4, tok, d_model), F32),
            VMEM((2, 2, tok, half), F32), VMEM((2, tok, half), F32), VMEM((2, tok, half), F32),
            pltpu.SemaphoreType.DMA((10,)), pltpu.SemaphoreType.DMA((10,)),
        ],
        compiler_params=pltpu.CompilerParams(collective_id=1, has_side_effects=True, vmem_limit_bytes=16 * 1024 * 1024),
        name='reduce_outputs',
    )(in_vmem(partial), in_vmem(hid_f32))


ROWS = 64
SPLIT = 2
SLOTS = 6


def expert_kernel(meta_sm, z_ref, cols_ref, rw_ref, b1_in, b2_in, w1_hbm, w2_hbm, out_ref,
                  b1_ref, b2_ref, w1_buf, w2_buf, rank_s, gate_s, x_s, o_s, sem1, sem2):
    n_tok, d_model = cols_ref.shape[0], z_ref.shape[2]
    n_loc = w1_hbm.shape[0]
    ff = w1_hbm.shape[2]
    fc = ff // SPLIT
    n_step = meta_sm[2, 0] * SPLIT

    def copies(step, slot):
        e = meta_sm[1, step // SPLIT]
        f0 = pl.multiple_of((step % SPLIT) * fc, fc)
        return (pltpu.make_async_copy(w1_hbm.at[e, :, pl.ds(f0, fc)], w1_buf.at[slot], sem1.at[slot]),
                pltpu.make_async_copy(w2_hbm.at[e, pl.ds(f0, fc), :], w2_buf.at[slot], sem2.at[slot]))

    for s in range(SLOTS):
        @pl.when(s < n_step)
        def _():
            for c in copies(s, s):
                c.start()

    b1_ref[...] = b1_in[...].astype(F32)
    b2_ref[...] = b2_in[...].astype(F32)
    z_all = z_ref[...].reshape(n_tok, d_model)
    id0, id1, lane, hit_t = named_experts(cols_ref[...], lax.axis_index('ep') * n_loc, n_loc)
    base = lax.axis_index('ep') * n_loc
    row_i = lax.broadcasted_iota(jnp.int32, (n_tok, n_tok), 0)
    col_i = lax.broadcasted_iota(jnp.int32, (n_tok, n_tok), 1)
    before = (row_i < col_i).astype(BF16)
    hit = jnp.transpose(hit_t)
    rank = jnp.dot(hit.astype(BF16), before, preferred_element_type=F32)
    rank_s[...] = jnp.where(hit > 0.5, rank, -1.0)

    logits = jnp.dot(z_all, rw_ref[...], preferred_element_type=F32)
    top = jnp.max(logits, axis=-1, keepdims=True)
    ex = jnp.exp(logits - top)
    probs = ex / jnp.sum(ex, axis=-1, keepdims=True)
    p0 = jnp.sum(jnp.where(lane == id0 + base, probs, 0.0), axis=-1, keepdims=True)
    p1 = jnp.sum(jnp.where(lane == id1 + base, probs, 0.0), axis=-1, keepdims=True)
    tot = p0 + p1
    g0, g1 = p0 / tot, p1 / tot
    gate_s[...] = jnp.where(lane == id0, g0, jnp.where(lane == id1, g1, 0.0))
    out_ref[...] = jnp.zeros_like(out_ref)

    def step_body(step, carry):
        slot = step % SLOTS
        e = meta_sm[1, step // SPLIT]
        part = step % SPLIT
        blocks = (meta_sm[0, e] + ROWS - 1) // ROWS
        slot_i = lax.broadcasted_iota(jnp.int32, (ROWS, n_tok), 0)

        def pick(j):
            want = (slot_i + j * ROWS).astype(F32)
            return (want == rank_s[pl.ds(e, 1), :]).astype(BF16)

        @pl.when(part == 0)
        def _():
            def gather_body(j, c):
                x_s[j] = jnp.dot(pick(j), z_ref[...].reshape(n_tok, d_model), preferred_element_type=F32).astype(BF16)
                o_s[j] = jnp.broadcast_to(b2_ref[pl.ds(e, 1), :], (ROWS, d_model))
                return c
            lax.fori_loop(0, blocks, gather_body, 0)

        for c in copies(step, slot):
            c.wait()
        bias = b1_ref[pl.ds(e, 1), pl.ds(pl.multiple_of(part * fc, fc), fc)]

        def block_body(j, c):
            inner = jnp.dot(x_s[j], w1_buf[slot], preferred_element_type=F32) + bias
            inner = jnp.maximum(inner, 0.0).astype(BF16)
            o_s[j] += jnp.dot(inner, w2_buf[slot], preferred_element_type=F32)
            return c
        lax.fori_loop(0, blocks, block_body, 0)

        @pl.when(step + SLOTS < n_step)
        def _():
            for c in copies(step + SLOTS, slot):
                c.start()

        @pl.when(part == SPLIT - 1)
        def _():
            lane_g = lax.broadcasted_iota(jnp.int32, (n_tok, 128), 1)
            gate = jnp.sum(jnp.where(lane_g == e, gate_s[...], 0.0), axis=-1, keepdims=True)

            def scatter_body(j, c):
                back = lax.dot_general(pick(j), o_s[j].astype(BF16), (((0,), (0,)), ((), ())), preferred_element_type=F32)
                out_ref[...] += (gate * back).reshape(out_ref.shape)
                return c
            lax.fori_loop(0, blocks, scatter_body, 0)
        return carry

    lax.fori_loop(0, n_step, step_body, 0)


def run_experts(meta, z_all, cols, router_w, exp_w1, exp_b1, exp_w2, exp_b2):
    group_n, tok, d_model = z_all.shape
    n_tok = group_n * tok
    n_loc, _, ff = exp_w1.shape
    fc = ff // SPLIT
    n_blk = n_tok // ROWS
    vm = pl.BlockSpec(memory_space=VMEM)
    hbm = pl.BlockSpec(memory_space=pl.ANY)
    return pl.pallas_call(
        expert_kernel,
        out_shape=VMEM((group_n, tok, d_model), F32),
        in_specs=[pl.BlockSpec(memory_space=pltpu.SMEM)] + [vm] * 5 + [hbm] * 2,
        out_specs=vm,
        scratch_shapes=[
            VMEM((n_loc, ff), F32), VMEM((n_loc, d_model), F32),
            VMEM((SLOTS, d_model, fc), BF16), VMEM((SLOTS, fc, d_model), BF16),
            VMEM((128, n_tok), F32), VMEM((n_tok, 128), F32),
            VMEM((n_blk, ROWS, d_model), BF16), VMEM((n_blk, ROWS, d_model), F32),
            pltpu.SemaphoreType.DMA((SLOTS,)), pltpu.SemaphoreType.DMA((SLOTS,)),
        ],
        compiler_params=pltpu.CompilerParams(vmem_limit_bytes=48 * 1024 * 1024),
        name='run_experts',
    )(meta, in_vmem(z_all), in_vmem(cols), router_w, exp_b1, exp_b2, exp_w1, exp_w2)


def solution(mesh):
    group_n = mesh.shape['ep']

    def local_step(hidden, self_pos, src_len, cache_a, cross_a, cache_b, cross_b, route_ids, ln_gain, ln_shift, attn_w, attn_b, ffn_w1, ffn_b1, ffn_w2, ffn_b2, router_w, exp_w1, exp_b1, exp_w2, exp_b2):
        hid_f32, z_bf, cache_a_new, cache_b_new = dense_layers(hidden, self_pos, src_len, cache_a, cross_a, cache_b, cross_b, ln_gain, ln_shift, attn_w, attn_b, ffn_w1, ffn_b1, ffn_w2, ffn_b2)
        z_all, cols, meta = gather_tokens(z_bf, route_ids.T, group_n, exp_w1.shape[0])
        partial = run_experts(meta, z_all, cols, router_w, exp_w1, exp_b1, exp_w2, exp_b2)
        out = reduce_outputs(partial, hid_f32)
        return out, cache_a_new, cache_b_new

    tok_spec = P(('dp', 'ep'))
    cache_spec = P(None, ('dp', 'ep'))
    rep_spec = P()
    exp_spec = P('ep')
    in_specs = (tok_spec, tok_spec, tok_spec, cache_spec, cache_spec, cache_spec, cache_spec, tok_spec) + (rep_spec,) * 9 + (exp_spec,) * 4
    out_specs = (tok_spec, cache_spec, cache_spec)
    return jax.shard_map(local_step, mesh=mesh, in_specs=in_specs, out_specs=out_specs, check_vma=False)
```
